32 devices in a mesh: dp: 8 (over z, x), tensor: 4 (over y, core).
Axes of the slice: x: 2, y: 2, z: 4, core: 2. Of those that a mesh axis runs over, the one named last changes fastest.
Arguments:
- inputs: bfloat16 [8, 2048, 768], P('dp', 'tensor'), may hold values from -6 to 6
- segments: int32 [8, 2048], P('dp', 'tensor'), may hold values from 0 to 7, never falling along the last dimension, each value on 1 to 1792 neighbouring positions
- query_weight: bfloat16 [768, 768], P('dp', 'tensor'), may hold values from -0.21875 to 0.21875
- query_bias: bfloat16 [768], P('tensor'), may hold values from -1.75 to 1.75
- key_weight: bfloat16 [768, 768], P('dp', 'tensor'), may hold values from -0.21875 to 0.21875
- value_weight: bfloat16 [768, 768], P('dp', 'tensor'), may hold values from -0.21875 to 0.21875
- value_bias: bfloat16 [768], P('tensor'), may hold values from -1.75 to 1.75
- output_weight: bfloat16 [768, 768], P('tensor', 'dp'), may hold values from -0.875 to 0.875
- output_bias: bfloat16 [768], replicated, may hold values from -1.75 to 1.75
- up_weight: bfloat16 [768, 3072], P('dp', 'tensor'), may hold values from -0.21875 to 0.21875
- up_bias: bfloat16 [3072], P('tensor'), may hold values from -1.75 to 1.75
- down_weight: bfloat16 [3072, 768], P('tensor', 'dp'), may hold values from -0.109375 to 0.109375
- down_bias: bfloat16 [768], replicated, may hold values from -1.75 to 1.75
- first_gain: float32 [768], replicated, may hold values from 0.5 to 1.5
- first_shift: float32 [768], replicated, may hold values from -1.75 to 1.75
- second_gain: float32 [768], replicated, may hold values from 0.5 to 1.5
- second_shift: float32 [768], replicated, may hold values from -1.75 to 1.75
- cotangent: bfloat16 [8, 2048, 768], P('dp', 'tensor'), may hold values from -6 to 6
Outputs:
- layer_out: bfloat16 [8, 2048, 768], P('dp', 'tensor')
- grad_inputs: float32 [8, 2048, 768], P('dp', 'tensor')
- query_weight_gradient: float32 [768, 768], P('dp', 'tensor')
- sum_query: float32 [768], P('tensor')
- key_weight_gradient: float32 [768, 768], P('dp', 'tensor')
- value_weight_gradient: float32 [768, 768], P('dp', 'tensor')
- sum_value: float32 [768], P('tensor')
- grad_output: float32 [768, 768], P('tensor', 'dp')
- sum_output: float32 [768], replicated
- up_weight_gradient: float32 [768, 3072], P('dp', 'tensor')
- sum_up: float32 [3072], P('tensor')
- down_weight_gradient: float32 [3072, 768], P('tensor', 'dp')
- sum_down: float32 [768], replicated
- gain_first: float32 [768], replicated
- shift_first: float32 [768], replicated
- gain_second: float32 [768], replicated
- shift_second: float32 [768], replicated
The draws below stay inside these ranges and needn't reach their ends.
Inputs may be any that keep to these rules, and one draw needn't show every extreme that they name: `segments`: document numbers never fall along a sequence; each document has 1 to 1792 tokens, and one has exactly 1792.
All inputs are finite; a program needn't handle non-finite values.
Results may differ from the reference program's by a relative error of at most 0.014.
Values may be sent and summed in bfloat16 or wider, within the bound.
No kernel may reach another device: no remote copies, remote signals or barrier semaphores. Data moves between devices by JAX's collectives and lax.ppermute only.
A program may use at most 128 MiB of HBM per device.

```python
import math
import jax
import jax.numpy as jnp
import numpy as np
from jax import lax

D = 768
HEADS = 12
HEAD = 64
FF = 3072
LEN = 2048
DOCS = 8
NSEQ = 8
QBLOCK = 512
DOC_MOST = 1792


def level_of(stream_key, dims, split, smallest, top_value):
    loudness = 1.0
    for dim, blocks in split:
        draws = jax.random.uniform(jax.random.fold_in(jax.random.fold_in(stream_key, 6), dim), (blocks,), jnp.float32, smallest / len(split), top_value / len(split))
        loudness = loudness * jnp.repeat(jnp.exp(draws), dims[dim] // blocks).reshape((-1,) + (1,) * (len(dims) - 1 - dim))
    return loudness


def split_up(count, total, limit, skew):
    weights = [(1 << 20) // math.isqrt(standing ** skew) + 1 for standing in range(2, count + 1)]
    spare, counts = total - limit - (count - 1), [1] * (count - 1)
    while spare > 0:
        candidates = [i for i in range(count - 1) if counts[i] < limit]
        whole, left = sum([weights[i] for i in candidates]), spare
        for i in candidates:
            addition = min(limit - counts[i], max(1, left * weights[i] // whole), spare)
            counts[i] = counts[i] + addition
            spare = spare - addition
    return np.array([limit] + counts)


def ragged(key, amount, total, most, lean):
    if amount == 2:
        one = jax.random.randint(key, (), max(1, total - most), min(most, total - 1) + 1)
        return jnp.stack([one, total - one])
    sizes = jnp.asarray(split_up(amount, total, most, lean), jnp.int32)
    pairs = (amount - 1) // 2
    giver, sink = sizes[1:1 + 2 * pairs:2], sizes[2:2 + 2 * pairs:2]
    margin = jnp.minimum(giver - 1, most - sink)
    moved = jax.random.randint(jax.random.fold_in(key, 1), (pairs,), 0, 1 << 20) % (margin + 1)
    sizes = sizes.at[1:1 + 2 * pairs:2].set(giver - moved).at[2:2 + 2 * pairs:2].set(sink + moved)
    return sizes[jax.random.permutation(jax.random.fold_in(key, 2), amount)]


def noise(own_key, shape, scale, limit, cuts=(), dtype=jnp.bfloat16):
    values = jax.random.normal(own_key, shape, jnp.float32) * scale
    if len(cuts) > 0:
        values = level_of(own_key, shape, cuts, -0.22, 0.18) * values
    return jnp.clip(values, min=-limit, max=limit).astype(dtype)


def setup_inputs(seed: int = 0) -> dict:
    arg_keys = jax.random.split(jax.random.key(seed), 19)
    inputs = noise(arg_keys[0], (NSEQ, LEN, D), 1.0, 6.0, ((0, 8), (1, 4)))
    segments = jax.vmap(lambda own: jnp.searchsorted(jnp.cumsum(ragged(own, DOCS, LEN, DOC_MOST, 2)), jnp.arange(LEN), side="right"))(jax.random.split(arg_keys[1], NSEQ)).reshape((NSEQ, LEN)).astype(jnp.int32)
    query_weight = noise(arg_keys[2], (D, D), D ** -0.5, 0.21875, ((0, 8), (1, 4)))
    query_bias = noise(arg_keys[3], (D,), 0.3, 1.75, ((0, 4),))
    key_weight = noise(arg_keys[4], (D, D), D ** -0.5, 0.21875, ((0, 8), (1, 4)))
    value_weight = noise(arg_keys[5], (D, D), D ** -0.5, 0.21875, ((0, 8), (1, 4)))
    value_bias = noise(arg_keys[6], (D,), 0.3, 1.75, ((0, 4),))
    output_weight = noise(arg_keys[7], (D, D), (D // 16) ** -0.5, 0.875, ((0, 4), (1, 8)))
    output_bias = noise(arg_keys[8], (D,), 0.3, 1.75)
    up_weight = noise(arg_keys[9], (D, FF), D ** -0.5, 0.21875, ((0, 8), (1, 4)))
    up_bias = noise(arg_keys[10], (FF,), 0.3, 1.75, ((0, 4),))
    down_weight = noise(arg_keys[11], (FF, D), FF ** -0.5, 0.109375, ((0, 4), (1, 8)))
    down_bias = noise(arg_keys[12], (D,), 0.3, 1.75)
    first_gain = jnp.clip(1.0 + 0.1 * jax.random.normal(arg_keys[13], (D,), jnp.float32), 0.5, 1.5)
    first_shift = noise(arg_keys[14], (D,), 0.3, 1.75, (), jnp.float32)
    second_gain = jnp.clip(1.0 + 0.1 * jax.random.normal(arg_keys[15], (D,), jnp.float32), 0.5, 1.5)
    second_shift = noise(arg_keys[16], (D,), 0.3, 1.75, (), jnp.float32)
    cotangent = noise(arg_keys[17], (NSEQ, LEN, D), 1.0, 6.0, ((0, 8), (1, 4)))
    return dict(inputs=inputs, segments=segments, query_weight=query_weight, query_bias=query_bias, key_weight=key_weight, value_weight=value_weight, value_bias=value_bias, output_weight=output_weight, output_bias=output_bias, up_weight=up_weight, up_bias=up_bias, down_weight=down_weight, down_bias=down_bias, first_gain=first_gain, first_shift=first_shift, second_gain=second_gain, second_shift=second_shift, cotangent=cotangent)


highest = lax.Precision.HIGHEST
eps_norm = 1e-12

@jax.custom_vjp
def low(v):
    return lax.optimization_barrier(v.astype(jnp.bfloat16)).astype(jnp.float32)

@jax.custom_vjp
def low_back(v):
    return v

def low_keep(v):
    return (low(v), None)

def low_pass(kept, grad):
    return (grad,)

def back_keep(v):
    return (v, None)

def back_low(kept, grad):
    return (low(grad),)
low.defvjp(low_keep, low_pass)
low_back.defvjp(back_keep, back_low)

def rounded(values):
    return low(low_back(values))

def matmul_high(left, right):
    return jnp.matmul(left, right, precision=highest)

def normalize(values, gain, offset):
    average = lax.optimization_barrier(jnp.mean(values, axis=-1, keepdims=True))
    centred = values - average
    spread = lax.optimization_barrier(jnp.mean(centred * centred, axis=-1, keepdims=True))
    return centred * lax.rsqrt(spread + eps_norm) * gain + offset

def layer(rows, doc_ids, params):
    query_weight, query_bias, key_weight, value_weight, value_bias, output_weight, output_bias, up_weight, up_bias, down_weight, down_bias, first_gain, first_shift, second_gain, second_shift = params
    length = rows.shape[0]
    queries = rounded(matmul_high(rows, query_weight) + query_bias).reshape(length, HEADS, HEAD)
    keys_all = rounded(matmul_high(rows, key_weight)).reshape(length, HEADS, HEAD)
    values_all = rounded(matmul_high(rows, value_weight) + value_bias).reshape(length, HEADS, HEAD)
    blocks = length // QBLOCK
    query_blocks = queries.reshape(blocks, QBLOCK, HEADS, HEAD)
    doc_blocks = doc_ids.reshape(blocks, QBLOCK)

    def attend(pair):
        block_queries, block_docs = pair
        scores = low_back(jnp.einsum('qhd,khd->hqk', block_queries, keys_all, precision=highest) * 0.125)
        same_doc = block_docs[:, None] == doc_ids[None, :]
        scores = jnp.where(same_doc[None], scores, -1e+30)
        weights = low(jax.nn.softmax(scores, axis=-1))
        return jnp.einsum('hqk,khd->qhd', weights, values_all, precision=highest)
    mixed = lax.map(jax.checkpoint(attend), (query_blocks, doc_blocks))
    mixed = rounded(mixed.reshape(length, HEADS * HEAD))
    attn_branch = low_back(matmul_high(mixed, output_weight))
    hidden = rows + attn_branch + output_bias
    normed_first = normalize(hidden, first_gain, first_shift)
    inner = low_back(matmul_high(low(normed_first), up_weight) + up_bias)
    gelu_activation_out = low(jax.nn.gelu(inner, approximate=False))
    ffn_branch = low_back(matmul_high(gelu_activation_out, down_weight))
    second_in = normed_first + ffn_branch + down_bias
    return normalize(second_in, second_gain, second_shift)

def reference(inputs, segments, query_weight, query_bias, key_weight, value_weight, value_bias, output_weight, output_bias, up_weight, up_bias, down_weight, down_bias, first_gain, first_shift, second_gain, second_shift, cotangent):
    params = (query_weight.astype(jnp.float32), query_bias.astype(jnp.float32), key_weight.astype(jnp.float32), value_weight.astype(jnp.float32), value_bias.astype(jnp.float32), output_weight.astype(jnp.float32), output_bias.astype(jnp.float32), up_weight.astype(jnp.float32), up_bias.astype(jnp.float32), down_weight.astype(jnp.float32), down_bias.astype(jnp.float32), first_gain.astype(jnp.float32), first_shift.astype(jnp.float32), second_gain.astype(jnp.float32), second_shift.astype(jnp.float32))

    def accumulate(totals, item):
        rows, doc_ids, upstream = item

        def run(rows_float, weights):
            return layer(rows_float, doc_ids, weights)
        result, pull = jax.vjp(run, rows.astype(jnp.float32), params)
        grad_rows, grad_params = pull(upstream.astype(jnp.float32))
        totals = jax.tree.map(jnp.add, totals, grad_params)
        return (totals, (result.astype(jnp.bfloat16), grad_rows))
    zeros = jax.tree.map(jnp.zeros_like, params)
    totals, outputs = lax.scan(accumulate, zeros, (inputs, segments, cotangent))
    return (outputs[0], outputs[1], totals[0], totals[1], totals[2], totals[3], totals[4], totals[5], totals[6], totals[7], totals[8], totals[9], totals[10], totals[11], totals[12], totals[13], totals[14])
```

```python
import functools

import jax
import jax.numpy as jnp
from jax import lax
from jax.experimental import pallas as pl
from jax.experimental.pallas import tpu as pltpu
from jax.sharding import PartitionSpec as P

HEAD = 64
BF = jnp.bfloat16
F32 = jnp.float32

eps_norm = 1e-12
root_half = 0.7071067811865476
density = 0.3989422804014327
scale = 0.125
log2e = 1.4426950408889634
far = 1e30
vmem_bytes = 60 * 1024 * 1024


def product(left, right):
    return jnp.dot(left, right, preferred_element_type=F32)


def product_nt(left, right):
    return lax.dot_general(
        left, right, (((1,), (1,)), ((), ())), preferred_element_type=F32
    )


def product_tn(left, right):
    return lax.dot_general(
        left, right, (((0,), (0,)), ((), ())), preferred_element_type=F32
    )


def normalize(values, gain, offset):
    average = jnp.mean(values, axis=-1, keepdims=True)
    centred = values - average
    inverse = lax.rsqrt(jnp.mean(centred * centred, axis=-1, keepdims=True) + eps_norm)
    normed = centred * inverse
    return (normed * gain + offset, normed, inverse)


def norm_back(upstream, normed, inverse, gain):
    scaled = upstream * gain
    centred = scaled - jnp.mean(scaled, axis=-1, keepdims=True)
    return (centred - normed * jnp.mean(scaled * normed, axis=-1, keepdims=True)) * inverse


def load_keys(quarters, aux_key_ref, heads, first, keys_ref):
    width = heads * HEAD
    rows = quarters[0].shape[0]
    for h in range(heads):
        for r, ref in enumerate(quarters):
            block = pl.ds(r * rows, rows)
            keys_ref[h, block, :] = jnp.concatenate(
                [ref[:, first * width + h * HEAD : first * width + (h + 1) * HEAD], aux_key_ref[block, :]],
                axis=1,
            )


def forward_body(heads, *refs):
    quarters, (aux_query_ref, aux_key_ref, query_refs) = refs[:4], (refs[4], refs[5], refs[6:8])
    mixed_ref, log_ref = refs[8:10]
    keys_ref, query_ref, values_ref, out_ref = refs[10:]
    rows = quarters[0].shape[0]
    load_keys(quarters, aux_key_ref, heads, 1, keys_ref)
    width = heads * HEAD
    for h in range(heads):
        for r, ref in enumerate(quarters):
            piece = ref[:, 2 * width + h * HEAD : 2 * width + (h + 1) * HEAD]
            values_ref[h, :, r * rows : (r + 1) * rows] = piece.T
        for r, ref in enumerate(query_refs):
            block = pl.ds(r * rows, rows)
            query_ref[h, block, :] = jnp.concatenate(
                [ref[:, h * HEAD : (h + 1) * HEAD], aux_query_ref[block, :]], axis=1
            )

    def one_head(h, carry):
        scores = product_nt(keys_ref[h], query_ref[h])
        highest = jnp.max(scores, axis=0, keepdims=True)
        raised = jnp.exp2((scores - highest) * (scale * log2e))
        totals = jnp.sum(raised, axis=0, keepdims=True)
        out_ref[h] = product(values_ref[h], raised.astype(BF)) / totals
        log_ref[h] = highest * (scale * log2e) + jnp.log2(totals)
        return carry

    lax.fori_loop(0, heads, one_head, 0)
    for h in range(heads):
        mixed_ref[:, h * HEAD : (h + 1) * HEAD] = out_ref[h].T.astype(BF)


def attend_forward(quarters, aux_query, aux_key, which):
    rows = quarters[0].shape[0]
    length = 4 * rows
    heads = quarters[0].shape[1] // (3 * HEAD)
    count = 2 * rows
    whole = pl.BlockSpec(memory_space=pltpu.VMEM)
    flops = 4 * heads * count * length * HEAD * 4
    return pl.pallas_call(
        functools.partial(forward_body, heads),
        in_specs=[whole] * 8,
        out_specs=[whole] * 2,
        out_shape=[
            jax.ShapeDtypeStruct((count, heads * HEAD), BF),
            jax.ShapeDtypeStruct((heads, 1, count), F32),
        ],
        scratch_shapes=[
            pltpu.VMEM((heads, length, 2 * HEAD), BF),
            pltpu.VMEM((heads, count, 2 * HEAD), BF),
            pltpu.VMEM((heads, HEAD, length), BF),
            pltpu.VMEM((heads, HEAD, count), F32),
        ],
        compiler_params=pltpu.CompilerParams(vmem_limit_bytes=vmem_bytes),
        cost_estimate=pl.CostEstimate(
            flops=flops, bytes_accessed=8 * length * 576, transcendentals=heads * count * length
        ),
        name="attend_forward",
    )(*quarters, aux_query, aux_key, quarters[which[0]], quarters[which[1]])


def backward_body(heads, *refs):
    quarters, (aux_query_ref, aux_key_ref) = refs[:4], refs[4:6]
    mixed_refs, log_refs, grad_refs = refs[6:8], refs[8:10], refs[10:14]
    result_ref = refs[14]
    keys_ref, query_ref, values_ref, up_ref, keys_flat_ref, delta_ref, dq_ref, dk_ref, dv_ref = refs[15:]
    rows = quarters[0].shape[0]
    half = 2 * rows
    width = heads * HEAD
    load_keys(quarters, aux_key_ref, heads, 1, keys_ref)
    load_keys(quarters, aux_query_ref, heads, 0, query_ref)
    for h in range(heads):
        lanes = slice(h * HEAD, (h + 1) * HEAD)
        for r, ref in enumerate(quarters):
            block = pl.ds(r * rows, rows)
            values_ref[h, block, :] = ref[:, 2 * width + h * HEAD : 2 * width + (h + 1) * HEAD]
            keys_flat_ref[h, :, r * rows : (r + 1) * rows] = ref[
                :, width + h * HEAD : width + (h + 1) * HEAD
            ].T
            grad = grad_refs[r][:, lanes]
            up_ref[h, block, :] = grad
            out = mixed_refs[r // 2][(r % 2) * rows : (r % 2 + 1) * rows, lanes]
            both = grad.astype(F32) * out.astype(F32)
            delta_ref[h, :, r * rows : (r + 1) * rows] = jnp.sum(both.T, axis=0, keepdims=True)

    def one_head(h, carry):
        for part in range(2):
            block = pl.ds(part * half, half)
            scores = product_nt(keys_ref[h], query_ref[h, block, :])
            weights = jnp.exp2(scores * (scale * log2e) - log_refs[part][h])
            grad_weights = product_nt(values_ref[h], up_ref[h, block, :])
            grad_scores = (weights * (grad_weights - delta_ref[h, :, block])).astype(BF)
            dq_ref[h, :, block] = product(keys_flat_ref[h], grad_scores) * scale
            dk = product(grad_scores, query_ref[h, block, :])
            dv = product(weights.astype(BF), up_ref[h, block, :])
            if part == 0:
                dk_ref[h] = dk
                dv_ref[h] = dv
            else:
                dk_ref[h] = (dk_ref[h] + dk) * scale
                dv_ref[h] = dv_ref[h] + dv
        return carry

    lax.fori_loop(0, heads, one_head, 0)
    for h in range(heads):
        result_ref[:, h * HEAD : (h + 1) * HEAD] = dq_ref[h].T.astype(BF)
        result_ref[:, width + h * HEAD : width + (h + 1) * HEAD] = dk_ref[h, :, :HEAD].astype(BF)
        result_ref[:, 2 * width + h * HEAD : 2 * width + (h + 1) * HEAD] = dv_ref[h].astype(BF)


def attend_back(quarters, aux_query, aux_key, mixed, logs, grads):
    rows = quarters[0].shape[0]
    length = 4 * rows
    heads = quarters[0].shape[1] // (3 * HEAD)
    whole = pl.BlockSpec(memory_space=pltpu.VMEM)
    return pl.pallas_call(
        functools.partial(backward_body, heads),
        in_specs=[whole] * 14,
        out_specs=whole,
        out_shape=jax.ShapeDtypeStruct((length, 3 * heads * HEAD), BF),
        scratch_shapes=[
            pltpu.VMEM((heads, length, 2 * HEAD), BF),
            pltpu.VMEM((heads, length, 2 * HEAD), BF),
            pltpu.VMEM((heads, length, HEAD), BF),
            pltpu.VMEM((heads, length, HEAD), BF),
            pltpu.VMEM((heads, HEAD, length), BF),
            pltpu.VMEM((heads, 1, length), F32),
            pltpu.VMEM((heads, HEAD, length), F32),
            pltpu.VMEM((heads, length, 2 * HEAD), F32),
            pltpu.VMEM((heads, length, HEAD), F32),
        ],
        compiler_params=pltpu.CompilerParams(vmem_limit_bytes=vmem_bytes),
        cost_estimate=pl.CostEstimate(
            flops=10 * heads * length * length * HEAD * 4,
            bytes_accessed=12 * length * 576,
            transcendentals=heads * length * length,
        ),
        name="attend_back",
    )(*quarters, aux_query, aux_key, *mixed, *logs, *grads)


def exchanger(axis_dp, axis_tensor):
    def swap(values, dp_bits, tensor_bits):
        pairs = [
            (d * axis_tensor + t, (d ^ dp_bits) * axis_tensor + (t ^ tensor_bits))
            for d in range(axis_dp)
            for t in range(axis_tensor)
        ]
        return lax.ppermute(values, ("dp", "tensor"), pairs)

    return swap


def gather_bits(values, bits, swap):
    for bit in bits:
        values = jnp.concatenate([values, swap(values, bit, 0)], axis=0)
    return values


def block_order(device, count, bits):
    order = []
    for block in range(count):
        other = device ^ block
        place = jnp.int32(0)
        for i, bit in enumerate(bits):
            place = place + jnp.where((other & bit) != 0, 1 << i, 0)
        order.append(place)
    return order


def to_natural(values, order):
    rows = values.shape[0] // len(order)
    return jnp.concatenate(
        [lax.dynamic_slice_in_dim(values, place * rows, rows, 0) for place in order], axis=0
    )


def from_natural(values, device, bits):
    count = 1 << len(bits)
    rows = values.shape[0] // count
    blocks = []
    for place in range(count):
        other = sum(bit for i, bit in enumerate(bits) if place >> i & 1)
        blocks.append(lax.dynamic_slice_in_dim(values, (device ^ other) * rows, rows, 0))
    return jnp.concatenate(blocks, axis=0)


def fold_bits(values, bits, swap):
    for bit in reversed(bits):
        half = values.shape[0] // 2
        moved = swap(values[half:].astype(BF), bit, 0)
        values = values[:half].astype(F32) + moved.astype(F32)
    return values


def local(
    axis_dp,
    axis_tensor,
    inputs,
    segments,
    query_weight,
    query_bias,
    key_weight,
    value_weight,
    value_bias,
    output_weight,
    output_bias,
    up_weight,
    up_bias,
    down_weight,
    down_bias,
    first_gain,
    first_shift,
    second_gain,
    second_shift,
    cotangent,
):
    swap = exchanger(axis_dp, axis_tensor)
    device = lax.axis_index("dp")
    levels = axis_dp.bit_length() - 1
    bits = [1 << i for i in reversed(range(levels))]
    order = block_order(device, axis_dp, bits)
    rows, width = inputs.shape[1:]

    own = inputs[0]
    across = swap(own, 0, 2)
    docs = segments[0]
    docs = jnp.concatenate([docs, swap(docs, 0, 1)])
    docs = jnp.concatenate([docs, swap(docs, 0, 2)])
    own_qkv = jnp.concatenate([query_weight, key_weight, value_weight], axis=1)
    qkv_weight = gather_bits(own_qkv, bits, swap)
    tokens = [own, swap(own, 0, 1), across, swap(across, 0, 1)]

    bundle = jnp.concatenate([up_weight, output_weight.T, down_weight.T], axis=1)
    units = up_weight.shape[1]
    feats = output_weight.shape[0]
    bundle = gather_bits(bundle, bits[:-1], swap)
    last = bits[-1]
    bundle_a, bundle_b = bundle[:, : units + feats], bundle[:, units + feats :]
    bundle_a = jnp.concatenate([bundle_a, swap(bundle_a, last, 0)], axis=0)
    bundle_b2 = swap(bundle_b, 0, 2)
    bundle_a2 = swap(bundle_a, 0, 2)
    bundle_b = jnp.concatenate([bundle_b, swap(bundle_b, last, 0)], axis=0)
    bundle_b2 = jnp.concatenate([bundle_b2, swap(bundle_b2, last, 0)], axis=0)
    bundle_a = to_natural(bundle_a, order)
    bundle_a2 = to_natural(bundle_a2, order)
    bundle_b = to_natural(bundle_b, order)
    bundle_b2 = to_natural(bundle_b2, order)
    bundles_a = [bundle_a, swap(bundle_a, 0, 1), bundle_a2, swap(bundle_a2, 0, 1)]
    bundles_b = [bundle_b, swap(bundle_b, 0, 1), bundle_b2, swap(bundle_b2, 0, 1)]
    bias = up_bias.reshape(1, -1)
    bias = jnp.concatenate([bias, swap(bias, 0, 1)])
    bias = jnp.concatenate([bias, swap(bias, 0, 2)])

    qkv_weight = to_natural(qkv_weight, order)
    qkv_bias = jnp.concatenate(
        [query_bias, jnp.zeros_like(query_bias), value_bias]
    ).astype(F32)
    quarters = [(product(x, qkv_weight) + qkv_bias).astype(BF) for x in tokens]

    lane = lax.broadcasted_iota(jnp.int32, (1, HEAD), 1)
    same = docs[:, None] == lane
    aux_query = same.astype(BF)
    aux_key = jnp.where(same | (lane >= 8), 0.0, -far).astype(BF)
    half = 2 * rows
    mixed_other, log_other = attend_forward(quarters, aux_query[half:], aux_key, (2, 3))
    mixed_own, log_own = attend_forward(quarters, aux_query[:half], aux_key, (0, 1))
    mixed = [
        mixed_own[:rows],
        swap(mixed_own[rows:], 0, 1),
        swap(mixed_other[:rows], 0, 2),
        swap(mixed_other[rows:], 0, 3),
    ]

    attn = sum(product_nt(m, b[:, units:]) for m, b in zip(mixed, bundles_a))
    hidden = own.astype(F32) + attn + output_bias
    normed_first, unit_first, inverse_first = normalize(hidden, first_gain, first_shift)
    low = normed_first.astype(BF)
    activated, slopes = [], []
    ffn = 0.0
    for g in range(4):
        inner = product(low, bundles_a[g][:, :units]) + bias[g]
        both = 0.5 * (1.0 + lax.erf(inner * root_half))
        activated.append((inner * both).astype(BF))
        slopes.append((both + inner * density * jnp.exp(-0.5 * inner * inner)).astype(BF))
        ffn = ffn + product_nt(activated[g], bundles_b[g])
    second_in = normed_first + ffn + down_bias
    layer_out, unit_second, inverse_second = normalize(second_in, second_gain, second_shift)
    upstream = cotangent[0].astype(F32)
    grad_second = norm_back(upstream, unit_second, inverse_second, second_gain)
    second_low = grad_second.astype(BF)
    grad_inner = []
    back = 0.0
    for g in range(4):
        grad = product(second_low, bundles_b[g])
        grad_inner.append((grad * slopes[g].astype(F32)).astype(BF))
        back = back + product_nt(grad_inner[g], bundles_a[g][:, :units])
    grad_first = grad_second + back
    grad_hidden = norm_back(grad_first, unit_first, inverse_first, first_gain)
    grad_attn = grad_hidden.astype(BF)
    grad_mixed = [product(grad_attn, b[:, units:]).astype(BF) for b in bundles_a]
    upstreams = [
        grad_mixed[0],
        swap(grad_mixed[1], 0, 1),
        swap(grad_mixed[2], 0, 2),
        swap(grad_mixed[3], 0, 3),
    ]

    grads_a = [
        jnp.concatenate(
            [product_tn(low, grad_inner[g]), product_tn(grad_attn, mixed[g])], axis=1
        ).astype(BF)
        for g in range(4)
    ]
    grads_b = [product_tn(second_low, activated[g]).astype(BF) for g in range(4)]

    def add(left, right):
        return (left.astype(F32) + right.astype(F32)).astype(BF)

    a0 = add(grads_a[0], swap(grads_a[1], 0, 1))
    a2 = add(grads_a[2], swap(grads_a[3], 0, 1))
    b0 = add(grads_b[0], swap(grads_b[1], 0, 1))
    b2 = add(grads_b[2], swap(grads_b[3], 0, 1))
    a0, a2, b0, b2 = (from_natural(v, device, bits) for v in (a0, a2, b0, b2))
    part_a = add(a0, swap(a2, 0, 2))
    own_a = fold_bits(part_a, bits, swap)
    b0 = fold_bits(b0, bits[-1:], swap)
    b2 = fold_bits(b2, bits[-1:], swap).astype(BF)
    part_b = b0 + swap(b2, 0, 2).astype(F32)
    own_b = fold_bits(part_b, bits[:-1], swap)

    column = functools.partial(jnp.sum, axis=0)
    sums = jnp.stack(
        [
            column(grad_hidden),
            column(grad_second),
            column(grad_first * unit_first),
            column(grad_first),
            column(upstream * unit_second),
            column(upstream),
        ]
    )
    sum_up = [column(g.astype(F32)) for g in grad_inner]
    up_pair = jnp.stack([sum_up[0], sum_up[2], sum_up[1], sum_up[3]])
    moved = swap(jnp.concatenate([sums, up_pair[2:]]), 0, 1)
    sums, up_pair = sums + moved[:6], up_pair[:2] + moved[6:]
    moved = swap(jnp.concatenate([sums, up_pair[1:]]), 0, 2)
    totals = jnp.concatenate([sums + moved[:6], up_pair[:1] + moved[6:]])
    for bit in bits:
        totals = totals + swap(totals, bit, 0)

    grad_qkv = attend_back(
        quarters, aux_query, aux_key, (mixed_own, mixed_other), (log_own, log_other), upstreams
    )
    all_tokens = jnp.concatenate(tokens, axis=0)
    back_rows = [
        product_nt(grad_qkv[r * rows : (r + 1) * rows], qkv_weight) for r in range(4)
    ]
    moved = swap(jnp.concatenate([back_rows[1], back_rows[3]]).astype(BF), 0, 1)
    far_rows = (back_rows[2] + moved[rows:].astype(F32)).astype(BF)
    near_rows = back_rows[0] + moved[:rows].astype(F32)
    grad_inputs = grad_hidden + near_rows + swap(far_rows, 0, 2).astype(F32)

    grads_qkv = product_tn(all_tokens, grad_qkv).astype(BF)
    own_qkv = fold_bits(from_natural(grads_qkv, device, bits), bits, swap)
    head_sums = column(grad_qkv.astype(F32)).reshape(1, -1)
    for bit in bits:
        head_sums = head_sums + swap(head_sums, bit, 0)
    head_sums = head_sums[0]

    return (
        layer_out.astype(BF)[None],
        grad_inputs[None],
        own_qkv[:, :feats],
        head_sums[:feats],
        own_qkv[:, feats : 2 * feats],
        own_qkv[:, 2 * feats :],
        head_sums[2 * feats :],
        own_a[:, units:].T,
        totals[0],
        own_a[:, :units],
        totals[6],
        own_b.T,
        totals[1],
        totals[2],
        totals[3],
        totals[4],
        totals[5],
    )


def solution(mesh):
    axis_dp, axis_tensor = mesh.shape["dp"], mesh.shape["tensor"]
    if axis_tensor != 4 or axis_dp & (axis_dp - 1):
        raise ValueError("mesh sizes")
    return jax.shard_map(
        functools.partial(local, axis_dp, axis_tensor),
        mesh=mesh,
        in_specs=(
            P("dp", "tensor", None),
            P("dp", "tensor"),
            P("dp", "tensor"),
            P("tensor"),
            P("dp", "tensor"),
            P("dp", "tensor"),
            P("tensor"),
            P("tensor", "dp"),
            P(),
            P("dp", "tensor"),
            P("tensor"),
            P("tensor", "dp"),
            P(),
            P(),
            P(),
            P(),
            P(),
            P("dp", "tensor", None),
        ),
        out_specs=(
            P("dp", "tensor", None),
            P("dp", "tensor", None),
            P("dp", "tensor"),
            P("tensor"),
            P("dp", "tensor"),
            P("dp", "tensor"),
            P("tensor"),
            P("tensor", "dp"),
            P(),
            P("dp", "tensor"),
            P("tensor"),
            P("tensor", "dp"),
            P(),
            P(),
            P(),
            P(),
            P(),
        ),
        check_vma=False,
    )
```

```python
import functools

import jax
import jax.numpy as jnp
from jax import lax
from jax.experimental import pallas as pl
from jax.experimental.pallas import tpu as pltpu
from jax.sharding import PartitionSpec as P

HEAD = 64
BF = jnp.bfloat16
F32 = jnp.float32

eps_norm = 1e-12
root_half = 0.7071067811865476
density = 0.3989422804014327
scale = 0.125
log2e = 1.4426950408889634
far_score = 1e30
vmem_bytes = 60 * 1024 * 1024


def product(left, right):
    return jnp.dot(left, right, preferred_element_type=F32)


def product_nt(left, right):
    return lax.dot_general(left, right, (((1,), (1,)), ((), ())), preferred_element_type=F32)


def product_tn(left, right):
    return lax.dot_general(left, right, (((0,), (0,)), ((), ())), preferred_element_type=F32)


def normalize(values, gain, offset):
    average = jnp.mean(values, axis=-1, keepdims=True)
    centred = values - average
    inverse = lax.rsqrt(jnp.mean(centred * centred, axis=-1, keepdims=True) + eps_norm)
    normed = centred * inverse
    return (normed * gain + offset, normed, inverse)


def norm_back(upstream, normed, inverse, gain):
    scaled = upstream * gain
    centred = scaled - jnp.mean(scaled, axis=-1, keepdims=True)
    return (centred - normed * jnp.mean(scaled * normed, axis=-1, keepdims=True)) * inverse


def vmem():
    return pl.BlockSpec(memory_space=pltpu.VMEM)


def smem():
    return pl.BlockSpec(memory_space=pltpu.SMEM)


def params():
    return pltpu.CompilerParams(vmem_limit_bytes=vmem_bytes)


def cost(flops, moved, hard=0):
    return pl.CostEstimate(flops=int(flops), bytes_accessed=int(moved), transcendentals=int(hard))


def spec(dtype, *dims):
    return jax.ShapeDtypeStruct(dims, dtype)


def project_body(heads, *refs):
    token_refs, (weight_ref, row_bias_ref, column_bias_ref, aux_query_ref, aux_key_ref) = refs[:4], refs[4:9]
    all_ref, turned_ref, query_ref, key_ref, value_ref, value_t_ref, key_t_ref = refs[9:16]
    step = pl.program_id(0)
    width = heads * HEAD
    rows = all_ref.shape[0]

    @pl.when(step == 0)
    def _():
        turned_ref[...] = weight_ref[...].T

    for r, ref in enumerate(token_refs):

        @pl.when(step == r)
        def _(ref=ref):
            all_ref[...] = ref[:rows, :]

    tokens = all_ref[...]
    turned = (product_nt(turned_ref[...], tokens) + column_bias_ref[...]).astype(BF)
    plain = (product(tokens, weight_ref[:, width : 3 * width]) + row_bias_ref[...]).astype(BF)
    for h in range(heads):
        at = slice(h * HEAD, (h + 1) * HEAD)
        query_ref[h, :HEAD, :] = turned[at]
        query_ref[h, HEAD:, :] = aux_query_ref[...]
        key_t_ref[at, :] = turned[width : 2 * width][at]
        value_t_ref[at, :] = turned[2 * width :][at]
        key_ref[h] = jnp.concatenate([plain[:, at], aux_key_ref[...]], axis=1)
        value_ref[h] = plain[:, width + h * HEAD : width + (h + 1) * HEAD]


def project(weight, tokens, rows, row_bias, column_bias, aux_query, aux_key, heads):
    width = weight.shape[0]
    length = 4 * rows
    by_row = lambda n: pl.BlockSpec((rows, n), lambda r: (r, 0))
    headed = lambda n: pl.BlockSpec((heads, rows, n), lambda r: (0, r, 0))
    flat = pl.BlockSpec((heads * HEAD, rows), lambda r: (0, r))
    return pl.pallas_call(
        functools.partial(project_body, heads),
        grid=(4,),
        in_specs=[vmem()] * 7 + [pl.BlockSpec((HEAD, rows), lambda r: (0, r)), by_row(HEAD)],
        out_specs=[
            by_row(width),
            pl.BlockSpec((3 * heads * HEAD, width), lambda r: (0, 0)),
            pl.BlockSpec((heads, 2 * HEAD, rows), lambda r: (0, 0, r)),
            headed(2 * HEAD),
            headed(HEAD),
            flat,
            flat,
        ],
        out_shape=[
            spec(BF, length, width),
            spec(BF, 3 * heads * HEAD, width),
            spec(BF, heads, 2 * HEAD, length),
            spec(BF, heads, length, 2 * HEAD),
            spec(BF, heads, length, HEAD),
            spec(BF, heads * HEAD, length),
            spec(BF, heads * HEAD, length),
        ],
        compiler_params=params(),
        cost_estimate=cost(4 * length * width * 3 * heads * HEAD, 16 << 20),
        name="project",
    )(*tokens, weight, row_bias, column_bias, aux_query, aux_key)


def forward_body(count, key_ref, *refs):
    query_refs, value_ref, out_ref, log_ref = refs[:count], refs[count], refs[count + 1], refs[count + 2]
    chunk = key_ref.shape[1] // 4
    for i in range(count):
        query = query_refs[i][0]
        scores = [product(key_ref[0, c * chunk : (c + 1) * chunk, :], query) for c in range(4)]
        highest = None
        for c in range(4):
            peak = jnp.max(scores[c], axis=0, keepdims=True)
            now = peak if highest is None else jnp.maximum(highest, peak)
            raised = jnp.exp2((scores[c] - now) * (scale * log2e))
            part = jnp.sum(raised, axis=0, keepdims=True)
            mixed = product(value_ref[:, c * chunk : (c + 1) * chunk], raised.astype(BF))
            if highest is None:
                total, out = part, mixed
            else:
                shrink = jnp.exp2((highest - now) * (scale * log2e))
                total, out = total * shrink + part, out * shrink + mixed
            highest = now
        out_ref[i] = (out / total).astype(BF)
        log_ref[i, 0] = highest * (scale * log2e) + jnp.log2(total)


def attend_forward(keys, queries, values_t, quarters):
    heads, length, _ = keys.shape
    rows = length // 4
    count = len(quarters)
    return pl.pallas_call(
        functools.partial(forward_body, count),
        grid=(heads,),
        in_specs=[pl.BlockSpec((1, length, 2 * HEAD), lambda h: (h, 0, 0))]
        + [pl.BlockSpec((1, 2 * HEAD, rows), lambda h, q=q: (h, 0, q)) for q in quarters]
        + [pl.BlockSpec((HEAD, length), lambda h: (h, 0))],
        out_specs=[
            pl.BlockSpec((count, HEAD, rows), lambda h: (0, h, 0)),
            pl.BlockSpec((count, 1, 1, rows), lambda h: (0, h, 0, 0)),
        ],
        out_shape=[spec(BF, count, heads * HEAD, rows), spec(F32, count, heads, 1, rows)],
        compiler_params=params(),
        cost_estimate=cost(
            20 * count * heads * rows * length * HEAD, 4 << 20, heads * rows * length
        ),
        name="attend_forward",
    )(keys, *[queries] * count, values_t)


def backward_body(count, first, last, key_ref, value_ref, key_t_ref, *refs):
    groups, refs = [refs[4 * i : 4 * i + 4] for i in range(count)], refs[4 * count :]
    if not first:
        (old_dk_ref, old_dv_ref), refs = refs[:2], refs[2:]
    dq_refs, (dk_ref, dv_ref) = refs[:count], refs[count:]
    dk = dv = None
    for (query_ref, log_ref, mixed_ref, grad_ref), dq_ref in zip(groups, dq_refs):
        grad = grad_ref[...]
        delta = jnp.sum(grad.astype(F32) * mixed_ref[0].astype(F32), axis=0, keepdims=True)
        scores = product(key_ref[0], query_ref[0])
        weights = jnp.exp2(scores * (scale * log2e) - log_ref[0, 0])
        grad_weights = product(value_ref[0], grad)
        grad_scores = (weights * (grad_weights - delta)).astype(BF)
        dq_ref[...] = (product(key_t_ref[...], grad_scores) * scale).astype(BF)
        add_dk = product_nt(query_ref[0, :HEAD, :], grad_scores)
        add_dv = product_nt(grad, weights.astype(BF))
        dk = add_dk if dk is None else dk + add_dk
        dv = add_dv if dv is None else dv + add_dv
    if not first:
        dk = dk + old_dk_ref[...]
        dv = dv + old_dv_ref[...]
    if last:
        dk = dk * scale
    dk_ref[...] = dk.astype(dk_ref.dtype)
    dv_ref[...] = dv.astype(dv_ref.dtype)


def attend_back(operands, quarters, logs, mixed, grads, carried, last):
    keys, queries, values, keys_t = operands
    heads, length, _ = keys.shape
    rows = length // 4
    first = carried is None
    flat = lambda n: pl.BlockSpec((HEAD, n), lambda h: (h, 0))
    by_head = lambda *dims: pl.BlockSpec((1,) + dims, lambda h: (h, 0, 0))
    in_specs = [by_head(length, 2 * HEAD), by_head(length, HEAD), flat(length)]
    args = [keys, values, keys_t]
    for q, (log, i), (out, j), grad in zip(quarters, logs, mixed, grads):
        in_specs += [
            pl.BlockSpec((1, 2 * HEAD, rows), lambda h, q=q: (h, 0, q)),
            pl.BlockSpec((1, 1, 1, rows), lambda h, i=i: (i, h, 0, 0)),
            pl.BlockSpec((1, HEAD, rows), lambda h, j=j: (j, h, 0)),
            flat(rows),
        ]
        args += [queries, log, out, grad]
    count = len(quarters)
    aliases = {}
    if not first:
        if not last:
            aliases = {len(args): count, len(args) + 1: count + 1}
        in_specs += [flat(length)] * 2
        args += list(carried)
    kind = BF if last else F32
    outs = pl.pallas_call(
        functools.partial(backward_body, count, first, last),
        grid=(heads,),
        in_specs=in_specs,
        out_specs=[flat(rows)] * count + [flat(length)] * 2,
        out_shape=[spec(BF, heads * HEAD, rows)] * count + [spec(kind, heads * HEAD, length)] * 2,
        input_output_aliases=aliases,
        compiler_params=params(),
        cost_estimate=cost(
            50 * count * heads * rows * length * HEAD, 8 << 20, count * heads * rows * length
        ),
        name="attend_back",
    )(*args)
    return outs[:count], outs[count:]


def gelu_parts(inner):
    both = 0.5 * (1.0 + lax.erf(inner * root_half))
    slope = both + inner * density * jnp.exp(-0.5 * inner * inner)
    return (inner * both).astype(BF), slope.astype(BF)


def group_spec(rows, units):
    return pl.BlockSpec((1, rows, units), lambda t: (t, 0, 0))


def fixed(*dims):
    return pl.BlockSpec(dims, lambda t: (0,) * len(dims))


def out_copy(bundle_ref, out_ref, sem, units):
    feats = out_ref.shape[2]
    return pltpu.make_async_copy(bundle_ref.at[:, :, pl.ds(units, feats)], out_ref, sem)


def enter_body(units, meta_ref, bundle_ref, *refs):
    mixed_refs, (own_ref, out_bias_ref, gain_ref, shift_ref, up_ref, bias_ref) = refs[:4], refs[4:10]
    low_ref, unit_ref, inverse_ref, act_ref, slope_ref, out_ref, sem = refs[10:]

    @pl.when(pl.program_id(0) == 0)
    def _():
        copy = out_copy(bundle_ref, out_ref, sem, units)
        copy.start()
        hidden = own_ref[...].astype(F32) + out_bias_ref[...]
        copy.wait()
        for j, ref in enumerate(mixed_refs):
            hidden = hidden + product_nt(ref[...].T, out_ref[meta_ref[0] ^ j])
        first, unit, inverse = normalize(hidden, gain_ref[...], shift_ref[...])
        unit_ref[...] = unit
        inverse_ref[...] = inverse
        low_ref[...] = first.astype(BF)

    low = low_ref[...]
    step = units // 3
    for c in range(0, units, step):
        lanes = slice(c, c + step)
        inner = product(low, up_ref[0, :, lanes]) + bias_ref[0, :, lanes]
        act_ref[0, :, lanes], slope_ref[0, :, lanes] = gelu_parts(inner)


def enter(meta, bundle, units, mixed, own, out_bias, gain, shift, bias):
    rows, width = own.shape
    groups = bundle.shape[0]
    return pl.pallas_call(
        functools.partial(enter_body, units),
        grid=(groups,),
        in_specs=[smem(), pl.BlockSpec(memory_space=pl.ANY)]
        + [vmem()] * 8
        + [group_spec(width, units), group_spec(1, units)],
        out_specs=[fixed(rows, width), fixed(rows, width), fixed(rows, 1)]
        + [group_spec(rows, units)] * 2,
        out_shape=[spec(BF, rows, width), spec(F32, rows, width), spec(F32, rows, 1)]
        + [spec(BF, groups, rows, units)] * 2,
        scratch_shapes=[
            pltpu.VMEM((groups, width, bundle.shape[2] - units), BF),
            pltpu.SemaphoreType.DMA,
        ],
        compiler_params=params(),
        cost_estimate=cost(12 * rows * width * units, 20 << 20, 8 * rows * units),
        name="enter",
    )(meta, bundle, *mixed, own, out_bias, gain, shift, bundle, bias)


def turn_body(*refs):
    act_ref, down_ref, unit_ref, first_gain_ref, first_shift_ref = refs[:5]
    bias_ref, gain_ref, shift_ref, up_ref, out_ref, grad_ref, low_ref, sums_ref, total_ref = refs[5:]
    part = product_nt(act_ref[0], down_ref[0])
    step = pl.program_id(0)

    @pl.when(step == 0)
    def _():
        total_ref[...] = part

    @pl.when(step > 0)
    def _():
        total_ref[...] += part

    @pl.when(step == pl.num_programs(0) - 1)
    def _():
        first = unit_ref[...] * first_gain_ref[...] + first_shift_ref[...]
        second, unit, inverse = normalize(
            first + total_ref[...] + bias_ref[...], gain_ref[...], shift_ref[...]
        )
        out_ref[...] = second.astype(BF)
        upstream = up_ref[...].astype(F32)
        grad = norm_back(upstream, unit, inverse, gain_ref[...])
        grad_ref[...] = grad
        low_ref[...] = grad.astype(BF)
        sums_ref[0:1, :] = jnp.sum(grad, axis=0, keepdims=True)
        sums_ref[1:2, :] = jnp.sum(upstream * unit, axis=0, keepdims=True)
        sums_ref[2:3, :] = jnp.sum(upstream, axis=0, keepdims=True)


def turn(acts, downs, unit, first_gain, first_shift, bias, gain, shift, cotangent):
    rows, width = unit.shape
    groups, _, units = acts.shape
    return pl.pallas_call(
        turn_body,
        grid=(groups,),
        in_specs=[group_spec(rows, units), group_spec(width, units)] + [vmem()] * 7,
        out_specs=[fixed(rows, width)] * 3 + [fixed(3, width)],
        out_shape=[
            spec(BF, rows, width),
            spec(F32, rows, width),
            spec(BF, rows, width),
            spec(F32, 3, width),
        ],
        scratch_shapes=[pltpu.VMEM((rows, width), F32)],
        compiler_params=params(),
        cost_estimate=cost(8 * rows * width * units, 16 << 20),
        name="turn",
    )(acts, downs, unit, first_gain, first_shift, bias, gain, shift, cotangent)


def leave_body(units, meta_ref, bundle_ref, *refs):
    up_ref, down_ref, slope_ref, low_ref, second_ref, unit_ref, inverse_ref, gain_ref = refs[:8]
    inner_ref, hidden_ref, attn_ref, own_ref, next_ref, far_ref, sums_ref, out_ref, sem = refs[8:]
    step = pl.program_id(0)

    @pl.when(step == 0)
    def _():
        out_copy(bundle_ref, out_ref, sem, units).start()
        hidden_ref[...] = second_ref[...]

    grad = product(low_ref[...], down_ref[0]) * slope_ref[0].astype(F32)
    inner = grad.astype(BF)
    inner_ref[0] = inner
    sums_ref[pl.ds(3 + step, 1), :] = jnp.sum(inner.astype(F32), axis=0, keepdims=True)
    hidden_ref[...] += product_nt(inner, up_ref[0])

    @pl.when(step == pl.num_programs(0) - 1)
    def _():
        out_copy(bundle_ref, out_ref, sem, units).wait()
        back = hidden_ref[...]
        unit = unit_ref[...]
        hidden = norm_back(back, unit, inverse_ref[...], gain_ref[...])
        hidden_ref[...] = hidden
        sums_ref[0:1, :] = jnp.sum(hidden, axis=0, keepdims=True)
        sums_ref[1:2, :] = jnp.sum(back * unit, axis=0, keepdims=True)
        sums_ref[2:3, :] = jnp.sum(back, axis=0, keepdims=True)
        attn = hidden.astype(BF)
        attn_ref[...] = attn
        for j in range(4):
            mixed = product(attn, out_ref[meta_ref[0] ^ j]).T.astype(BF)
            if j == 0:
                own_ref[...] = mixed
            elif j == 1:
                next_ref[...] = mixed
            else:
                far_ref[j - 2] = mixed


def leave(meta, bundle, downs, slopes, low, second, unit, inverse, gain):
    rows, width = low.shape
    groups, _, units = downs.shape
    feats = bundle.shape[2] - units
    return pl.pallas_call(
        functools.partial(leave_body, units),
        grid=(groups,),
        in_specs=[smem(), pl.BlockSpec(memory_space=pl.ANY)]
        + [group_spec(width, units), group_spec(width, units), group_spec(rows, units)]
        + [vmem()] * 5,
        out_specs=[
            group_spec(rows, units),
            fixed(rows, width),
            fixed(rows, width),
            fixed(feats, rows),
            fixed(feats, rows),
            fixed(2, feats, rows),
            fixed(3 + groups, width),
        ],
        out_shape=[
            spec(BF, groups, rows, units),
            spec(F32, rows, width),
            spec(BF, rows, width),
            spec(BF, feats, rows),
            spec(BF, feats, rows),
            spec(BF, 2, feats, rows),
            spec(F32, 3 + groups, width),
        ],
        scratch_shapes=[pltpu.VMEM((groups, width, feats), BF), pltpu.SemaphoreType.DMA],
        compiler_params=params(),
        cost_estimate=cost(16 * rows * width * units, 28 << 20),
        name="leave",
    )(meta, bundle, bundle, downs, slopes, low, second, unit, inverse, gain)


def outer_body(shard, extra, meta_ref, left_ref, right_ref, *refs):
    if extra:
        attn_ref, mixed_refs, sum_refs, refs = refs[0], refs[1:5], refs[5:7], refs[7:]
    keep_ref, send_ref, left_t_ref = refs[:3]
    step = pl.program_id(0)
    units = right_ref.shape[2]
    width = left_ref.shape[1]
    pairs = width // shard // 2
    lanes = keep_ref.shape[3]

    @pl.when(step == 0)
    def _():
        left_t_ref[...] = left_ref[...].T
        if extra:
            refs[3][...] = attn_ref[...].T

    def put(out_ref, values, lane):
        for block in range(2 * pairs):
            rows = slice(block // 2 * shard, (block // 2 + 1) * shard)
            out_ref[block % 2, 0, rows, lane] = values[block * shard : (block + 1) * shard]

    values = product(left_t_ref[...], right_ref[0]).astype(BF)

    def fill(out_ref, other):
        put(out_ref, values, slice(0, units))
        if not extra:
            return
        for j in range(other, 4, 2):

            @pl.when((step % 2) ^ (meta_ref[0] // 2) == j // 2)
            def _(j=j):
                small = product_nt(refs[3][...], mixed_refs[j][...]).astype(BF)
                put(out_ref, small, slice(units, lanes))

        sums = jnp.concatenate(
            [sum_refs[0][...], sum_refs[1][...], jnp.zeros((16 - 10, width), F32)], axis=0
        ).astype(BF)
        for low in range(2):
            out_ref[low, 0, pairs * shard :, 0:width] = sums
            out_ref[low, 0, pairs * shard :, width:lanes] = jnp.zeros((16, lanes - width), BF)

    @pl.when(step < 2)
    def _():
        fill(keep_ref, 0)

    @pl.when(step >= 2)
    def _():
        fill(send_ref, 1)


def outer(meta, shard, left, rights, attn=None, mixed=(), sums=()):
    rows, width = left.shape
    groups, _, units = rights.shape
    extra = attn is not None
    feats = mixed[0].shape[0] if extra else 0
    depth = width // 2 + (16 if extra else 0)

    def owner(i, meta_ref):
        core = meta_ref[0] % 2
        return 2 * (i % 2) + jnp.where(i < 2, core, 1 - core)

    args = [left, rights] + ([attn, *mixed, *sums] if extra else [])
    block = (2, 1, depth, units + feats)
    grid_spec = pltpu.PrefetchScalarGridSpec(
        num_scalar_prefetch=1,
        grid=(4,),
        in_specs=[vmem(), pl.BlockSpec((1, rows, units), lambda i, m: (owner(i, m), 0, 0))]
        + [vmem()] * (len(args) - 2),
        out_specs=[
            pl.BlockSpec(block, lambda i, m: (0, jnp.minimum(i, 1), 0, 0)),
            pl.BlockSpec(block, lambda i, m: (0, jnp.maximum(i - 2, 0), 0, 0)),
        ],
        scratch_shapes=[pltpu.VMEM((width, rows), BF)] * (2 if extra else 1),
    )
    return pl.pallas_call(
        functools.partial(outer_body, shard, extra),
        grid_spec=grid_spec,
        out_shape=[spec(BF, 2, 2, depth, units + feats)] * 2,
        compiler_params=params(),
        cost_estimate=cost(8 * rows * width * units, 12 << 20),
        name="outer",
    )(meta, *args)


def inputs_body(*refs):
    dq_refs, (dk_ref, dv_ref, turned_ref) = refs[:4], refs[4:7]
    own_ref, next_ref, out_ref = refs[7:10]
    rows = dq_refs[0].shape[1]
    weight = turned_ref[...]
    for r in (1, 3, 0, 2):
        at = slice(r * rows, (r + 1) * rows)
        grad = jnp.concatenate([dq_refs[r][...], dk_ref[:, at], dv_ref[:, at]], axis=0)
        back = product(grad.T, weight)
        if r == 0:
            own_ref[...] = back
        elif r == 2:
            next_ref[...] = back
        else:
            out_ref[(r // 2) * rows : (r // 2 + 1) * rows, :] = back.astype(BF)


def input_grads(dq, dk, dv, turned):
    rows = dq[0].shape[1]
    width = turned.shape[1]
    return pl.pallas_call(
        inputs_body,
        in_specs=[vmem()] * 7,
        out_specs=[vmem()] * 3,
        out_shape=[spec(F32, rows, width), spec(F32, rows, width), spec(BF, 2 * rows, width)],
        compiler_params=params(),
        cost_estimate=cost(8 * rows * width * width, 12 << 20),
        name="input_grads",
    )(*dq, dk, dv, turned)


def projections_body(shard, *refs):
    meta_ref, dq_refs, (dk_ref, dv_ref, all_ref, keep_ref, send_ref) = refs[0], refs[1:5], refs[5:10]
    held_ref = refs[10]
    rows = dq_refs[0].shape[1]
    depth = keep_ref.shape[0] - 16
    grad = jnp.concatenate(
        [jnp.concatenate([ref[...] for ref in dq_refs], axis=1), dk_ref[...], dv_ref[...]], axis=0
    )
    held_ref[...] = product(grad, all_ref[...]).T.astype(BF)
    sums = product_nt(jnp.ones((16, 4 * rows), BF), grad).astype(BF)
    for flip, out_ref in ((0, keep_ref), (1, send_ref)):
        for i in range(depth // shard):
            block = 2 * i + (meta_ref[1] ^ flip)
            if shard % 16 == 0:
                start = pl.multiple_of(block * shard, shard)
                out_ref[i * shard : (i + 1) * shard, :] = held_ref[pl.ds(start, shard), :]
            else:
                even = held_ref[2 * i * shard : (2 * i + 1) * shard, :]
                odd = held_ref[(2 * i + 1) * shard : (2 * i + 2) * shard, :]
                out_ref[i * shard : (i + 1) * shard, :] = jnp.where(block % 2 == 0, even, odd)
        out_ref[depth:, :] = sums


def projection_grads(meta, shard, dq, dk, dv, tokens):
    width = tokens.shape[1]
    feats = dq[0].shape[0]
    return pl.pallas_call(
        functools.partial(projections_body, shard),
        in_specs=[smem()] + [vmem()] * 7,
        out_specs=[vmem()] * 2,
        out_shape=[spec(BF, width // 2 + 16, 3 * feats)] * 2,
        scratch_shapes=[pltpu.VMEM((width, 3 * feats), BF)],
        compiler_params=params(),
        cost_estimate=cost(2 * tokens.shape[0] * width * 3 * feats, 12 << 20),
        name="projection_grads",
    )(meta, *dq, dk, dv, tokens)


def exchanger(axis_dp, axis_tensor):
    def swap(values, dp_bits, tensor_bits):
        pairs = [
            (d * axis_tensor + t, (d ^ dp_bits) * axis_tensor + (t ^ tensor_bits))
            for d in range(axis_dp)
            for t in range(axis_tensor)
        ]
        return lax.ppermute(values, ("dp", "tensor"), pairs)

    return swap


def tie(*values):
    return lax.optimization_barrier(values)


def add(left, right):
    return (left.astype(F32) + right.astype(F32)).astype(BF)


def total(parts):
    return functools.reduce(jnp.add, [parts[i].astype(F32) for i in range(parts.shape[0])])


def local(
    axis_dp,
    axis_tensor,
    inputs,
    segments,
    query_weight,
    query_bias,
    key_weight,
    value_weight,
    value_bias,
    output_weight,
    output_bias,
    up_weight,
    up_bias,
    down_weight,
    down_bias,
    first_gain,
    first_shift,
    second_gain,
    second_shift,
    cotangent,
):
    swap = exchanger(axis_dp, axis_tensor)
    place_dp, place_tensor = lax.axis_index("dp"), lax.axis_index("tensor")
    meta = jnp.stack([place_tensor, place_dp % 2]).astype(jnp.int32)
    rows, width = inputs.shape[1:]
    shard = query_weight.shape[0]
    feats = output_weight.shape[0]
    heads = feats // HEAD
    units = up_weight.shape[1]
    pairs = axis_dp // 2
    row = lambda v: v.reshape(1, -1).astype(F32)
    flat = lambda z, x, y, c: (2 * z + x) * axis_tensor + 2 * y + c
    near_groups = [
        [flat(z, x, y, c) for x in range(2) for y in range(2)] for z in range(pairs) for c in range(2)
    ]
    deep_groups = [[2 * z + x for z in range(pairs)] for x in range(2)]

    own = inputs[0]
    notes = jnp.zeros((16, width), BF)
    notes = notes.at[0, :rows].set(segments[0].astype(BF)).at[1, :units].set(up_bias)
    message = jnp.concatenate([own, notes])
    across = swap(message, 0, 2)
    bundle = jnp.concatenate([query_weight, key_weight, value_weight], axis=1)
    copies = jnp.broadcast_to(bundle[None], (axis_dp,) + bundle.shape)
    qkv_weight = lax.all_to_all(copies, "dp", 0, 0, tiled=True).reshape(width, 3 * feats)
    near = swap(message, 0, 1)
    far = swap(across, 0, 1)
    tokens = [message, near, across, far]

    up_bundle = lax.all_gather(
        jnp.concatenate([up_weight, output_weight.T], axis=1), ("tensor", "dp"), axis=0, tiled=True
    ).reshape(axis_tensor, width, units + feats)
    downs = lax.all_gather(down_weight.T, ("tensor", "dp"), axis=0, tiled=True)
    downs = downs.reshape(axis_tensor, width, units)

    noted = jnp.stack([v[rows:] for v in tokens]).astype(F32)
    docs = noted[:, 0, :rows].reshape(-1)
    bias = noted[:, 1:2, :units]
    bias = jnp.stack([lax.dynamic_index_in_dim(bias, place_tensor ^ j, 0, False) for j in range(4)])
    lane = jnp.arange(HEAD, dtype=F32)
    same = docs[:, None] == lane[None, :]
    aux_query = (docs[None, :] == lane[:, None]).astype(BF)
    aux_key = jnp.where(same | (lane[None, :] >= 8), 0.0, -far_score).astype(BF)
    qkv_bias = jnp.concatenate([query_bias, jnp.zeros_like(query_bias), value_bias]).astype(F32)
    all_tokens, turned, queries, keys, values, values_t, keys_t = project(
        qkv_weight, tokens, rows, qkv_bias[feats:].reshape(1, -1), qkv_bias.reshape(-1, 1),
        aux_query, aux_key, heads,
    )

    mixed23, log23 = attend_forward(keys, queries, values_t, (2, 3))
    queries, mixed23 = tie(queries, mixed23)
    arrived = swap(mixed23, 0, 2)
    mixed1, log1 = attend_forward(keys, queries, values_t, (1,))
    queries, mixed1 = tie(queries, mixed1)
    arrived1 = swap(mixed1, 0, 1)
    mixed0, log0 = attend_forward(keys, queries, values_t, (0,))
    mixed = [mixed0[0], arrived1[0], arrived[0], swap(arrived[1], 0, 1)]

    low, unit_first, inverse_first, acts, slopes = enter(
        meta, up_bundle, units, mixed, own, row(output_bias), row(first_gain), row(first_shift), bias
    )
    layer_out, grad_second, second_low, sums_second = turn(
        acts, downs, unit_first, row(first_gain), row(first_shift),
        row(down_bias), row(second_gain), row(second_shift), cotangent[0],
    )
    keep_b, send_b = outer(meta, shard, second_low, acts)
    second_low, send_b = tie(second_low, send_b)
    moved_b = swap(send_b, 0, 1)
    inners, grad_hidden, grad_attn, grad0, next_mixed, far_mixed, sums_first = leave(
        meta, up_bundle, downs, slopes, second_low, grad_second, unit_first, inverse_first, row(first_gain)
    )

    def reduce_near(values):
        values = values.reshape((4,) + values.shape[2:])
        return lax.all_to_all(values, ("dp", "tensor"), 0, 0, axis_index_groups=near_groups, tiled=True)

    def reduce_deep(values):
        return lax.all_to_all(values, "dp", 0, 0, axis_index_groups=deep_groups, tiled=True)

    def deep_parts(values, extra):
        depth = values.shape[0] - extra
        parts = values[:depth].reshape(pairs, shard, -1)
        if not extra:
            return parts
        return jnp.stack([jnp.concatenate([parts[i], values[depth:]]) for i in range(pairs)])

    arrived_g = swap(far_mixed, 0, 2)
    g1 = swap(next_mixed, 0, 1)
    part_b = add(keep_b, moved_b)
    inners, part_b, arrived_g = tie(inners, part_b, arrived_g)
    near_b = reduce_near(part_b)
    g2, g3 = arrived_g[0], swap(arrived_g[1], 0, 1)
    keep_a, send_a = outer(
        meta, shard, low, inners, grad_attn, mixed, (sums_first, sums_second)
    )
    grad0, send_a, g1 = tie(grad0, send_a, g1)
    moved_a = swap(send_a, 0, 1)
    operands = (keys, queries, values, keys_t)
    (dq0, dq1), carried = attend_back(
        operands, (0, 1), ((log0, 0), (log1, 0)), ((mixed0, 0), (mixed1, 0)), (grad0, g1), None, False
    )
    part_a = add(keep_a, moved_a)
    sum_b = deep_parts(total(near_b).astype(BF), 0)
    carried, part_a, sum_b, g2, g3 = tie(carried, part_a, sum_b, g2, g3)
    near_a = reduce_near(part_a)
    deep_b = reduce_deep(sum_b)
    (dq2, dq3), (dk, dv) = attend_back(
        operands, (2, 3), ((log23, 0), (log23, 1)), ((mixed23, 0), (mixed23, 1)), (g2, g3), carried, True
    )
    dq = (dq0, dq1, dq2, dq3)
    own_rows, next_rows, sent_rows = input_grads(dq, dk, dv, turned)
    moved = swap(sent_rows, 0, 1)
    dk, sent_rows = tie(dk, sent_rows)
    keep_c, send_c = projection_grads(meta, shard, dq, dk, dv, all_tokens)
    next_rows = add(next_rows, moved[rows:])
    send_c, next_rows, near_a, deep_b = tie(send_c, next_rows, near_a, deep_b)
    arrived_c = swap(send_c, 1, 0)
    arrived_rows = swap(next_rows, 0, 2)
    sum_a = deep_parts(total(near_a).astype(BF), 16)
    deep_a = reduce_deep(sum_a)
    sum_c = deep_parts(add(keep_c, arrived_c), 16)
    deep_c = reduce_deep(sum_c)
    own_b, own_a, own_c = total(deep_b), total(deep_a), total(deep_c)
    grad_inputs = grad_hidden + own_rows + moved[:rows].astype(F32) + arrived_rows.astype(F32)
    sums = own_a[shard:, :width]
    sum_up = lax.dynamic_index_in_dim(sums[3:7], place_tensor, 0, False)
    head_sums = own_c[shard]

    return (
        layer_out[None],
        grad_inputs[None],
        own_c[:shard, :feats],
        head_sums[:feats],
        own_c[:shard, feats : 2 * feats],
        own_c[:shard, 2 * feats :],
        head_sums[2 * feats :],
        own_a[:shard, units:].T,
        sums[0],
        own_a[:shard, :units],
        sum_up,
        own_b.T,
        sums[7],
        sums[1],
        sums[2],
        sums[8],
        sums[9],
    )


def solution(mesh):
    axis_dp, axis_tensor = mesh.shape["dp"], mesh.shape["tensor"]
    if axis_tensor != 4 or axis_dp % 2:
        raise ValueError("mesh sizes")
    return jax.shard_map(
        functools.partial(local, axis_dp, axis_tensor),
        mesh=mesh,
        in_specs=(
            P("dp", "tensor", None),
            P("dp", "tensor"),
            P("dp", "tensor"),
            P("tensor"),
            P("dp", "tensor"),
            P("dp", "tensor"),
            P("tensor"),
            P("tensor", "dp"),
            P(),
            P("dp", "tensor"),
            P("tensor"),
            P("tensor", "dp"),
            P(),
            P(),
            P(),
            P(),
            P(),
            P("dp", "tensor", None),
        ),
        out_specs=(
            P("dp", "tensor", None),
            P("dp", "tensor", None),
            P("dp", "tensor"),
            P("tensor"),
            P("dp", "tensor"),
            P("dp", "tensor"),
            P("tensor"),
            P("tensor", "dp"),
            P(),
            P("dp", "tensor"),
            P("tensor"),
            P("tensor", "dp"),
            P(),
            P(),
            P(),
            P(),
            P(),
        ),
        check_vma=False,
    )
```

```python
import functools

import jax
import jax.numpy as jnp
from jax import lax
from jax.experimental import pallas as pl
from jax.experimental.pallas import tpu as pltpu
from jax.sharding import PartitionSpec as P

HEAD = 64
BF = jnp.bfloat16
F32 = jnp.float32

eps_norm = 1e-12
root_half = 0.7071067811865476
density = 0.3989422804014327
scale = 0.125
log2e = 1.4426950408889634
far_score = 1e30
vmem_bytes = 60 * 1024 * 1024


def product(left, right):
    return jnp.dot(left, right, preferred_element_type=F32)


def product_nt(left, right):
    return lax.dot_general(left, right, (((1,), (1,)), ((), ())), preferred_element_type=F32)


def product_tn(left, right):
    return lax.dot_general(left, right, (((0,), (0,)), ((), ())), preferred_element_type=F32)


def normalize(values, gain, offset):
    average = jnp.mean(values, axis=-1, keepdims=True)
    centred = values - average
    inverse = lax.rsqrt(jnp.mean(centred * centred, axis=-1, keepdims=True) + eps_norm)
    normed = centred * inverse
    return (normed * gain + offset, normed, inverse)


def norm_back(upstream, normed, inverse, gain):
    scaled = upstream * gain
    centred = scaled - jnp.mean(scaled, axis=-1, keepdims=True)
    return (centred - normed * jnp.mean(scaled * normed, axis=-1, keepdims=True)) * inverse


def fold(values):
    return functools.reduce(jnp.add, [values[i : i + 8] for i in range(0, values.shape[0], 8)])


def by_chunks(rows, width, count, chunk):
    def step(i, sums):
        at = pl.ds(pl.multiple_of(i * 32, 32), 32)
        return tuple(a + fold(b) for a, b in zip(sums, chunk(at)))

    sums = lax.fori_loop(0, rows // 32, step, (jnp.zeros((8, width), F32),) * count)
    return [jnp.sum(v, axis=0, keepdims=True) for v in sums]


def vmem():
    return pl.BlockSpec(memory_space=pltpu.VMEM)


def smem():
    return pl.BlockSpec(memory_space=pltpu.SMEM)


def params():
    return pltpu.CompilerParams(vmem_limit_bytes=vmem_bytes)


def cost(flops, moved, hard=0):
    return pl.CostEstimate(flops=int(flops), bytes_accessed=int(moved), transcendentals=int(hard))


def spec(dtype, *dims):
    return jax.ShapeDtypeStruct(dims, dtype)


def project_body(heads, *refs):
    token_refs, (weight_ref, row_bias_ref, column_bias_ref, aux_query_ref, aux_key_ref) = refs[:4], refs[4:9]
    all_ref, turned_ref, query_ref, key_ref, value_ref, value_t_ref, key_t_ref = refs[9:16]
    step = pl.program_id(0)
    width = heads * HEAD
    rows = all_ref.shape[0]

    @pl.when(step == 0)
    def _():
        turned_ref[...] = weight_ref[...].T

    for r, ref in enumerate(token_refs):

        @pl.when(step == r)
        def _(ref=ref):
            all_ref[...] = ref[:rows, :]

    tokens = all_ref[...]
    turned = (product_nt(turned_ref[...], tokens) + column_bias_ref[...]).astype(BF)
    plain = (product(tokens, weight_ref[:, width : 3 * width]) + row_bias_ref[...]).astype(BF)
    for h in range(heads):
        at = slice(h * HEAD, (h + 1) * HEAD)
        query_ref[h, :HEAD, :] = turned[at]
        query_ref[h, HEAD:, :] = aux_query_ref[...]
        key_t_ref[at, :] = turned[width : 2 * width][at]
        value_t_ref[at, :] = turned[2 * width :][at]
        key_ref[h] = jnp.concatenate([plain[:, at], aux_key_ref[...]], axis=1)
        value_ref[h] = plain[:, width + h * HEAD : width + (h + 1) * HEAD]


def project(weight, tokens, rows, row_bias, column_bias, aux_query, aux_key, heads):
    width = weight.shape[0]
    length = 4 * rows
    by_row = lambda n: pl.BlockSpec((rows, n), lambda r: (r, 0))
    headed = lambda n: pl.BlockSpec((heads, rows, n), lambda r: (0, r, 0))
    flat = pl.BlockSpec((heads * HEAD, rows), lambda r: (0, r))
    return pl.pallas_call(
        functools.partial(project_body, heads),
        grid=(4,),
        in_specs=[vmem()] * 7 + [pl.BlockSpec((HEAD, rows), lambda r: (0, r)), by_row(HEAD)],
        out_specs=[
            by_row(width),
            pl.BlockSpec((3 * heads * HEAD, width), lambda r: (0, 0)),
            pl.BlockSpec((heads, 2 * HEAD, rows), lambda r: (0, 0, r)),
            headed(2 * HEAD),
            headed(HEAD),
            flat,
            flat,
        ],
        out_shape=[
            spec(BF, length, width),
            spec(BF, 3 * heads * HEAD, width),
            spec(BF, heads, 2 * HEAD, length),
            spec(BF, heads, length, 2 * HEAD),
            spec(BF, heads, length, HEAD),
            spec(BF, heads * HEAD, length),
            spec(BF, heads * HEAD, length),
        ],
        compiler_params=params(),
        cost_estimate=cost(4 * length * width * 3 * heads * HEAD, 16 << 20),
        name="project",
    )(*tokens, weight, row_bias, column_bias, aux_query, aux_key)


def forward_body(count, key_ref, *refs):
    query_refs, value_ref, out_ref, log_ref = refs[:count], refs[count], refs[count + 1], refs[count + 2]
    chunk = key_ref.shape[1] // 4
    for i in range(count):
        query = query_refs[i][0]
        scores = [product(key_ref[0, c * chunk : (c + 1) * chunk, :], query) for c in range(4)]
        highest = None
        for c in range(4):
            peak = jnp.max(scores[c], axis=0, keepdims=True)
            now = peak if highest is None else jnp.maximum(highest, peak)
            raised = jnp.exp2((scores[c] - now) * (scale * log2e))
            part = jnp.sum(raised, axis=0, keepdims=True)
            mixed = product(value_ref[:, c * chunk : (c + 1) * chunk], raised.astype(BF))
            if highest is None:
                total, out = part, mixed
            else:
                shrink = jnp.exp2((highest - now) * (scale * log2e))
                total, out = total * shrink + part, out * shrink + mixed
            highest = now
        out_ref[i] = (out / total).astype(BF)
        log_ref[i, 0] = highest * (scale * log2e) + jnp.log2(total)


def attend_forward(keys, queries, values_t, quarters):
    heads, length, _ = keys.shape
    rows = length // 4
    count = len(quarters)
    return pl.pallas_call(
        functools.partial(forward_body, count),
        grid=(heads,),
        in_specs=[pl.BlockSpec((1, length, 2 * HEAD), lambda h: (h, 0, 0))]
        + [pl.BlockSpec((1, 2 * HEAD, rows), lambda h, q=q: (h, 0, q)) for q in quarters]
        + [pl.BlockSpec((HEAD, length), lambda h: (h, 0))],
        out_specs=[
            pl.BlockSpec((count, HEAD, rows), lambda h: (0, h, 0)),
            pl.BlockSpec((count, 1, 1, rows), lambda h: (0, h, 0, 0)),
        ],
        out_shape=[spec(BF, count, heads * HEAD, rows), spec(F32, count, heads, 1, rows)],
        compiler_params=params(),
        cost_estimate=cost(
            20 * count * heads * rows * length * HEAD, 4 << 20, heads * rows * length
        ),
        name="attend_forward",
    )(keys, *[queries] * count, values_t)


def backward_body(count, first, last, key_ref, value_ref, key_t_ref, *refs):
    groups, refs = [refs[4 * i : 4 * i + 4] for i in range(count)], refs[4 * count :]
    if not first:
        (old_dk_ref, old_dv_ref), refs = refs[:2], refs[2:]
    dq_refs, (dk_ref, dv_ref) = refs[:count], refs[count:]
    dk = dv = None
    for (query_ref, log_ref, mixed_ref, grad_ref), dq_ref in zip(groups, dq_refs):
        grad = grad_ref[...]
        delta = jnp.sum(grad.astype(F32) * mixed_ref[0].astype(F32), axis=0, keepdims=True)
        scores = product(key_ref[0], query_ref[0])
        weights = jnp.exp2(scores * (scale * log2e) - log_ref[0, 0])
        grad_weights = product(value_ref[0], grad)
        grad_scores = (weights * (grad_weights - delta)).astype(BF)
        dq_ref[...] = (product(key_t_ref[...], grad_scores) * scale).astype(BF)
        add_dk = product_nt(query_ref[0, :HEAD, :], grad_scores)
        add_dv = product_nt(grad, weights.astype(BF))
        dk = add_dk if dk is None else dk + add_dk
        dv = add_dv if dv is None else dv + add_dv
    if not first:
        dk = dk + old_dk_ref[...]
        dv = dv + old_dv_ref[...]
    if last:
        dk = dk * scale
    dk_ref[...] = dk.astype(dk_ref.dtype)
    dv_ref[...] = dv.astype(dv_ref.dtype)


def attend_back(operands, quarters, logs, mixed, grads, carried, last):
    keys, queries, values, keys_t = operands
    heads, length, _ = keys.shape
    rows = length // 4
    first = carried is None
    flat = lambda n: pl.BlockSpec((HEAD, n), lambda h: (h, 0))
    by_head = lambda *dims: pl.BlockSpec((1,) + dims, lambda h: (h, 0, 0))
    in_specs = [by_head(length, 2 * HEAD), by_head(length, HEAD), flat(length)]
    args = [keys, values, keys_t]
    for q, (log, i), (out, j), grad in zip(quarters, logs, mixed, grads):
        in_specs += [
            pl.BlockSpec((1, 2 * HEAD, rows), lambda h, q=q: (h, 0, q)),
            pl.BlockSpec((1, 1, 1, rows), lambda h, i=i: (i, h, 0, 0)),
            pl.BlockSpec((1, HEAD, rows), lambda h, j=j: (j, h, 0)),
            flat(rows),
        ]
        args += [queries, log, out, grad]
    count = len(quarters)
    aliases = {}
    if not first:
        if not last:
            aliases = {len(args): count, len(args) + 1: count + 1}
        in_specs += [flat(length)] * 2
        args += list(carried)
    kind = BF if last else F32
    outs = pl.pallas_call(
        functools.partial(backward_body, count, first, last),
        grid=(heads,),
        in_specs=in_specs,
        out_specs=[flat(rows)] * count + [flat(length)] * 2,
        out_shape=[spec(BF, heads * HEAD, rows)] * count + [spec(kind, heads * HEAD, length)] * 2,
        input_output_aliases=aliases,
        compiler_params=params(),
        cost_estimate=cost(
            50 * count * heads * rows * length * HEAD, 8 << 20, count * heads * rows * length
        ),
        name="attend_back",
    )(*args)
    return outs[:count], outs[count:]


def gelu_parts(inner):
    both = 0.5 * (1.0 + lax.erf(inner * root_half))
    slope = both + inner * density * jnp.exp(-0.5 * inner * inner)
    return (inner * both).astype(BF), slope.astype(BF)


def group_spec(rows, units):
    return pl.BlockSpec((1, rows, units), lambda t: (t, 0, 0))


def fixed(*dims):
    return pl.BlockSpec(dims, lambda t: (0,) * len(dims))


def out_copy(bundle_ref, out_ref, sem, units):
    feats = out_ref.shape[2]
    return pltpu.make_async_copy(bundle_ref.at[:, :, pl.ds(units, feats)], out_ref, sem)


def enter_body(units, meta_ref, bundle_ref, *refs):
    mixed_refs, (own_ref, out_bias_ref, gain_ref, shift_ref, up_ref, bias_ref) = refs[:4], refs[4:10]
    low_ref, unit_ref, inverse_ref, act_ref, slope_ref, out_ref, hidden_ref, sem = refs[10:]

    @pl.when(pl.program_id(0) == 0)
    def _():
        copy = out_copy(bundle_ref, out_ref, sem, units)
        copy.start()
        hidden = own_ref[...].astype(F32) + out_bias_ref[...]
        copy.wait()
        for j, ref in enumerate(mixed_refs):
            hidden = hidden + product_nt(ref[...].T, out_ref[meta_ref[0] ^ j])
        hidden_ref[...] = hidden

        def chunk(at):
            first, unit, inverse = normalize(hidden_ref[at, :], gain_ref[...], shift_ref[...])
            unit_ref[at, :] = unit
            inverse_ref[at, :] = inverse
            low_ref[at, :] = first.astype(BF)
            return ()

        by_chunks(hidden.shape[0], hidden.shape[1], 0, chunk)

    low = low_ref[...]
    step = units // 3
    for c in range(0, units, step):
        lanes = slice(c, c + step)
        inner = product(low, up_ref[0, :, lanes]) + bias_ref[0, :, lanes]
        act_ref[0, :, lanes], slope_ref[0, :, lanes] = gelu_parts(inner)


def enter(meta, bundle, units, mixed, own, out_bias, gain, shift, bias):
    rows, width = own.shape
    groups = bundle.shape[0]
    return pl.pallas_call(
        functools.partial(enter_body, units),
        grid=(groups,),
        in_specs=[smem(), pl.BlockSpec(memory_space=pl.ANY)]
        + [vmem()] * 8
        + [group_spec(width, units), group_spec(1, units)],
        out_specs=[fixed(rows, width), fixed(rows, width), fixed(rows, 1)]
        + [group_spec(rows, units)] * 2,
        out_shape=[spec(BF, rows, width), spec(F32, rows, width), spec(F32, rows, 1)]
        + [spec(BF, groups, rows, units)] * 2,
        scratch_shapes=[
            pltpu.VMEM((groups, width, bundle.shape[2] - units), BF),
            pltpu.VMEM((rows, width), F32),
            pltpu.SemaphoreType.DMA,
        ],
        compiler_params=params(),
        cost_estimate=cost(12 * rows * width * units, 20 << 20, 8 * rows * units),
        name="enter",
    )(meta, bundle, *mixed, own, out_bias, gain, shift, bundle, bias)


def turn_body(*refs):
    act_ref, down_ref, unit_ref, first_gain_ref, first_shift_ref = refs[:5]
    bias_ref, gain_ref, shift_ref, up_ref, out_ref, grad_ref, low_ref, sums_ref, total_ref = refs[5:]
    part = product_nt(act_ref[0], down_ref[0])
    step = pl.program_id(0)

    @pl.when(step == 0)
    def _():
        total_ref[...] = part

    @pl.when(step > 0)
    def _():
        total_ref[...] += part

    @pl.when(step == pl.num_programs(0) - 1)
    def _():
        def chunk(at):
            first = unit_ref[at, :] * first_gain_ref[...] + first_shift_ref[...]
            second, unit, inverse = normalize(
                first + total_ref[at, :] + bias_ref[...], gain_ref[...], shift_ref[...]
            )
            out_ref[at, :] = second.astype(BF)
            upstream = up_ref[at, :].astype(F32)
            grad = norm_back(upstream, unit, inverse, gain_ref[...])
            grad_ref[at, :] = grad
            low_ref[at, :] = grad.astype(BF)
            return grad, upstream * unit, upstream

        sums = by_chunks(total_ref.shape[0], total_ref.shape[1], 3, chunk)
        for k in range(3):
            sums_ref[k : k + 1, :] = sums[k]


def turn(acts, downs, unit, first_gain, first_shift, bias, gain, shift, cotangent):
    rows, width = unit.shape
    groups, _, units = acts.shape
    return pl.pallas_call(
        turn_body,
        grid=(groups,),
        in_specs=[group_spec(rows, units), group_spec(width, units)] + [vmem()] * 7,
        out_specs=[fixed(rows, width)] * 3 + [fixed(3, width)],
        out_shape=[
            spec(BF, rows, width),
            spec(F32, rows, width),
            spec(BF, rows, width),
            spec(F32, 3, width),
        ],
        scratch_shapes=[pltpu.VMEM((rows, width), F32)],
        compiler_params=params(),
        cost_estimate=cost(8 * rows * width * units, 16 << 20),
        name="turn",
    )(acts, downs, unit, first_gain, first_shift, bias, gain, shift, cotangent)


def leave_body(units, meta_ref, bundle_ref, *refs):
    up_ref, down_ref, slope_ref, low_ref, second_ref, unit_ref, inverse_ref, gain_ref = refs[:8]
    inner_ref, hidden_ref, attn_ref, own_ref, next_ref, far_ref, sums_ref, out_ref, sem = refs[8:]
    step = pl.program_id(0)

    @pl.when(step == 0)
    def _():
        out_copy(bundle_ref, out_ref, sem, units).start()
        hidden_ref[...] = second_ref[...]

    grad = product(low_ref[...], down_ref[0]) * slope_ref[0].astype(F32)
    inner = grad.astype(BF)
    inner_ref[0] = inner
    sums_ref[pl.ds(3 + step, 1), :] = jnp.sum(inner.astype(F32), axis=0, keepdims=True)
    hidden_ref[...] += product_nt(inner, up_ref[0])

    @pl.when(step == pl.num_programs(0) - 1)
    def _():
        out_copy(bundle_ref, out_ref, sem, units).wait()

        def chunk(at):
            back = hidden_ref[at, :]
            unit = unit_ref[at, :]
            hidden = norm_back(back, unit, inverse_ref[at, :], gain_ref[...])
            hidden_ref[at, :] = hidden
            attn_ref[at, :] = hidden.astype(BF)
            return hidden, back * unit, back

        sums = by_chunks(hidden_ref.shape[0], hidden_ref.shape[1], 3, chunk)
        for k in range(3):
            sums_ref[k : k + 1, :] = sums[k]
        attn = attn_ref[...]
        for j in range(4):
            mixed = product(attn, out_ref[meta_ref[0] ^ j]).T.astype(BF)
            if j == 0:
                own_ref[...] = mixed
            elif j == 1:
                next_ref[...] = mixed
            else:
                far_ref[j - 2] = mixed


def leave(meta, bundle, downs, slopes, low, second, unit, inverse, gain):
    rows, width = low.shape
    groups, _, units = downs.shape
    feats = bundle.shape[2] - units
    return pl.pallas_call(
        functools.partial(leave_body, units),
        grid=(groups,),
        in_specs=[smem(), pl.BlockSpec(memory_space=pl.ANY)]
        + [group_spec(width, units), group_spec(width, units), group_spec(rows, units)]
        + [vmem()] * 5,
        out_specs=[
            group_spec(rows, units),
            fixed(rows, width),
            fixed(rows, width),
            fixed(feats, rows),
            fixed(feats, rows),
            fixed(2, feats, rows),
            fixed(3 + groups, width),
        ],
        out_shape=[
            spec(BF, groups, rows, units),
            spec(F32, rows, width),
            spec(BF, rows, width),
            spec(BF, feats, rows),
            spec(BF, feats, rows),
            spec(BF, 2, feats, rows),
            spec(F32, 3 + groups, width),
        ],
        scratch_shapes=[pltpu.VMEM((groups, width, feats), BF), pltpu.SemaphoreType.DMA],
        compiler_params=params(),
        cost_estimate=cost(16 * rows * width * units, 28 << 20),
        name="leave",
    )(meta, bundle, bundle, downs, slopes, low, second, unit, inverse, gain)


def outer_body(shard, extra, keep, meta_ref, left_ref, right_ref, *refs):
    if extra:
        attn_ref, mixed_refs, sum_refs, refs = refs[0], refs[1:3], refs[3:5], refs[5:]
    if keep:
        arrived_ref, refs = refs[0], refs[1:]
        left_t_ref, attn_t_ref = left_ref, attn_ref if extra else None
    else:
        left_t_ref, attn_t_ref = refs[1], refs[2] if extra else None
    out_ref = refs[0]
    step = pl.program_id(0)
    units = right_ref.shape[2]
    width = left_t_ref.shape[0]
    pairs = width // shard // 2
    lanes = out_ref.shape[3]

    if not keep:

        @pl.when(step == 0)
        def _():
            left_t_ref[...] = left_ref[...].T
            if extra:
                attn_t_ref[...] = attn_ref[...].T

    def put(low, rows, lane, values):
        if keep:
            values = values + arrived_ref[low, 0, rows, lane].astype(F32)
        out_ref[low, 0, rows, lane] = values.astype(BF)

    def spread(values, lane):
        for block in range(2 * pairs):
            rows = slice(block // 2 * shard, (block // 2 + 1) * shard)
            put(block % 2, rows, lane, values[block * shard : (block + 1) * shard])

    spread(product(left_t_ref[...], right_ref[0]), slice(0, units))
    if extra:
        for j in range(2):

            @pl.when(step ^ (meta_ref[0] // 2) == j)
            def _(j=j):
                spread(product_nt(attn_t_ref[...], mixed_refs[j][...]), slice(units, lanes))

        sums = jnp.concatenate(
            [sum_refs[0][...], sum_refs[1][...], jnp.zeros((16 - 10, width), F32)], axis=0
        )
        for low in range(2):
            put(low, slice(pairs * shard, pairs * shard + 16), slice(0, width), sums)
            out_ref[low, 0, pairs * shard :, width:lanes] = jnp.zeros((16, lanes - width), BF)


def outer(meta, shard, left, rights, attn=None, mixed=(), sums=(), arrived=None):
    keep = arrived is not None
    rows, width = left.shape[::-1] if keep else left.shape
    groups, _, units = rights.shape
    extra = attn is not None
    feats = mixed[0].shape[0] if extra else 0
    depth = width // 2 + (16 if extra else 0)

    def owner(i, meta_ref):
        core = meta_ref[0] % 2
        return 2 * i + (core if keep else 1 - core)

    args = [left, rights] + ([attn, *mixed, *sums] if extra else [])
    block = pl.BlockSpec((2, 1, depth, units + feats), lambda i, m: (0, i, 0, 0))
    turned = [] if keep else [left, attn] if extra else [left]
    grid_spec = pltpu.PrefetchScalarGridSpec(
        num_scalar_prefetch=1,
        grid=(2,),
        in_specs=[vmem(), pl.BlockSpec((1, rows, units), lambda i, m: (owner(i, m), 0, 0))]
        + [vmem()] * (len(args) - 2)
        + ([block] if keep else []),
        out_specs=[block] + [vmem()] * len(turned),
    )
    return pl.pallas_call(
        functools.partial(outer_body, shard, extra, keep),
        grid_spec=grid_spec,
        out_shape=[spec(BF, 2, 2, depth, units + feats)] + [spec(BF, width, rows) for _ in turned],
        compiler_params=params(),
        cost_estimate=cost(4 * rows * width * units, 8 << 20),
        name="outer",
    )(meta, *args, *([arrived] if keep else []))


def inputs_body(*refs):
    dq_refs, (dk_ref, dv_ref, turned_ref) = refs[:4], refs[4:7]
    own_ref, next_ref, out_ref = refs[7:10]
    rows = dq_refs[0].shape[1]
    weight = turned_ref[...]
    for r in (1, 3, 0, 2):
        at = slice(r * rows, (r + 1) * rows)
        grad = jnp.concatenate([dq_refs[r][...], dk_ref[:, at], dv_ref[:, at]], axis=0)
        back = product(grad.T, weight)
        if r == 0:
            own_ref[...] = back
        elif r == 2:
            next_ref[...] = back
        else:
            out_ref[(r // 2) * rows : (r // 2 + 1) * rows, :] = back.astype(BF)


def input_grads(dq, dk, dv, turned):
    rows = dq[0].shape[1]
    width = turned.shape[1]
    return pl.pallas_call(
        inputs_body,
        in_specs=[vmem()] * 7,
        out_specs=[vmem()] * 3,
        out_shape=[spec(F32, rows, width), spec(F32, rows, width), spec(BF, 2 * rows, width)],
        compiler_params=params(),
        cost_estimate=cost(8 * rows * width * width, 12 << 20),
        name="input_grads",
    )(*dq, dk, dv, turned)


def projections_body(shard, *refs):
    meta_ref, dq_refs, (dk_ref, dv_ref, all_ref, keep_ref, send_ref) = refs[0], refs[1:5], refs[5:10]
    held_ref = refs[10]
    rows = dq_refs[0].shape[1]
    depth = keep_ref.shape[0] - 16
    grad = jnp.concatenate(
        [jnp.concatenate([ref[...] for ref in dq_refs], axis=1), dk_ref[...], dv_ref[...]], axis=0
    )
    held_ref[...] = product(grad, all_ref[...]).T.astype(BF)
    sums = product_nt(jnp.ones((16, 4 * rows), BF), grad).astype(BF)
    for flip, out_ref in ((0, keep_ref), (1, send_ref)):
        for i in range(depth // shard):
            block = 2 * i + (meta_ref[1] ^ flip)
            if shard % 16 == 0:
                start = pl.multiple_of(block * shard, shard)
                out_ref[i * shard : (i + 1) * shard, :] = held_ref[pl.ds(start, shard), :]
            else:
                even = held_ref[2 * i * shard : (2 * i + 1) * shard, :]
                odd = held_ref[(2 * i + 1) * shard : (2 * i + 2) * shard, :]
                out_ref[i * shard : (i + 1) * shard, :] = jnp.where(block % 2 == 0, even, odd)
        out_ref[depth:, :] = sums


def projection_grads(meta, shard, dq, dk, dv, tokens):
    width = tokens.shape[1]
    feats = dq[0].shape[0]
    return pl.pallas_call(
        functools.partial(projections_body, shard),
        in_specs=[smem()] + [vmem()] * 7,
        out_specs=[vmem()] * 2,
        out_shape=[spec(BF, width // 2 + 16, 3 * feats)] * 2,
        scratch_shapes=[pltpu.VMEM((width, 3 * feats), BF)],
        compiler_params=params(),
        cost_estimate=cost(2 * tokens.shape[0] * width * 3 * feats, 12 << 20),
        name="projection_grads",
    )(meta, *dq, dk, dv, tokens)


def exchanger(axis_dp, axis_tensor):
    def swap(values, dp_bits, tensor_bits):
        pairs = [
            (d * axis_tensor + t, (d ^ dp_bits) * axis_tensor + (t ^ tensor_bits))
            for d in range(axis_dp)
            for t in range(axis_tensor)
        ]
        return lax.ppermute(values, ("dp", "tensor"), pairs)

    return swap


def tie(*values):
    return lax.optimization_barrier(values)


def add(left, right):
    return (left.astype(F32) + right.astype(F32)).astype(BF)


def total(parts):
    return functools.reduce(jnp.add, [parts[i].astype(F32) for i in range(parts.shape[0])])


def local(
    axis_dp,
    axis_tensor,
    inputs,
    segments,
    query_weight,
    query_bias,
    key_weight,
    value_weight,
    value_bias,
    output_weight,
    output_bias,
    up_weight,
    up_bias,
    down_weight,
    down_bias,
    first_gain,
    first_shift,
    second_gain,
    second_shift,
    cotangent,
):
    swap = exchanger(axis_dp, axis_tensor)
    place_dp, place_tensor = lax.axis_index("dp"), lax.axis_index("tensor")
    meta = jnp.stack([place_tensor, place_dp % 2]).astype(jnp.int32)
    rows, width = inputs.shape[1:]
    shard = query_weight.shape[0]
    feats = output_weight.shape[0]
    heads = feats // HEAD
    units = up_weight.shape[1]
    pairs = axis_dp // 2
    row = lambda v: v.reshape(1, -1).astype(F32)
    flat = lambda z, x, y, c: (2 * z + x) * axis_tensor + 2 * y + c
    near_groups = [
        [flat(z, x, y, c) for x in range(2) for y in range(2)] for z in range(pairs) for c in range(2)
    ]
    deep_groups = [[2 * z + x for z in range(pairs)] for x in range(2)]

    own = inputs[0]
    notes = jnp.zeros((16, width), BF)
    notes = notes.at[0, :rows].set(segments[0].astype(BF)).at[1, :units].set(up_bias)
    message = jnp.concatenate([own, notes])
    across = swap(message, 0, 2)
    bundle = jnp.concatenate([query_weight, key_weight, value_weight], axis=1)
    copies = jnp.broadcast_to(bundle[None], (axis_dp,) + bundle.shape)
    qkv_weight = lax.all_to_all(copies, "dp", 0, 0, tiled=True).reshape(width, 3 * feats)
    near = swap(message, 0, 1)
    far = swap(across, 0, 1)
    tokens = [message, near, across, far]

    up_bundle = lax.all_gather(
        jnp.concatenate([up_weight, output_weight.T], axis=1), ("tensor", "dp"), axis=0, tiled=True
    ).reshape(axis_tensor, width, units + feats)
    downs = lax.all_gather(down_weight.T, ("tensor", "dp"), axis=0, tiled=True)
    downs = downs.reshape(axis_tensor, width, units)

    noted = jnp.stack([v[rows:] for v in tokens]).astype(F32)
    docs = noted[:, 0, :rows].reshape(-1)
    bias = noted[:, 1:2, :units]
    bias = jnp.stack([lax.dynamic_index_in_dim(bias, place_tensor ^ j, 0, False) for j in range(4)])
    lane = jnp.arange(HEAD, dtype=F32)
    same = docs[:, None] == lane[None, :]
    aux_query = (docs[None, :] == lane[:, None]).astype(BF)
    aux_key = jnp.where(same | (lane[None, :] >= 8), 0.0, -far_score).astype(BF)
    qkv_bias = jnp.concatenate([query_bias, jnp.zeros_like(query_bias), value_bias]).astype(F32)
    all_tokens, turned, queries, keys, values, values_t, keys_t = project(
        qkv_weight, tokens, rows, qkv_bias[feats:].reshape(1, -1), qkv_bias.reshape(-1, 1),
        aux_query, aux_key, heads,
    )

    mixed23, log23 = attend_forward(keys, queries, values_t, (2, 3))
    queries, mixed23 = tie(queries, mixed23)
    arrived = swap(mixed23, 0, 2)
    mixed1, log1 = attend_forward(keys, queries, values_t, (1,))
    queries, mixed1 = tie(queries, mixed1)
    arrived1 = swap(mixed1, 0, 1)
    mixed0, log0 = attend_forward(keys, queries, values_t, (0,))
    mixed = [mixed0[0], arrived1[0], arrived[0], swap(arrived[1], 0, 1)]

    low, unit_first, inverse_first, acts, slopes = enter(
        meta, up_bundle, units, mixed, own, row(output_bias), row(first_gain), row(first_shift), bias
    )
    layer_out, grad_second, second_low, sums_second = turn(
        acts, downs, unit_first, row(first_gain), row(first_shift),
        row(down_bias), row(second_gain), row(second_shift), cotangent[0],
    )
    send_b, second_t = outer(meta, shard, second_low, acts)
    second_low, send_b = tie(second_low, send_b)
    moved_b = swap(send_b, 0, 1)
    inners, grad_hidden, grad_attn, grad0, next_mixed, far_mixed, sums_first = leave(
        meta, up_bundle, downs, slopes, second_low, grad_second, unit_first, inverse_first, row(first_gain)
    )

    def reduce_near(values):
        values = values.reshape((4,) + values.shape[2:])
        return lax.all_to_all(values, ("dp", "tensor"), 0, 0, axis_index_groups=near_groups, tiled=True)

    def reduce_deep(values):
        return lax.all_to_all(values, "dp", 0, 0, axis_index_groups=deep_groups, tiled=True)

    def deep_parts(values):
        return values[: pairs * shard].reshape(pairs, shard, -1)

    arrived_g = swap(far_mixed, 0, 2)
    g1 = swap(next_mixed, 0, 1)
    (part_b,) = outer(meta, shard, second_t, acts, arrived=moved_b)
    inners, part_b = tie(inners, part_b)
    near_b = reduce_near(part_b)
    sums_both = (sums_first, sums_second)
    send_a, low_t, attn_t = outer(meta, shard, low, inners, grad_attn, mixed[1::2], sums_both)
    grad0, send_a, g1, arrived_g = tie(grad0, send_a, g1, arrived_g)
    moved_a = swap(send_a, 0, 1)
    g2, g3 = arrived_g[0], swap(arrived_g[1], 0, 1)
    operands = (keys, queries, values, keys_t)
    (dq0, dq1), carried = attend_back(
        operands, (0, 1), ((log0, 0), (log1, 0)), ((mixed0, 0), (mixed1, 0)), (grad0, g1), None, False
    )
    low_t, carried, moved_a = tie(low_t, carried, moved_a)
    (part_a,) = outer(meta, shard, low_t, inners, attn_t, mixed[::2], sums_both, moved_a)
    carried, part_a, near_b, g2, g3 = tie(carried, part_a, near_b, g2, g3)
    near_a = reduce_near(part_a)
    (dq2, dq3), (dk, dv) = attend_back(
        operands, (2, 3), ((log23, 0), (log23, 1)), ((mixed23, 0), (mixed23, 1)), (g2, g3), carried, True
    )
    dq = (dq0, dq1, dq2, dq3)
    own_rows, next_rows, sent_rows = input_grads(dq, dk, dv, turned)
    moved = swap(sent_rows, 0, 1)
    dk, sent_rows = tie(dk, sent_rows)
    keep_c, send_c = projection_grads(meta, shard, dq, dk, dv, all_tokens)
    next_rows = add(next_rows, moved[rows:])
    send_c, next_rows = tie(send_c, next_rows)
    arrived_c = swap(send_c, 1, 0)
    arrived_rows = swap(next_rows, 0, 2)
    sum_a, sum_b = total(near_a).astype(BF), total(near_b).astype(BF)
    notes = jnp.broadcast_to(sum_a[None, pairs * shard :], (pairs, 16, sum_a.shape[1]))
    sum_ab = jnp.concatenate([deep_parts(sum_a), deep_parts(sum_b)], axis=2)
    notes = jnp.pad(notes, ((0, 0), (0, 0), (0, sum_b.shape[1])))
    deep_ab = reduce_deep(jnp.concatenate([sum_ab, notes], axis=1))
    sum_c = add(keep_c, arrived_c)
    parts_c = sum_c[: pairs * shard].reshape(pairs, shard, -1)
    own_c = lax.dynamic_index_in_dim(parts_c, place_dp // 2, 0, False).astype(F32)
    own_c = jnp.concatenate([own_c, sum_c[pairs * shard :].astype(F32)])
    for k in range(1, pairs):
        part = lax.dynamic_index_in_dim(parts_c, (place_dp // 2) ^ k, 0, False)
        own_c = own_c + swap(jnp.concatenate([part, sum_c[pairs * shard :]]), 2 * k, 0).astype(F32)
    own_ab = total(deep_ab)
    own_a, own_b = own_ab[:, : sum_a.shape[1]], own_ab[:shard, sum_a.shape[1] :]
    grad_inputs = grad_hidden + own_rows + moved[:rows].astype(F32) + arrived_rows.astype(F32)
    sums = own_a[shard:, :width]
    sum_up = lax.dynamic_index_in_dim(sums[3:7], place_tensor, 0, False)
    head_sums = own_c[shard]

    return (
        layer_out[None],
        grad_inputs[None],
        own_c[:shard, :feats],
        head_sums[:feats],
        own_c[:shard, feats : 2 * feats],
        own_c[:shard, 2 * feats :],
        head_sums[2 * feats :],
        own_a[:shard, units:].T,
        sums[0],
        own_a[:shard, :units],
        sum_up,
        own_b.T,
        sums[7],
        sums[1],
        sums[2],
        sums[8],
        sums[9],
    )


def solution(mesh):
    axis_dp, axis_tensor = mesh.shape["dp"], mesh.shape["tensor"]
    if axis_tensor != 4 or axis_dp < 2 or axis_dp & (axis_dp - 1):
        raise ValueError("mesh sizes")
    return jax.shard_map(
        functools.partial(local, axis_dp, axis_tensor),
        mesh=mesh,
        in_specs=(
            P("dp", "tensor", None),
            P("dp", "tensor"),
            P("dp", "tensor"),
            P("tensor"),
            P("dp", "tensor"),
            P("dp", "tensor"),
            P("tensor"),
            P("tensor", "dp"),
            P(),
            P("dp", "tensor"),
            P("tensor"),
            P("tensor", "dp"),
            P(),
            P(),
            P(),
            P(),
            P(),
            P("dp", "tensor", None),
        ),
        out_specs=(
            P("dp", "tensor", None),
            P("dp", "tensor", None),
            P("dp", "tensor"),
            P("tensor"),
            P("dp", "tensor"),
            P("dp", "tensor"),
            P("tensor"),
            P("tensor", "dp"),
            P(),
            P("dp", "tensor"),
            P("tensor"),
            P("tensor", "dp"),
            P(),
            P(),
            P(),
            P(),
            P(),
        ),
        check_vma=False,
    )
```

```python
import functools

import jax
import jax.numpy as jnp
from jax import lax
from jax.experimental import pallas as pl
from jax.experimental.pallas import tpu as pltpu
from jax.sharding import PartitionSpec as P

HEAD = 64
BF = jnp.bfloat16
F32 = jnp.float32

eps_norm = 1e-12
root_half = 0.7071067811865476
density = 0.3989422804014327
scale = 0.125
log2e = 1.4426950408889634
far_score = 1e30
vmem_bytes = 60 * 1024 * 1024


def product(left, right):
    return jnp.dot(left, right, preferred_element_type=F32)


def product_nt(left, right):
    return lax.dot_general(left, right, (((1,), (1,)), ((), ())), preferred_element_type=F32)


def product_tn(left, right):
    return lax.dot_general(left, right, (((0,), (0,)), ((), ())), preferred_element_type=F32)


def normalize(values, gain, offset):
    average = jnp.mean(values, axis=-1, keepdims=True)
    centred = values - average
    inverse = lax.rsqrt(jnp.mean(centred * centred, axis=-1, keepdims=True) + eps_norm)
    normed = centred * inverse
    return (normed * gain + offset, normed, inverse)


def norm_back(upstream, normed, inverse, gain):
    scaled = upstream * gain
    centred = scaled - jnp.mean(scaled, axis=-1, keepdims=True)
    return (centred - normed * jnp.mean(scaled * normed, axis=-1, keepdims=True)) * inverse


def fold(values):
    return functools.reduce(jnp.add, [values[i : i + 8] for i in range(0, values.shape[0], 8)])


def by_chunks(rows, width, size, chunk):
    def step(i, sums):
        at = pl.ds(pl.multiple_of(i * size, size), size)
        return tuple(a + fold(b) for a, b in zip(sums, chunk(at)))

    sums = lax.fori_loop(0, rows // size, step, (jnp.zeros((8, width), F32),) * 3)
    return [jnp.sum(v, axis=0, keepdims=True) for v in sums]


def vmem():
    return pl.BlockSpec(memory_space=pltpu.VMEM)


def smem():
    return pl.BlockSpec(memory_space=pltpu.SMEM)


def params():
    return pltpu.CompilerParams(vmem_limit_bytes=vmem_bytes)


def cost(flops, moved, hard=0):
    return pl.CostEstimate(flops=int(flops), bytes_accessed=int(moved), transcendentals=int(hard))


def spec(dtype, *dims):
    return jax.ShapeDtypeStruct(dims, dtype)


def project_body(heads, *refs):
    token_refs, (weight_ref, row_bias_ref, column_bias_ref, aux_query_ref, aux_key_ref) = refs[:4], refs[4:9]
    all_ref, turned_ref, query_ref, key_ref, value_ref, value_t_ref, key_t_ref = refs[9:16]
    step = pl.program_id(0)
    width = heads * HEAD
    rows = all_ref.shape[0]

    @pl.when(step == 0)
    def _():
        turned_ref[...] = weight_ref[...].T

    for r, ref in enumerate(token_refs):

        @pl.when(step == r)
        def _(ref=ref):
            all_ref[...] = ref[:rows, :]

    tokens = all_ref[...]
    turned = (product_nt(turned_ref[...], tokens) + column_bias_ref[...]).astype(BF)
    plain = (product(tokens, weight_ref[:, width : 3 * width]) + row_bias_ref[...]).astype(BF)
    for h in range(heads):
        at = slice(h * HEAD, (h + 1) * HEAD)
        query_ref[h, :HEAD, :] = turned[at]
        query_ref[h, HEAD:, :] = aux_query_ref[...]
        key_t_ref[at, :] = turned[width : 2 * width][at]
        value_t_ref[at, :] = turned[2 * width :][at]
        key_ref[h] = jnp.concatenate([plain[:, at], aux_key_ref[...]], axis=1)
        value_ref[h] = plain[:, width + h * HEAD : width + (h + 1) * HEAD]


def project(weight, tokens, rows, row_bias, column_bias, aux_query, aux_key, heads):
    width = weight.shape[0]
    length = 4 * rows
    by_row = lambda n: pl.BlockSpec((rows, n), lambda r: (r, 0))
    headed = lambda n: pl.BlockSpec((heads, rows, n), lambda r: (0, r, 0))
    flat = pl.BlockSpec((heads * HEAD, rows), lambda r: (0, r))
    return pl.pallas_call(
        functools.partial(project_body, heads),
        grid=(4,),
        in_specs=[vmem()] * 7 + [pl.BlockSpec((HEAD, rows), lambda r: (0, r)), by_row(HEAD)],
        out_specs=[
            by_row(width),
            pl.BlockSpec((3 * heads * HEAD, width), lambda r: (0, 0)),
            pl.BlockSpec((heads, 2 * HEAD, rows), lambda r: (0, 0, r)),
            headed(2 * HEAD),
            headed(HEAD),
            flat,
            flat,
        ],
        out_shape=[
            spec(BF, length, width),
            spec(BF, 3 * heads * HEAD, width),
            spec(BF, heads, 2 * HEAD, length),
            spec(BF, heads, length, 2 * HEAD),
            spec(BF, heads, length, HEAD),
            spec(BF, heads * HEAD, length),
            spec(BF, heads * HEAD, length),
        ],
        compiler_params=params(),
        cost_estimate=cost(4 * length * width * 3 * heads * HEAD, 16 << 20),
        name="project",
    )(*tokens, weight, row_bias, column_bias, aux_query, aux_key)


def forward_body(count, key_ref, *refs):
    query_refs, value_ref, out_ref, log_ref = refs[:count], refs[count], refs[count + 1], refs[count + 2]
    chunk = key_ref.shape[1] // 4
    for i in range(count):
        query = query_refs[i][0]
        scores = [product(key_ref[0, c * chunk : (c + 1) * chunk, :], query) for c in range(4)]
        highest = None
        for c in range(4):
            peak = jnp.max(scores[c], axis=0, keepdims=True)
            now = peak if highest is None else jnp.maximum(highest, peak)
            raised = jnp.exp2((scores[c] - now) * (scale * log2e))
            part = jnp.sum(raised, axis=0, keepdims=True)
            mixed = product(value_ref[:, c * chunk : (c + 1) * chunk], raised.astype(BF))
            if highest is None:
                total, out = part, mixed
            else:
                shrink = jnp.exp2((highest - now) * (scale * log2e))
                total, out = total * shrink + part, out * shrink + mixed
            highest = now
        out_ref[i] = (out / total).astype(BF)
        log_ref[i, 0] = highest * (scale * log2e) + jnp.log2(total)


def attend_forward(keys, queries, values_t, quarters):
    heads, length, _ = keys.shape
    rows = length // 4
    count = len(quarters)
    return pl.pallas_call(
        functools.partial(forward_body, count),
        grid=(heads,),
        in_specs=[pl.BlockSpec((1, length, 2 * HEAD), lambda h: (h, 0, 0))]
        + [pl.BlockSpec((1, 2 * HEAD, rows), lambda h, q=q: (h, 0, q)) for q in quarters]
        + [pl.BlockSpec((HEAD, length), lambda h: (h, 0))],
        out_specs=[
            pl.BlockSpec((count, HEAD, rows), lambda h: (0, h, 0)),
            pl.BlockSpec((count, 1, 1, rows), lambda h: (0, h, 0, 0)),
        ],
        out_shape=[spec(BF, count, heads * HEAD, rows), spec(F32, count, heads, 1, rows)],
        compiler_params=params(),
        cost_estimate=cost(
            20 * count * heads * rows * length * HEAD, 4 << 20, heads * rows * length
        ),
        name="attend_forward",
    )(keys, *[queries] * count, values_t)


def backward_body(count, first, last, key_ref, value_ref, key_t_ref, *refs):
    groups, refs = [refs[4 * i : 4 * i + 4] for i in range(count)], refs[4 * count :]
    if not first:
        (old_dk_ref, old_dv_ref), refs = refs[:2], refs[2:]
    dq_refs, (dk_ref, dv_ref) = refs[:count], refs[count:]
    dk = dv = None
    for (query_ref, log_ref, mixed_ref, grad_ref), dq_ref in zip(groups, dq_refs):
        grad = grad_ref[...]
        delta = jnp.sum(grad.astype(F32) * mixed_ref[0].astype(F32), axis=0, keepdims=True)
        scores = product(key_ref[0], query_ref[0])
        weights = jnp.exp2(scores * (scale * log2e) - log_ref[0, 0])
        grad_weights = product(value_ref[0], grad)
        grad_scores = (weights * (grad_weights - delta)).astype(BF)
        dq_ref[...] = (product(key_t_ref[...], grad_scores) * scale).astype(BF)
        add_dk = product_nt(query_ref[0, :HEAD, :], grad_scores)
        add_dv = product_nt(grad, weights.astype(BF))
        dk = add_dk if dk is None else dk + add_dk
        dv = add_dv if dv is None else dv + add_dv
    if not first:
        dk = dk + old_dk_ref[...]
        dv = dv + old_dv_ref[...]
    if last:
        dk = dk * scale
    dk_ref[...] = dk.astype(dk_ref.dtype)
    dv_ref[...] = dv.astype(dv_ref.dtype)


def attend_back(operands, quarters, logs, mixed, grads, carried, last):
    keys, queries, values, keys_t = operands
    heads, length, _ = keys.shape
    rows = length // 4
    first = carried is None
    flat = lambda n: pl.BlockSpec((HEAD, n), lambda h: (h, 0))
    by_head = lambda *dims: pl.BlockSpec((1,) + dims, lambda h: (h, 0, 0))
    in_specs = [by_head(length, 2 * HEAD), by_head(length, HEAD), flat(length)]
    args = [keys, values, keys_t]
    for q, (log, i), (out, j), grad in zip(quarters, logs, mixed, grads):
        in_specs += [
            pl.BlockSpec((1, 2 * HEAD, rows), lambda h, q=q: (h, 0, q)),
            pl.BlockSpec((1, 1, 1, rows), lambda h, i=i: (i, h, 0, 0)),
            pl.BlockSpec((1, HEAD, rows), lambda h, j=j: (j, h, 0)),
            flat(rows),
        ]
        args += [queries, log, out, grad]
    count = len(quarters)
    aliases = {}
    if not first:
        if not last:
            aliases = {len(args): count, len(args) + 1: count + 1}
        in_specs += [flat(length)] * 2
        args += list(carried)
    kind = BF if last else F32
    outs = pl.pallas_call(
        functools.partial(backward_body, count, first, last),
        grid=(heads,),
        in_specs=in_specs,
        out_specs=[flat(rows)] * count + [flat(length)] * 2,
        out_shape=[spec(BF, heads * HEAD, rows)] * count + [spec(kind, heads * HEAD, length)] * 2,
        input_output_aliases=aliases,
        compiler_params=params(),
        cost_estimate=cost(
            50 * count * heads * rows * length * HEAD, 8 << 20, count * heads * rows * length
        ),
        name="attend_back",
    )(*args)
    return outs[:count], outs[count:]


def group_place(meta_ref, j):
    return 2 * (j % 2) + ((meta_ref[0] // 2) ^ (j // 2))


def group_owner(meta_ref, group):
    return 2 * (group % 2) + ((meta_ref[0] % 2) ^ (group // 2))


def group_copies(near_ref, far_ref, held_ref, sems, start):
    lanes = pl.ds(start, held_ref.shape[2])
    return [
        pltpu.make_async_copy(ref.at[g % 2, :, lanes], held_ref.at[g], sems.at[g])
        for g, ref in enumerate((near_ref, near_ref, far_ref, far_ref))
    ]


def group_wait(near_ref, held_ref, sems, start, group):
    lanes = pl.ds(start, held_ref.shape[2])
    pltpu.make_async_copy(near_ref.at[0, :, lanes], held_ref.at[group], sems.at[group]).wait()


def held(width, lanes):
    return [pltpu.VMEM((4, width, lanes), BF), pltpu.SemaphoreType.DMA((4,))]


def unmoved():
    return pl.BlockSpec(memory_space=pl.ANY)


def gelu_parts(inner):
    both = 0.5 * (1.0 + lax.erf(inner * root_half))
    slope = both + inner * density * jnp.exp(-0.5 * inner * inner)
    return (inner * both).astype(BF), slope.astype(BF)


def group_spec(rows, units):
    return pl.BlockSpec((1, rows, units), lambda t: (t, 0, 0))


def fixed(*dims):
    return pl.BlockSpec(dims, lambda t: (0,) * len(dims))


def enter_body(units, meta_ref, near_ref, far_ref, *refs):
    mixed_refs, (own_ref, out_bias_ref, gain_ref, shift_ref, bias_ref) = refs[:4], refs[4:9]
    low_ref, unit_ref, inverse_ref, act_ref, slope_ref = refs[9:14]
    out_ref, out_sems, up_ref, up_sems = refs[14:]
    group = pl.program_id(0)

    @pl.when(group == 0)
    def _():
        copies = group_copies(near_ref, far_ref, out_ref, out_sems, 2 * units)
        for copy in copies + group_copies(near_ref, far_ref, up_ref, up_sems, 0):
            copy.start()
        hidden = own_ref[...].astype(F32) + out_bias_ref[...]
        for copy in copies:
            copy.wait()
        for j, ref in enumerate(mixed_refs):
            hidden = hidden + product_nt(ref[...].T, out_ref[group_place(meta_ref, j)])
        first, unit, inverse = normalize(hidden, gain_ref[...], shift_ref[...])
        unit_ref[...] = unit
        inverse_ref[...] = inverse
        low_ref[...] = first.astype(BF)

    group_wait(near_ref, up_ref, up_sems, 0, group)
    low = low_ref[...]
    step = units // 3
    for c in range(0, units, step):
        lanes = slice(c, c + step)
        inner = product(low, up_ref[group, :, lanes]) + bias_ref[0, :, lanes]
        act_ref[0, :, lanes], slope_ref[0, :, lanes] = gelu_parts(inner)


def enter(meta, weights, mixed, own, out_bias, gain, shift, bias):
    rows, width = own.shape
    groups, _, units = bias.shape
    return pl.pallas_call(
        functools.partial(enter_body, units),
        grid=(groups,),
        in_specs=[smem()] + [unmoved()] * 2 + [vmem()] * 8 + [group_spec(1, units)],
        out_specs=[fixed(rows, width), fixed(rows, width), fixed(rows, 1)]
        + [group_spec(rows, units)] * 2,
        out_shape=[spec(BF, rows, width), spec(F32, rows, width), spec(F32, rows, 1)]
        + [spec(BF, groups, rows, units)] * 2,
        scratch_shapes=held(width, mixed[0].shape[0]) + held(width, units),
        compiler_params=params(),
        cost_estimate=cost(12 * rows * width * units, 20 << 20, 8 * rows * units),
        name="enter",
    )(meta, *weights, *mixed, own, out_bias, gain, shift, bias)


def turn_body(near_ref, far_ref, act_ref, *refs):
    unit_ref, first_gain_ref, first_shift_ref, bias_ref, gain_ref, shift_ref, up_ref = refs[:7]
    out_ref, grad_ref, low_ref, sums_ref, total_ref, down_ref, sems = refs[7:]
    step = pl.program_id(0)
    units = act_ref.shape[2]

    @pl.when(step == 0)
    def _():
        for copy in group_copies(near_ref, far_ref, down_ref, sems, units):
            copy.start()

    group_wait(near_ref, down_ref, sems, units, step)
    part = product_nt(act_ref[0], down_ref[step])

    @pl.when(step == 0)
    def _():
        total_ref[...] = part

    @pl.when(step > 0)
    def _():
        total_ref[...] += part

    @pl.when(step == pl.num_programs(0) - 1)
    def _():
        def chunk(at):
            first = unit_ref[at, :] * first_gain_ref[...] + first_shift_ref[...]
            second, unit, inverse = normalize(
                first + total_ref[at, :] + bias_ref[...], gain_ref[...], shift_ref[...]
            )
            out_ref[at, :] = second.astype(BF)
            upstream = up_ref[at, :].astype(F32)
            grad = norm_back(upstream, unit, inverse, gain_ref[...])
            grad_ref[at, :] = grad
            low_ref[at, :] = grad.astype(BF)
            return grad, upstream * unit, upstream

        sums = by_chunks(total_ref.shape[0], total_ref.shape[1], 64, chunk)
        for k in range(3):
            sums_ref[k : k + 1, :] = sums[k]


def turn(weights, acts, unit, first_gain, first_shift, bias, gain, shift, cotangent):
    rows, width = unit.shape
    groups, _, units = acts.shape
    return pl.pallas_call(
        turn_body,
        grid=(groups,),
        in_specs=[unmoved()] * 2 + [group_spec(rows, units)] + [vmem()] * 7,
        out_specs=[fixed(rows, width)] * 3 + [fixed(3, width)],
        out_shape=[
            spec(BF, rows, width),
            spec(F32, rows, width),
            spec(BF, rows, width),
            spec(F32, 3, width),
        ],
        scratch_shapes=[pltpu.VMEM((rows, width), F32)] + held(width, units),
        compiler_params=params(),
        cost_estimate=cost(8 * rows * width * units, 16 << 20),
        name="turn",
    )(*weights, acts, unit, first_gain, first_shift, bias, gain, shift, cotangent)


def leave_body(units, meta_ref, near_ref, far_ref, *refs):
    slope_ref, low_ref, second_ref, unit_ref, inverse_ref, gain_ref = refs[:6]
    inner_ref, hidden_ref, attn_ref, own_ref, next_ref, far_rows_ref, sums_ref = refs[6:13]
    out_ref, out_sems, up_ref, up_sems, down_ref, down_sems = refs[13:]
    step = pl.program_id(0)

    @pl.when(step == 0)
    def _():
        for down, up in zip(
            group_copies(near_ref, far_ref, down_ref, down_sems, units),
            group_copies(near_ref, far_ref, up_ref, up_sems, 0),
        ):
            down.start()
            up.start()
        for copy in group_copies(near_ref, far_ref, out_ref, out_sems, 2 * units):
            copy.start()
        hidden_ref[...] = second_ref[...]

    group_wait(near_ref, down_ref, down_sems, units, step)
    grad = product(low_ref[...], down_ref[step]) * slope_ref[0].astype(F32)
    inner = grad.astype(BF)
    inner_ref[0] = inner
    total_inner = jnp.sum(inner.astype(F32), axis=0, keepdims=True)
    sums_ref[pl.ds(3 + group_owner(meta_ref, step), 1), :] = total_inner
    group_wait(near_ref, up_ref, up_sems, 0, step)
    hidden_ref[...] += product_nt(inner, up_ref[step])

    @pl.when(step == pl.num_programs(0) - 1)
    def _():
        for copy in group_copies(near_ref, far_ref, out_ref, out_sems, 2 * units):
            copy.wait()
        back = hidden_ref[...]
        unit = unit_ref[...]
        hidden = norm_back(back, unit, inverse_ref[...], gain_ref[...])
        hidden_ref[...] = hidden
        sums_ref[0:1, :] = jnp.sum(hidden, axis=0, keepdims=True)
        sums_ref[1:2, :] = jnp.sum(back * unit, axis=0, keepdims=True)
        sums_ref[2:3, :] = jnp.sum(back, axis=0, keepdims=True)
        attn = hidden.astype(BF)
        attn_ref[...] = attn
        for j in range(4):
            mixed = product(attn, out_ref[group_place(meta_ref, j)]).T.astype(BF)
            if j == 0:
                own_ref[...] = mixed
            elif j == 1:
                next_ref[...] = mixed
            else:
                far_rows_ref[j - 2] = mixed


def leave(meta, weights, slopes, low, second, unit, inverse, gain):
    rows, width = low.shape
    groups, _, units = slopes.shape
    feats = weights[0].shape[2] - 2 * units
    return pl.pallas_call(
        functools.partial(leave_body, units),
        grid=(groups,),
        in_specs=[smem()] + [unmoved()] * 2 + [group_spec(rows, units)] + [vmem()] * 5,
        out_specs=[
            group_spec(rows, units),
            fixed(rows, width),
            fixed(rows, width),
            fixed(feats, rows),
            fixed(feats, rows),
            fixed(2, feats, rows),
            fixed(3 + groups, width),
        ],
        out_shape=[
            spec(BF, groups, rows, units),
            spec(F32, rows, width),
            spec(BF, rows, width),
            spec(BF, feats, rows),
            spec(BF, feats, rows),
            spec(BF, 2, feats, rows),
            spec(F32, 3 + groups, width),
        ],
        scratch_shapes=held(width, feats) + held(width, units) + held(width, units),
        compiler_params=params(),
        cost_estimate=cost(16 * rows * width * units, 28 << 20),
        name="leave",
    )(meta, *weights, slopes, low, second, unit, inverse, gain)


def outer_body(shard, extra, keep, meta_ref, left_ref, right_ref, *refs):
    if extra:
        attn_ref, mixed_refs, sum_refs, refs = refs[0], refs[1:3], refs[3:5], refs[5:]
    if keep:
        arrived_ref, refs = refs[0], refs[1:]
        left_t_ref, attn_t_ref = left_ref, attn_ref if extra else None
    else:
        left_t_ref, attn_t_ref = refs[1], refs[2] if extra else None
    out_ref = refs[0]
    step = pl.program_id(0)
    units = right_ref.shape[2]
    width = left_t_ref.shape[0]
    pairs = width // shard // 2
    lanes = out_ref.shape[3]

    if not keep:

        @pl.when(step == 0)
        def _():
            left_t_ref[...] = left_ref[...].T
            if extra:
                attn_t_ref[...] = attn_ref[...].T

    def put(low, rows, lane, values):
        if keep:
            values = values + arrived_ref[low, 0, rows, lane].astype(F32)
        out_ref[low, 0, rows, lane] = values.astype(BF)

    def spread(values, lane):
        for block in range(2 * pairs):
            rows = slice(block // 2 * shard, (block // 2 + 1) * shard)
            put(block % 2, rows, lane, values[block * shard : (block + 1) * shard])

    spread(product(left_t_ref[...], right_ref[0]), slice(0, units))
    if extra:
        for j in range(2):

            @pl.when(step ^ (meta_ref[0] // 2) == j)
            def _(j=j):
                spread(product_nt(attn_t_ref[...], mixed_refs[j][...]), slice(units, lanes))

        sums = jnp.concatenate(
            [sum_refs[0][...], sum_refs[1][...], jnp.zeros((16 - 10, width), F32)], axis=0
        )
        for low in range(2):
            put(low, slice(pairs * shard, pairs * shard + 16), slice(0, width), sums)
            out_ref[low, 0, pairs * shard :, width:lanes] = jnp.zeros((16, lanes - width), BF)


def outer(meta, shard, left, rights, attn=None, mixed=(), sums=(), arrived=None):
    keep = arrived is not None
    rows, width = left.shape[::-1] if keep else left.shape
    groups, _, units = rights.shape
    extra = attn is not None
    feats = mixed[0].shape[0] if extra else 0
    depth = width // 2 + (16 if extra else 0)

    args = [left, rights] + ([attn, *mixed, *sums] if extra else [])
    block = pl.BlockSpec((2, 1, depth, units + feats), lambda i, m: (0, i, 0, 0))
    turned = [] if keep else [left, attn] if extra else [left]
    grid_spec = pltpu.PrefetchScalarGridSpec(
        num_scalar_prefetch=1,
        grid=(2,),
        in_specs=[vmem(), pl.BlockSpec((1, rows, units), lambda i, m: (i if keep else i + 2, 0, 0))]
        + [vmem()] * (len(args) - 2)
        + ([block] if keep else []),
        out_specs=[block] + [vmem()] * len(turned),
    )
    return pl.pallas_call(
        functools.partial(outer_body, shard, extra, keep),
        grid_spec=grid_spec,
        out_shape=[spec(BF, 2, 2, depth, units + feats)] + [spec(BF, width, rows) for _ in turned],
        compiler_params=params(),
        cost_estimate=cost(4 * rows * width * units, 8 << 20),
        name="outer",
    )(meta, *args, *([arrived] if keep else []))


def inputs_body(*refs):
    dq_refs, (dk_ref, dv_ref, turned_ref) = refs[:4], refs[4:7]
    own_ref, next_ref, out_ref = refs[7:10]
    rows = dq_refs[0].shape[1]
    weight = turned_ref[...]
    for r in (1, 3, 0, 2):
        at = slice(r * rows, (r + 1) * rows)
        grad = jnp.concatenate([dq_refs[r][...], dk_ref[:, at], dv_ref[:, at]], axis=0)
        back = product(grad.T, weight)
        if r == 0:
            own_ref[...] = back
        elif r == 2:
            next_ref[...] = back
        else:
            out_ref[(r // 2) * rows : (r // 2 + 1) * rows, :] = back.astype(BF)


def input_grads(dq, dk, dv, turned):
    rows = dq[0].shape[1]
    width = turned.shape[1]
    return pl.pallas_call(
        inputs_body,
        in_specs=[vmem()] * 7,
        out_specs=[vmem()] * 3,
        out_shape=[spec(F32, rows, width), spec(F32, rows, width), spec(BF, 2 * rows, width)],
        compiler_params=params(),
        cost_estimate=cost(8 * rows * width * width, 12 << 20),
        name="input_grads",
    )(*dq, dk, dv, turned)


def projections_body(shard, *refs):
    meta_ref, dq_refs, (dk_ref, dv_ref, all_ref, keep_ref, send_ref) = refs[0], refs[1:5], refs[5:10]
    held_ref = refs[10]
    rows = dq_refs[0].shape[1]
    depth = keep_ref.shape[0] - 16
    grad = jnp.concatenate(
        [jnp.concatenate([ref[...] for ref in dq_refs], axis=1), dk_ref[...], dv_ref[...]], axis=0
    )
    held_ref[...] = product(grad, all_ref[...]).T.astype(BF)
    sums = product_nt(jnp.ones((16, 4 * rows), BF), grad).astype(BF)
    for flip, out_ref in ((0, keep_ref), (1, send_ref)):
        for i in range(depth // shard):
            block = 2 * i + (meta_ref[1] ^ flip)
            if shard % 16 == 0:
                start = pl.multiple_of(block * shard, shard)
                out_ref[i * shard : (i + 1) * shard, :] = held_ref[pl.ds(start, shard), :]
            else:
                even = held_ref[2 * i * shard : (2 * i + 1) * shard, :]
                odd = held_ref[(2 * i + 1) * shard : (2 * i + 2) * shard, :]
                out_ref[i * shard : (i + 1) * shard, :] = jnp.where(block % 2 == 0, even, odd)
        out_ref[depth:, :] = sums


def projection_grads(meta, shard, dq, dk, dv, tokens):
    width = tokens.shape[1]
    feats = dq[0].shape[0]
    return pl.pallas_call(
        functools.partial(projections_body, shard),
        in_specs=[smem()] + [vmem()] * 7,
        out_specs=[vmem()] * 2,
        out_shape=[spec(BF, width // 2 + 16, 3 * feats)] * 2,
        scratch_shapes=[pltpu.VMEM((width, 3 * feats), BF)],
        compiler_params=params(),
        cost_estimate=cost(2 * tokens.shape[0] * width * 3 * feats, 12 << 20),
        name="projection_grads",
    )(meta, *dq, dk, dv, tokens)


def exchanger(axis_dp, axis_tensor):
    def swap(values, dp_bits, tensor_bits):
        pairs = [
            (d * axis_tensor + t, (d ^ dp_bits) * axis_tensor + (t ^ tensor_bits))
            for d in range(axis_dp)
            for t in range(axis_tensor)
        ]
        return lax.ppermute(values, ("dp", "tensor"), pairs)

    return swap


def tie(*values):
    return lax.optimization_barrier(values)


def add(left, right):
    return (left.astype(F32) + right.astype(F32)).astype(BF)


def total(parts):
    return functools.reduce(jnp.add, [parts[i].astype(F32) for i in range(parts.shape[0])])


def local(
    axis_dp,
    axis_tensor,
    inputs,
    segments,
    query_weight,
    query_bias,
    key_weight,
    value_weight,
    value_bias,
    output_weight,
    output_bias,
    up_weight,
    up_bias,
    down_weight,
    down_bias,
    first_gain,
    first_shift,
    second_gain,
    second_shift,
    cotangent,
):
    swap = exchanger(axis_dp, axis_tensor)
    place_dp, place_tensor = lax.axis_index("dp"), lax.axis_index("tensor")
    meta = jnp.stack([place_tensor, place_dp % 2]).astype(jnp.int32)
    rows, width = inputs.shape[1:]
    shard = query_weight.shape[0]
    feats = output_weight.shape[0]
    heads = feats // HEAD
    units = up_weight.shape[1]
    pairs = axis_dp // 2
    row = lambda v: v.reshape(1, -1).astype(F32)
    flat = lambda z, x, y, c: (2 * z + x) * axis_tensor + 2 * y + c
    near_groups = [
        [flat(z, x, y, c) for x in range(2) for y in range(2)] for z in range(pairs) for c in range(2)
    ]
    deep_groups = [[2 * z + x for z in range(pairs)] for x in range(2)]

    own = inputs[0]
    notes = jnp.zeros((16, width), BF)
    notes = notes.at[0, :rows].set(segments[0].astype(BF)).at[1, :units].set(up_bias)
    message = jnp.concatenate([own, notes])
    across = swap(message, 0, 2)
    bundle = jnp.concatenate([query_weight, key_weight, value_weight], axis=1)
    copies = jnp.broadcast_to(bundle[None], (axis_dp,) + bundle.shape)
    qkv_weight = lax.all_to_all(copies, "dp", 0, 0, tiled=True).reshape(width, 3 * feats)
    near = swap(message, 0, 1)
    far = swap(across, 0, 1)
    tokens = [message, near, across, far]

    core_groups = [
        [d * axis_tensor + 2 * y + c for y in range(2) for d in range(axis_dp)] for c in range(2)
    ]
    near_weights = lax.all_gather(
        jnp.concatenate([up_weight, down_weight.T, output_weight.T], axis=1),
        ("dp", "tensor"), axis=0, axis_index_groups=core_groups, tiled=True,
    ).reshape(2, width, 2 * units + feats)
    weights = near_weights, swap(near_weights, 0, 1)

    noted = jnp.stack([v[rows:] for v in tokens]).astype(F32)
    docs = noted[:, 0, :rows].reshape(-1)
    bias = noted[:, 1:2, :units]
    bias = [
        lax.dynamic_index_in_dim(bias, 2 * ((g % 2) ^ (place_tensor // 2)) + g // 2, 0, False)
        for g in range(4)
    ]
    bias = jnp.stack(bias)
    lane = jnp.arange(HEAD, dtype=F32)
    same = docs[:, None] == lane[None, :]
    aux_query = (docs[None, :] == lane[:, None]).astype(BF)
    aux_key = jnp.where(same | (lane[None, :] >= 8), 0.0, -far_score).astype(BF)
    qkv_bias = jnp.concatenate([query_bias, jnp.zeros_like(query_bias), value_bias]).astype(F32)
    all_tokens, turned, queries, keys, values, values_t, keys_t = project(
        qkv_weight, tokens, rows, qkv_bias[feats:].reshape(1, -1), qkv_bias.reshape(-1, 1),
        aux_query, aux_key, heads,
    )

    mixed23, log23 = attend_forward(keys, queries, values_t, (2, 3))
    queries, mixed23 = tie(queries, mixed23)
    arrived = swap(mixed23, 0, 2)
    mixed1, log1 = attend_forward(keys, queries, values_t, (1,))
    queries, mixed1 = tie(queries, mixed1)
    arrived1 = swap(mixed1, 0, 1)
    mixed0, log0 = attend_forward(keys, queries, values_t, (0,))
    mixed = [mixed0[0], arrived1[0], arrived[0], swap(arrived[1], 0, 1)]

    low, unit_first, inverse_first, acts, slopes = enter(
        meta, weights, mixed, own, row(output_bias), row(first_gain), row(first_shift), bias
    )
    layer_out, grad_second, second_low, sums_second = turn(
        weights, acts, unit_first, row(first_gain), row(first_shift),
        row(down_bias), row(second_gain), row(second_shift), cotangent[0],
    )
    send_b, second_t = outer(meta, shard, second_low, acts)
    second_low, send_b = tie(second_low, send_b)
    moved_b = swap(send_b, 0, 1)
    inners, grad_hidden, grad_attn, grad0, next_mixed, far_mixed, sums_first = leave(
        meta, weights, slopes, second_low, grad_second, unit_first, inverse_first, row(first_gain)
    )

    def reduce_near(values):
        values = values.reshape((4,) + values.shape[2:])
        return lax.all_to_all(values, ("dp", "tensor"), 0, 0, axis_index_groups=near_groups, tiled=True)

    def reduce_deep(values):
        return lax.all_to_all(values, "dp", 0, 0, axis_index_groups=deep_groups, tiled=True)

    def deep_parts(values):
        return values[: pairs * shard].reshape(pairs, shard, -1)

    def part_at(parts, k):
        return lax.dynamic_index_in_dim(parts, (place_dp // 2) ^ k, 0, False)

    arrived_g = swap(far_mixed, 0, 2)
    g1 = swap(next_mixed, 0, 1)
    (part_b,) = outer(meta, shard, second_t, acts, arrived=moved_b)
    inners, part_b = tie(inners, part_b)
    near_b = reduce_near(part_b)
    sums_both = (sums_first, sums_second)
    send_a, low_t, attn_t = outer(meta, shard, low, inners, grad_attn, mixed[1::2], sums_both)
    grad0, send_a, g1, arrived_g = tie(grad0, send_a, g1, arrived_g)
    moved_a = swap(send_a, 0, 1)
    g2, g3 = arrived_g[0], swap(arrived_g[1], 0, 1)
    operands = (keys, queries, values, keys_t)
    (dq0, dq1), carried = attend_back(
        operands, (0, 1), ((log0, 0), (log1, 0)), ((mixed0, 0), (mixed1, 0)), (grad0, g1), None, False
    )
    low_t, carried, moved_a = tie(low_t, carried, moved_a)
    (part_a,) = outer(meta, shard, low_t, inners, attn_t, mixed[::2], sums_both, moved_a)
    carried, part_a, near_b, g2, g3 = tie(carried, part_a, near_b, g2, g3)
    near_a = reduce_near(part_a)
    parts_b = deep_parts(total(near_b).astype(BF))
    sent_b = [part_at(parts_b, k) for k in range(1, pairs)]
    carried, parts_b, *sent_b = tie(carried, parts_b, *sent_b)
    own_b = part_at(parts_b, 0).astype(F32)
    for k in range(1, pairs):
        own_b = own_b + swap(sent_b[k - 1], 2 * k, 0).astype(F32)
    (dq2, dq3), (dk, dv) = attend_back(
        operands, (2, 3), ((log23, 0), (log23, 1)), ((mixed23, 0), (mixed23, 1)), (g2, g3), carried, True
    )
    dq = (dq0, dq1, dq2, dq3)
    own_rows, next_rows, sent_rows = input_grads(dq, dk, dv, turned)
    moved = swap(sent_rows, 0, 1)
    dk, sent_rows = tie(dk, sent_rows)
    keep_c, send_c = projection_grads(meta, shard, dq, dk, dv, all_tokens)
    next_rows = add(next_rows, moved[rows:])
    send_c, next_rows, near_a, own_b = tie(send_c, next_rows, near_a, own_b)
    arrived_c = swap(send_c, 1, 0)
    arrived_rows = swap(next_rows, 0, 2)
    sum_a = total(near_a).astype(BF)
    notes = jnp.broadcast_to(sum_a[None, pairs * shard :], (pairs, 16, sum_a.shape[1]))
    deep_a = reduce_deep(jnp.concatenate([deep_parts(sum_a), notes], axis=1))
    sum_c, arrived_rows = tie(add(keep_c, arrived_c), arrived_rows)
    parts_c, notes = deep_parts(sum_c), sum_c[pairs * shard :]
    own_c = jnp.concatenate([part_at(parts_c, 0), notes]).astype(F32)
    for k in range(1, pairs):
        own_c = own_c + swap(jnp.concatenate([part_at(parts_c, k), notes]), 2 * k, 0).astype(F32)
    own_a = total(deep_a)
    grad_inputs = grad_hidden + own_rows + moved[:rows].astype(F32) + arrived_rows.astype(F32)
    sums = own_a[shard:, :width]
    sum_up = lax.dynamic_index_in_dim(sums[3:7], place_tensor, 0, False)
    head_sums = own_c[shard]

    return (
        layer_out[None],
        grad_inputs[None],
        own_c[:shard, :feats],
        head_sums[:feats],
        own_c[:shard, feats : 2 * feats],
        own_c[:shard, 2 * feats :],
        head_sums[2 * feats :],
        own_a[:shard, units:].T,
        sums[0],
        own_a[:shard, :units],
        sum_up,
        own_b.T,
        sums[7],
        sums[1],
        sums[2],
        sums[8],
        sums[9],
    )


def solution(mesh):
    axis_dp, axis_tensor = mesh.shape["dp"], mesh.shape["tensor"]
    if axis_tensor != 4 or axis_dp < 2 or axis_dp & (axis_dp - 1):
        raise ValueError("mesh sizes")
    return jax.shard_map(
        functools.partial(local, axis_dp, axis_tensor),
        mesh=mesh,
        in_specs=(
            P("dp", "tensor", None),
            P("dp", "tensor"),
            P("dp", "tensor"),
            P("tensor"),
            P("dp", "tensor"),
            P("dp", "tensor"),
            P("tensor"),
            P("tensor", "dp"),
            P(),
            P("dp", "tensor"),
            P("tensor"),
            P("tensor", "dp"),
            P(),
            P(),
            P(),
            P(),
            P(),
            P("dp", "tensor", None),
        ),
        out_specs=(
            P("dp", "tensor", None),
            P("dp", "tensor", None),
            P("dp", "tensor"),
            P("tensor"),
            P("dp", "tensor"),
            P("dp", "tensor"),
            P("tensor"),
            P("tensor", "dp"),
            P(),
            P("dp", "tensor"),
            P("tensor"),
            P("tensor", "dp"),
            P(),
            P(),
            P(),
            P(),
            P(),
        ),
        check_vma=False,
    )
```

```python
import functools

import jax
import jax.numpy as jnp
from jax import lax
from jax.experimental import pallas as pl
from jax.experimental.pallas import tpu as pltpu
from jax.sharding import PartitionSpec as P

HEAD = 64
BF = jnp.bfloat16
F32 = jnp.float32

eps_norm = 1e-12
root_half = 0.7071067811865476
density = 0.3989422804014327
scale = 0.125
log2e = 1.4426950408889634
far_score = 1e30
vmem_bytes = 60 * 1024 * 1024


def product(left, right):
    return jnp.dot(left, right, preferred_element_type=F32)


def product_nt(left, right):
    return lax.dot_general(left, right, (((1,), (1,)), ((), ())), preferred_element_type=F32)


def product_tn(left, right):
    return lax.dot_general(left, right, (((0,), (0,)), ((), ())), preferred_element_type=F32)


def normalize(values, gain, offset):
    average = jnp.mean(values, axis=-1, keepdims=True)
    centred = values - average
    inverse = lax.rsqrt(jnp.mean(centred * centred, axis=-1, keepdims=True) + eps_norm)
    normed = centred * inverse
    return (normed * gain + offset, normed, inverse)


def norm_back(upstream, normed, inverse, gain):
    scaled = upstream * gain
    centred = scaled - jnp.mean(scaled, axis=-1, keepdims=True)
    return (centred - normed * jnp.mean(scaled * normed, axis=-1, keepdims=True)) * inverse


def fold(values):
    return functools.reduce(jnp.add, [values[i : i + 8] for i in range(0, values.shape[0], 8)])


def by_chunks(rows, width, size, chunk):
    def step(i, sums):
        at = pl.ds(pl.multiple_of(i * size, size), size)
        return tuple(a + fold(b) for a, b in zip(sums, chunk(at)))

    sums = lax.fori_loop(0, rows // size, step, (jnp.zeros((8, width), F32),) * 3)
    return [jnp.sum(v, axis=0, keepdims=True) for v in sums]


def vmem():
    return pl.BlockSpec(memory_space=pltpu.VMEM)


def smem():
    return pl.BlockSpec(memory_space=pltpu.SMEM)


def params():
    return pltpu.CompilerParams(vmem_limit_bytes=vmem_bytes)


def cost(flops, moved, hard=0):
    return pl.CostEstimate(flops=int(flops), bytes_accessed=int(moved), transcendentals=int(hard))


def spec(dtype, *dims):
    return jax.ShapeDtypeStruct(dims, dtype)


def project_body(heads, *refs):
    token_refs, (weight_ref, row_bias_ref, column_bias_ref, aux_query_ref, aux_key_ref) = refs[:4], refs[4:9]
    all_ref, turned_ref, query_ref, key_ref, value_ref, value_t_ref, key_t_ref = refs[9:16]
    step = pl.program_id(0)
    width = heads * HEAD
    rows = all_ref.shape[0]

    @pl.when(step == 0)
    def _():
        turned_ref[...] = weight_ref[...].T

    for r, ref in enumerate(token_refs):

        @pl.when(step == r)
        def _(ref=ref):
            all_ref[...] = ref[:rows, :]

    tokens = all_ref[...]
    turned = (product_nt(turned_ref[...], tokens) + column_bias_ref[...]).astype(BF)
    plain = (product(tokens, weight_ref[:, width : 3 * width]) + row_bias_ref[...]).astype(BF)
    for h in range(heads):
        at = slice(h * HEAD, (h + 1) * HEAD)
        query_ref[h, :HEAD, :] = turned[at]
        query_ref[h, HEAD:, :] = aux_query_ref[...]
        key_t_ref[at, :] = turned[width : 2 * width][at]
        value_t_ref[at, :] = turned[2 * width :][at]
        key_ref[h] = jnp.concatenate([plain[:, at], aux_key_ref[...]], axis=1)
        value_ref[h] = plain[:, width + h * HEAD : width + (h + 1) * HEAD]


def project(weight, tokens, rows, row_bias, column_bias, aux_query, aux_key, heads):
    width = weight.shape[0]
    length = 4 * rows
    by_row = lambda n: pl.BlockSpec((rows, n), lambda r: (r, 0))
    headed = lambda n: pl.BlockSpec((heads, rows, n), lambda r: (0, r, 0))
    flat = pl.BlockSpec((heads * HEAD, rows), lambda r: (0, r))
    return pl.pallas_call(
        functools.partial(project_body, heads),
        grid=(4,),
        in_specs=[vmem()] * 7 + [pl.BlockSpec((HEAD, rows), lambda r: (0, r)), by_row(HEAD)],
        out_specs=[
            by_row(width),
            pl.BlockSpec((3 * heads * HEAD, width), lambda r: (0, 0)),
            pl.BlockSpec((heads, 2 * HEAD, rows), lambda r: (0, 0, r)),
            headed(2 * HEAD),
            headed(HEAD),
            flat,
            flat,
        ],
        out_shape=[
            spec(BF, length, width),
            spec(BF, 3 * heads * HEAD, width),
            spec(BF, heads, 2 * HEAD, length),
            spec(BF, heads, length, 2 * HEAD),
            spec(BF, heads, length, HEAD),
            spec(BF, heads * HEAD, length),
            spec(BF, heads * HEAD, length),
        ],
        compiler_params=params(),
        cost_estimate=cost(4 * length * width * 3 * heads * HEAD, 16 << 20),
        name="project",
    )(*tokens, weight, row_bias, column_bias, aux_query, aux_key)


def forward_body(count, key_ref, *refs):
    query_refs, value_ref, out_ref, log_ref = refs[:count], refs[count], refs[count + 1], refs[count + 2]
    chunk = key_ref.shape[1] // 4
    for i in range(count):
        query = query_refs[i][0]
        scores = [product(key_ref[0, c * chunk : (c + 1) * chunk, :], query) for c in range(4)]
        highest = None
        for c in range(4):
            peak = jnp.max(scores[c], axis=0, keepdims=True)
            now = peak if highest is None else jnp.maximum(highest, peak)
            raised = jnp.exp2((scores[c] - now) * (scale * log2e))
            part = jnp.sum(raised, axis=0, keepdims=True)
            mixed = product(value_ref[:, c * chunk : (c + 1) * chunk], raised.astype(BF))
            if highest is None:
                total, out = part, mixed
            else:
                shrink = jnp.exp2((highest - now) * (scale * log2e))
                total, out = total * shrink + part, out * shrink + mixed
            highest = now
        out_ref[i] = (out / total).astype(BF)
        log_ref[i, 0] = highest * (scale * log2e) + jnp.log2(total)


def attend_forward(keys, queries, values_t, quarters):
    heads, length, _ = keys.shape
    rows = length // 4
    count = len(quarters)
    return pl.pallas_call(
        functools.partial(forward_body, count),
        grid=(heads,),
        in_specs=[pl.BlockSpec((1, length, 2 * HEAD), lambda h: (h, 0, 0))]
        + [pl.BlockSpec((1, 2 * HEAD, rows), lambda h, q=q: (h, 0, q)) for q in quarters]
        + [pl.BlockSpec((HEAD, length), lambda h: (h, 0))],
        out_specs=[
            pl.BlockSpec((count, HEAD, rows), lambda h: (0, h, 0)),
            pl.BlockSpec((count, 1, 1, rows), lambda h: (0, h, 0, 0)),
        ],
        out_shape=[spec(BF, count, heads * HEAD, rows), spec(F32, count, heads, 1, rows)],
        compiler_params=params(),
        cost_estimate=cost(
            20 * count * heads * rows * length * HEAD, 4 << 20, heads * rows * length
        ),
        name="attend_forward",
    )(keys, *[queries] * count, values_t)


def backward_body(count, first, last, key_ref, value_ref, key_t_ref, *refs):
    groups, refs = [refs[4 * i : 4 * i + 4] for i in range(count)], refs[4 * count :]
    if not first:
        (old_dk_ref, old_dv_ref), refs = refs[:2], refs[2:]
    dq_refs, (dk_ref, dv_ref) = refs[:count], refs[count:]
    dk = dv = None
    for (query_ref, log_ref, mixed_ref, grad_ref), dq_ref in zip(groups, dq_refs):
        grad = grad_ref[...]
        delta = jnp.sum(grad.astype(F32) * mixed_ref[0].astype(F32), axis=0, keepdims=True)
        scores = product(key_ref[0], query_ref[0])
        weights = jnp.exp2(scores * (scale * log2e) - log_ref[0, 0])
        grad_weights = product(value_ref[0], grad)
        grad_scores = (weights * (grad_weights - delta)).astype(BF)
        dq_ref[...] = (product(key_t_ref[...], grad_scores) * scale).astype(BF)
        add_dk = product_nt(query_ref[0, :HEAD, :], grad_scores)
        add_dv = product_nt(grad, weights.astype(BF))
        dk = add_dk if dk is None else dk + add_dk
        dv = add_dv if dv is None else dv + add_dv
    if not first:
        dk = dk + old_dk_ref[...]
        dv = dv + old_dv_ref[...]
    if last:
        dk = dk * scale
    dk_ref[...] = dk.astype(dk_ref.dtype)
    dv_ref[...] = dv.astype(dv_ref.dtype)


def attend_back(operands, quarters, logs, mixed, grads, carried, last):
    keys, queries, values, keys_t = operands
    heads, length, _ = keys.shape
    rows = length // 4
    first = carried is None
    flat = lambda n: pl.BlockSpec((HEAD, n), lambda h: (h, 0))
    by_head = lambda *dims: pl.BlockSpec((1,) + dims, lambda h: (h, 0, 0))
    in_specs = [by_head(length, 2 * HEAD), by_head(length, HEAD), flat(length)]
    args = [keys, values, keys_t]
    for q, (log, i), (out, j), grad in zip(quarters, logs, mixed, grads):
        in_specs += [
            pl.BlockSpec((1, 2 * HEAD, rows), lambda h, q=q: (h, 0, q)),
            pl.BlockSpec((1, 1, 1, rows), lambda h, i=i: (i, h, 0, 0)),
            pl.BlockSpec((1, HEAD, rows), lambda h, j=j: (j, h, 0)),
            flat(rows),
        ]
        args += [queries, log, out, grad]
    count = len(quarters)
    aliases = {}
    if not first:
        if not last:
            aliases = {len(args): count, len(args) + 1: count + 1}
        in_specs += [flat(length)] * 2
        args += list(carried)
    kind = BF if last else F32
    outs = pl.pallas_call(
        functools.partial(backward_body, count, first, last),
        grid=(heads,),
        in_specs=in_specs,
        out_specs=[flat(rows)] * count + [flat(length)] * 2,
        out_shape=[spec(BF, heads * HEAD, rows)] * count + [spec(kind, heads * HEAD, length)] * 2,
        input_output_aliases=aliases,
        compiler_params=params(),
        cost_estimate=cost(
            50 * count * heads * rows * length * HEAD, 8 << 20, count * heads * rows * length
        ),
        name="attend_back",
    )(*args)
    return outs[:count], outs[count:]


def side_copies(meta_ref, bundle_ref, held_ref, sems, start):
    lanes = pl.ds(start, held_ref.shape[2])
    return [
        pltpu.make_async_copy(bundle_ref.at[meta_ref[0] ^ g, :, lanes], held_ref.at[g], sems.at[g])
        for g in range(4)
    ]


def side_wait(bundle_ref, held_ref, sems, start, group):
    lanes = pl.ds(start, held_ref.shape[2])
    pltpu.make_async_copy(bundle_ref.at[0, :, lanes], held_ref.at[group], sems.at[group]).wait()


def down_copies(meta_ref, down_refs, held_ref, sems):
    blocks = held_ref.shape[1]
    copies = []
    for g, ref in enumerate(down_refs):
        for p in range(blocks):
            place = (2 * (p % (blocks // 2)) + p // (blocks // 2)) ^ meta_ref[2] if blocks > 1 else 0
            copies.append(pltpu.make_async_copy(ref.at[p], held_ref.at[g, place], sems.at[g]))
    return copies


def down_group(down_refs, held_ref, sems, group):
    pltpu.make_async_copy(down_refs[0], held_ref.at[group], sems.at[group]).wait()
    return held_ref[group].reshape(-1, held_ref.shape[3])


def held(*dims):
    return [pltpu.VMEM((4, *dims), BF), pltpu.SemaphoreType.DMA((4,))]


def unmoved():
    return pl.BlockSpec(memory_space=pl.ANY)


def gelu_parts(inner):
    both = 0.5 * (1.0 + lax.erf(inner * root_half))
    slope = both + inner * density * jnp.exp(-0.5 * inner * inner)
    return (inner * both).astype(BF), slope.astype(BF)


def group_spec(rows, units):
    return pl.BlockSpec((1, rows, units), lambda t: (t, 0, 0))


def fixed(*dims):
    return pl.BlockSpec(dims, lambda t: (0,) * len(dims))


def enter_body(units, meta_ref, bundle_ref, *refs):
    mixed_refs, (own_ref, out_bias_ref, gain_ref, shift_ref, bias_ref) = refs[:4], refs[4:9]
    low_ref, unit_ref, inverse_ref, act_ref, slope_ref = refs[9:14]
    out_ref, out_sems, up_ref, up_sems = refs[14:]
    group = pl.program_id(0)

    @pl.when(group == 0)
    def _():
        copies = side_copies(meta_ref, bundle_ref, out_ref, out_sems, units)
        for copy in copies + side_copies(meta_ref, bundle_ref, up_ref, up_sems, 0):
            copy.start()
        hidden = own_ref[...].astype(F32) + out_bias_ref[...]
        for copy in copies:
            copy.wait()
        for j, ref in enumerate(mixed_refs):
            hidden = hidden + product_nt(ref[...].T, out_ref[j])
        first, unit, inverse = normalize(hidden, gain_ref[...], shift_ref[...])
        unit_ref[...] = unit
        inverse_ref[...] = inverse
        low_ref[...] = first.astype(BF)

    side_wait(bundle_ref, up_ref, up_sems, 0, group)
    low = low_ref[...]
    step = units // 3
    for c in range(0, units, step):
        lanes = slice(c, c + step)
        inner = product(low, up_ref[group, :, lanes]) + bias_ref[0, :, lanes]
        act_ref[0, :, lanes], slope_ref[0, :, lanes] = gelu_parts(inner)


def enter(meta, bundle, mixed, own, out_bias, gain, shift, bias):
    rows, width = own.shape
    groups, _, units = bias.shape
    return pl.pallas_call(
        functools.partial(enter_body, units),
        grid=(groups,),
        in_specs=[smem(), unmoved()] + [vmem()] * 8 + [group_spec(1, units)],
        out_specs=[fixed(rows, width), fixed(rows, width), fixed(rows, 1)]
        + [group_spec(rows, units)] * 2,
        out_shape=[spec(BF, rows, width), spec(F32, rows, width), spec(F32, rows, 1)]
        + [spec(BF, groups, rows, units)] * 2,
        scratch_shapes=held(width, mixed[0].shape[0]) + held(width, units),
        compiler_params=params(),
        cost_estimate=cost(12 * rows * width * units, 20 << 20, 8 * rows * units),
        name="enter",
    )(meta, bundle, *mixed, own, out_bias, gain, shift, bias)


def turn_body(meta_ref, *refs):
    down_refs, act_ref, refs = refs[:4], refs[4], refs[5:]
    unit_ref, first_gain_ref, first_shift_ref, bias_ref, gain_ref, shift_ref, up_ref = refs[:7]
    out_ref, grad_ref, low_ref, sums_ref, total_ref, down_ref, sems = refs[7:]
    step = pl.program_id(0)

    @pl.when(step == 0)
    def _():
        for copy in down_copies(meta_ref, down_refs, down_ref, sems):
            copy.start()

    part = product_nt(act_ref[0], down_group(down_refs, down_ref, sems, step))

    @pl.when(step == 0)
    def _():
        total_ref[...] = part

    @pl.when(step > 0)
    def _():
        total_ref[...] += part

    @pl.when(step == pl.num_programs(0) - 1)
    def _():
        def chunk(at):
            first = unit_ref[at, :] * first_gain_ref[...] + first_shift_ref[...]
            second, unit, inverse = normalize(
                first + total_ref[at, :] + bias_ref[...], gain_ref[...], shift_ref[...]
            )
            out_ref[at, :] = second.astype(BF)
            upstream = up_ref[at, :].astype(F32)
            grad = norm_back(upstream, unit, inverse, gain_ref[...])
            grad_ref[at, :] = grad
            low_ref[at, :] = grad.astype(BF)
            return grad, upstream * unit, upstream

        sums = by_chunks(total_ref.shape[0], total_ref.shape[1], 64, chunk)
        for k in range(3):
            sums_ref[k : k + 1, :] = sums[k]


def turn(meta, downs, acts, unit, first_gain, first_shift, bias, gain, shift, cotangent):
    rows, width = unit.shape
    groups, _, units = acts.shape
    return pl.pallas_call(
        turn_body,
        grid=(groups,),
        in_specs=[smem()] + [unmoved()] * 4 + [group_spec(rows, units)] + [vmem()] * 7,
        out_specs=[fixed(rows, width)] * 3 + [fixed(3, width)],
        out_shape=[
            spec(BF, rows, width),
            spec(F32, rows, width),
            spec(BF, rows, width),
            spec(F32, 3, width),
        ],
        scratch_shapes=[pltpu.VMEM((rows, width), F32)] + held(*downs[0].shape),
        compiler_params=params(),
        cost_estimate=cost(8 * rows * width * units, 16 << 20),
        name="turn",
    )(meta, *downs, acts, unit, first_gain, first_shift, bias, gain, shift, cotangent)


def leave_body(units, meta_ref, bundle_ref, *refs):
    down_refs, refs = refs[:4], refs[4:]
    slope_ref, low_ref, second_ref, unit_ref, inverse_ref, gain_ref = refs[:6]
    inner_ref, hidden_ref, attn_ref, own_ref, next_ref, far_rows_ref, sums_ref = refs[6:13]
    out_ref, out_sems, up_ref, up_sems, down_ref, down_sems = refs[13:]
    step = pl.program_id(0)

    @pl.when(step == 0)
    def _():
        copies = down_copies(meta_ref, down_refs, down_ref, down_sems)
        copies += side_copies(meta_ref, bundle_ref, up_ref, up_sems, 0)
        copies += side_copies(meta_ref, bundle_ref, out_ref, out_sems, units)
        for copy in copies:
            copy.start()
        hidden_ref[...] = second_ref[...]

    down = down_group(down_refs, down_ref, down_sems, step)
    grad = product(low_ref[...], down) * slope_ref[0].astype(F32)
    inner = grad.astype(BF)
    inner_ref[0] = inner
    total_inner = jnp.sum(inner.astype(F32), axis=0, keepdims=True)
    sums_ref[pl.ds(3 + (meta_ref[0] ^ step), 1), :] = total_inner
    side_wait(bundle_ref, up_ref, up_sems, 0, step)
    hidden_ref[...] += product_nt(inner, up_ref[step])

    @pl.when(step == pl.num_programs(0) - 1)
    def _():
        for copy in side_copies(meta_ref, bundle_ref, out_ref, out_sems, units):
            copy.wait()
        back = hidden_ref[...]
        unit = unit_ref[...]
        hidden = norm_back(back, unit, inverse_ref[...], gain_ref[...])
        hidden_ref[...] = hidden
        sums_ref[0:1, :] = jnp.sum(hidden, axis=0, keepdims=True)
        sums_ref[1:2, :] = jnp.sum(back * unit, axis=0, keepdims=True)
        sums_ref[2:3, :] = jnp.sum(back, axis=0, keepdims=True)
        attn = hidden.astype(BF)
        attn_ref[...] = attn
        for j in range(4):
            mixed = product(attn, out_ref[j]).T.astype(BF)
            if j == 0:
                own_ref[...] = mixed
            elif j == 1:
                next_ref[...] = mixed
            else:
                far_rows_ref[j - 2] = mixed


def leave(meta, bundle, downs, slopes, low, second, unit, inverse, gain):
    rows, width = low.shape
    groups, _, units = slopes.shape
    feats = bundle.shape[2] - units
    return pl.pallas_call(
        functools.partial(leave_body, units),
        grid=(groups,),
        in_specs=[smem()] + [unmoved()] * 5 + [group_spec(rows, units)] + [vmem()] * 5,
        out_specs=[
            group_spec(rows, units),
            fixed(rows, width),
            fixed(rows, width),
            fixed(feats, rows),
            fixed(feats, rows),
            fixed(2, feats, rows),
            fixed(3 + groups, width),
        ],
        out_shape=[
            spec(BF, groups, rows, units),
            spec(F32, rows, width),
            spec(BF, rows, width),
            spec(BF, feats, rows),
            spec(BF, feats, rows),
            spec(BF, 2, feats, rows),
            spec(F32, 3 + groups, width),
        ],
        scratch_shapes=held(width, feats) + held(width, units) + held(*downs[0].shape),
        compiler_params=params(),
        cost_estimate=cost(16 * rows * width * units, 28 << 20),
        name="leave",
    )(meta, bundle, *downs, slopes, low, second, unit, inverse, gain)


def outer_body(shard, extra, keep, meta_ref, left_ref, right_ref, *refs):
    if extra:
        attn_ref, mixed_refs, sum_refs, refs = refs[0], refs[1:3], refs[3:5], refs[5:]
    if keep:
        arrived_ref, refs = refs[0], refs[1:]
        left_t_ref, attn_t_ref = left_ref, attn_ref if extra else None
    else:
        left_t_ref, attn_t_ref = refs[1], refs[2] if extra else None
    out_ref = refs[0]
    step = pl.program_id(0)
    units = right_ref.shape[2]
    width = left_t_ref.shape[0]
    pairs = width // shard // 2
    lanes = out_ref.shape[3]

    if not keep:

        @pl.when(step == 0)
        def _():
            left_t_ref[...] = left_ref[...].T
            if extra:
                attn_t_ref[...] = attn_ref[...].T

    def put(low, rows, lane, values):
        if keep:
            values = values + arrived_ref[low, 0, rows, lane].astype(F32)
        out_ref[low, 0, rows, lane] = values.astype(BF)

    def spread(values, lane):
        for block in range(2 * pairs):
            rows = slice(block // 2 * shard, (block // 2 + 1) * shard)
            put(block % 2, rows, lane, values[block * shard : (block + 1) * shard])

    spread(product(left_t_ref[...], right_ref[0]), slice(0, units))
    if extra:
        for j in range(2):

            @pl.when(step ^ (meta_ref[0] // 2) == j)
            def _(j=j):
                spread(product_nt(attn_t_ref[...], mixed_refs[j][...]), slice(units, lanes))

        sums = jnp.concatenate(
            [sum_refs[0][...], sum_refs[1][...], jnp.zeros((16 - 10, width), F32)], axis=0
        )
        for low in range(2):
            put(low, slice(pairs * shard, pairs * shard + 16), slice(0, width), sums)
            out_ref[low, 0, pairs * shard :, width:lanes] = jnp.zeros((16, lanes - width), BF)


def outer(meta, shard, left, rights, attn=None, mixed=(), sums=(), arrived=None):
    keep = arrived is not None
    rows, width = left.shape[::-1] if keep else left.shape
    groups, _, units = rights.shape
    extra = attn is not None
    feats = mixed[0].shape[0] if extra else 0
    depth = width // 2 + (16 if extra else 0)

    def group(i, meta_ref):
        return 2 * (i ^ (meta_ref[0] // 2)) + (0 if keep else 1)

    args = [left, rights] + ([attn, *mixed, *sums] if extra else [])
    block = pl.BlockSpec((2, 1, depth, units + feats), lambda i, m: (0, i, 0, 0))
    turned = [] if keep else [left, attn] if extra else [left]
    grid_spec = pltpu.PrefetchScalarGridSpec(
        num_scalar_prefetch=1,
        grid=(2,),
        in_specs=[vmem(), pl.BlockSpec((1, rows, units), lambda i, m: (group(i, m), 0, 0))]
        + [vmem()] * (len(args) - 2)
        + ([block] if keep else []),
        out_specs=[block] + [vmem()] * len(turned),
    )
    return pl.pallas_call(
        functools.partial(outer_body, shard, extra, keep),
        grid_spec=grid_spec,
        out_shape=[spec(BF, 2, 2, depth, units + feats)] + [spec(BF, width, rows) for _ in turned],
        compiler_params=params(),
        cost_estimate=cost(4 * rows * width * units, 8 << 20),
        name="outer",
    )(meta, *args, *([arrived] if keep else []))


def inputs_body(*refs):
    dq_refs, (dk_ref, dv_ref, turned_ref) = refs[:4], refs[4:7]
    own_ref, next_ref, out_ref = refs[7:10]
    rows = dq_refs[0].shape[1]
    weight = turned_ref[...]
    for r in (1, 3, 0, 2):
        at = slice(r * rows, (r + 1) * rows)
        grad = jnp.concatenate([dq_refs[r][...], dk_ref[:, at], dv_ref[:, at]], axis=0)
        back = product(grad.T, weight)
        if r == 0:
            own_ref[...] = back
        elif r == 2:
            next_ref[...] = back
        else:
            out_ref[(r // 2) * rows : (r // 2 + 1) * rows, :] = back.astype(BF)


def input_grads(dq, dk, dv, turned):
    rows = dq[0].shape[1]
    width = turned.shape[1]
    return pl.pallas_call(
        inputs_body,
        in_specs=[vmem()] * 7,
        out_specs=[vmem()] * 3,
        out_shape=[spec(F32, rows, width), spec(F32, rows, width), spec(BF, 2 * rows, width)],
        compiler_params=params(),
        cost_estimate=cost(8 * rows * width * width, 12 << 20),
        name="input_grads",
    )(*dq, dk, dv, turned)


def projections_body(shard, *refs):
    meta_ref, dq_refs, (dk_ref, dv_ref, all_ref, keep_ref, send_ref) = refs[0], refs[1:5], refs[5:10]
    held_ref = refs[10]
    rows = dq_refs[0].shape[1]
    depth = keep_ref.shape[0] - 16
    grad = jnp.concatenate(
        [jnp.concatenate([ref[...] for ref in dq_refs], axis=1), dk_ref[...], dv_ref[...]], axis=0
    )
    held_ref[...] = product(grad, all_ref[...]).T.astype(BF)
    sums = product_nt(jnp.ones((16, 4 * rows), BF), grad).astype(BF)
    for flip, out_ref in ((0, keep_ref), (1, send_ref)):
        for i in range(depth // shard):
            block = 2 * i + (meta_ref[1] ^ flip)
            if shard % 16 == 0:
                start = pl.multiple_of(block * shard, shard)
                out_ref[i * shard : (i + 1) * shard, :] = held_ref[pl.ds(start, shard), :]
            else:
                even = held_ref[2 * i * shard : (2 * i + 1) * shard, :]
                odd = held_ref[(2 * i + 1) * shard : (2 * i + 2) * shard, :]
                out_ref[i * shard : (i + 1) * shard, :] = jnp.where(block % 2 == 0, even, odd)
        out_ref[depth:, :] = sums


def projection_grads(meta, shard, dq, dk, dv, tokens):
    width = tokens.shape[1]
    feats = dq[0].shape[0]
    return pl.pallas_call(
        functools.partial(projections_body, shard),
        in_specs=[smem()] + [vmem()] * 7,
        out_specs=[vmem()] * 2,
        out_shape=[spec(BF, width // 2 + 16, 3 * feats)] * 2,
        scratch_shapes=[pltpu.VMEM((width, 3 * feats), BF)],
        compiler_params=params(),
        cost_estimate=cost(2 * tokens.shape[0] * width * 3 * feats, 12 << 20),
        name="projection_grads",
    )(meta, *dq, dk, dv, tokens)


def exchanger(axis_dp, axis_tensor):
    def swap(values, dp_bits, tensor_bits):
        pairs = [
            (d * axis_tensor + t, (d ^ dp_bits) * axis_tensor + (t ^ tensor_bits))
            for d in range(axis_dp)
            for t in range(axis_tensor)
        ]
        return lax.ppermute(values, ("dp", "tensor"), pairs)

    return swap


def tie(*values):
    return lax.optimization_barrier(values)


def add(left, right):
    return (left.astype(F32) + right.astype(F32)).astype(BF)


def total(parts):
    return functools.reduce(jnp.add, [parts[i].astype(F32) for i in range(parts.shape[0])])


def local(
    axis_dp,
    axis_tensor,
    inputs,
    segments,
    query_weight,
    query_bias,
    key_weight,
    value_weight,
    value_bias,
    output_weight,
    output_bias,
    up_weight,
    up_bias,
    down_weight,
    down_bias,
    first_gain,
    first_shift,
    second_gain,
    second_shift,
    cotangent,
):
    swap = exchanger(axis_dp, axis_tensor)
    place_dp, place_tensor = lax.axis_index("dp"), lax.axis_index("tensor")
    meta = jnp.stack([place_tensor, place_dp % 2, place_dp]).astype(jnp.int32)
    rows, width = inputs.shape[1:]
    shard = query_weight.shape[0]
    feats = output_weight.shape[0]
    heads = feats // HEAD
    units = up_weight.shape[1]
    pairs = axis_dp // 2
    row = lambda v: v.reshape(1, -1).astype(F32)
    flat = lambda z, x, y, c: (2 * z + x) * axis_tensor + 2 * y + c
    near_groups = [
        [flat(z, x, y, c) for x in range(2) for y in range(2)] for z in range(pairs) for c in range(2)
    ]
    deep_groups = [[2 * z + x for z in range(pairs)] for x in range(2)]

    own = inputs[0]
    notes = jnp.zeros((16, width), BF)
    notes = notes.at[0, :rows].set(segments[0].astype(BF)).at[1, :units].set(up_bias)
    message = jnp.concatenate([own, notes])
    across = swap(message, 0, 2)
    bundle = jnp.concatenate([query_weight, key_weight, value_weight], axis=1)
    copies = jnp.broadcast_to(bundle[None], (axis_dp,) + bundle.shape)
    qkv_weight = lax.all_to_all(copies, "dp", 0, 0, tiled=True).reshape(width, 3 * feats)
    near = swap(message, 0, 1)
    far = swap(across, 0, 1)
    tokens = [message, near, across, far]

    up_bundle = lax.all_gather(
        jnp.concatenate([up_weight, output_weight.T], axis=1), ("tensor", "dp"), axis=0, tiled=True
    ).reshape(axis_tensor, width, units + feats)
    down = down_weight.T
    around = jnp.stack([down] + [swap(down, 2 * k, 0) for k in range(1, pairs)])
    qkv_weight, _ = tie(qkv_weight, around)
    beside = swap(around, 1, 0)

    noted = jnp.stack([v[rows:] for v in tokens]).astype(F32)
    docs = noted[:, 0, :rows].reshape(-1)
    bias = noted[:, 1:2, :units]
    lane = jnp.arange(HEAD, dtype=F32)
    same = docs[:, None] == lane[None, :]
    aux_query = (docs[None, :] == lane[:, None]).astype(BF)
    aux_key = jnp.where(same | (lane[None, :] >= 8), 0.0, -far_score).astype(BF)
    qkv_bias = jnp.concatenate([query_bias, jnp.zeros_like(query_bias), value_bias]).astype(F32)
    all_tokens, turned, queries, keys, values, values_t, keys_t = project(
        qkv_weight, tokens, rows, qkv_bias[feats:].reshape(1, -1), qkv_bias.reshape(-1, 1),
        aux_query, aux_key, heads,
    )

    queries, _ = tie(queries, beside)
    column = jnp.concatenate([around, beside])
    column_across = swap(column, 0, 2)
    column_core = swap(column, 0, 1)
    mixed23, log23 = attend_forward(keys, queries, values_t, (2, 3))
    queries, mixed23 = tie(queries, mixed23)
    arrived = swap(mixed23, 0, 2)
    mixed1, log1 = attend_forward(keys, queries, values_t, (1,))
    queries, mixed1 = tie(queries, mixed1)
    arrived1 = swap(mixed1, 0, 1)
    mixed0, log0 = attend_forward(keys, queries, values_t, (0,))
    mixed = [mixed0[0], arrived1[0], arrived[0], swap(arrived[1], 0, 1)]

    _, later = tie(mixed0, column_across)
    downs = [column, column_core, column_across, swap(later, 0, 1)]
    if shard % 16:
        order = [2 * k + b for b in range(2) for k in range(pairs)]
        places = jnp.argsort(jnp.array(order) ^ place_dp)
        downs = [v[places].reshape(1, width, units) for v in downs]

    low, unit_first, inverse_first, acts, slopes = enter(
        meta, up_bundle, mixed, own, row(output_bias), row(first_gain), row(first_shift), bias
    )
    layer_out, grad_second, second_low, sums_second = turn(
        meta, downs, acts, unit_first, row(first_gain), row(first_shift),
        row(down_bias), row(second_gain), row(second_shift), cotangent[0],
    )
    send_b, second_t = outer(meta, shard, second_low, acts)
    second_low, send_b = tie(second_low, send_b)
    moved_b = swap(send_b, 0, 1)
    inners, grad_hidden, grad_attn, grad0, next_mixed, far_mixed, sums_first = leave(
        meta, up_bundle, downs, slopes, second_low, grad_second, unit_first, inverse_first, row(first_gain)
    )

    def reduce_near(values):
        values = values.reshape((4,) + values.shape[2:])
        return lax.all_to_all(values, ("dp", "tensor"), 0, 0, axis_index_groups=near_groups, tiled=True)

    def reduce_deep(values):
        return lax.all_to_all(values, "dp", 0, 0, axis_index_groups=deep_groups, tiled=True)

    def deep_parts(values):
        return values[: pairs * shard].reshape(pairs, shard, -1)

    def part_at(parts, k):
        return lax.dynamic_index_in_dim(parts, (place_dp // 2) ^ k, 0, False)

    arrived_g = swap(far_mixed, 0, 2)
    g1 = swap(next_mixed, 0, 1)
    (part_b,) = outer(meta, shard, second_t, acts, arrived=moved_b)
    inners, part_b = tie(inners, part_b)
    near_b = reduce_near(part_b)
    sums_both = (sums_first, sums_second)
    send_a, low_t, attn_t = outer(meta, shard, low, inners, grad_attn, mixed[1::2], sums_both)
    grad0, send_a, g1, arrived_g = tie(grad0, send_a, g1, arrived_g)
    moved_a = swap(send_a, 0, 1)
    g2, g3 = arrived_g[0], swap(arrived_g[1], 0, 1)
    operands = (keys, queries, values, keys_t)
    (dq0, dq1), carried = attend_back(
        operands, (0, 1), ((log0, 0), (log1, 0)), ((mixed0, 0), (mixed1, 0)), (grad0, g1), None, False
    )
    low_t, carried, moved_a = tie(low_t, carried, moved_a)
    (part_a,) = outer(meta, shard, low_t, inners, attn_t, mixed[::2], sums_both, moved_a)
    carried, part_a, near_b, g2, g3 = tie(carried, part_a, near_b, g2, g3)
    near_a = reduce_near(part_a)
    parts_b = deep_parts(total(near_b).astype(BF))
    sent_b = [part_at(parts_b, k) for k in range(1, pairs)]
    carried, parts_b, *sent_b = tie(carried, parts_b, *sent_b)
    own_b = part_at(parts_b, 0).astype(F32)
    for k in range(1, pairs):
        own_b = own_b + swap(sent_b[k - 1], 2 * k, 0).astype(F32)
    (dq2, dq3), (dk, dv) = attend_back(
        operands, (2, 3), ((log23, 0), (log23, 1)), ((mixed23, 0), (mixed23, 1)), (g2, g3), carried, True
    )
    dq2, own_b = tie(dq2, own_b)
    dq = (dq0, dq1, dq2, dq3)
    own_rows, next_rows, sent_rows = input_grads(dq, dk, dv, turned)
    moved = swap(sent_rows, 0, 1)
    dk, sent_rows = tie(dk, sent_rows)
    keep_c, send_c = projection_grads(meta, shard, dq, dk, dv, all_tokens)
    _, moved = tie(send_c, moved)
    next_rows = add(next_rows, moved[rows:])
    arrived_c = swap(send_c, 1, 0)
    arrived_rows = swap(next_rows, 0, 2)
    _, _, near_a = tie(send_c, next_rows, near_a)
    sum_a = total(near_a).astype(BF)
    notes = jnp.broadcast_to(sum_a[None, pairs * shard :], (pairs, 16, sum_a.shape[1]))
    deep_a = reduce_deep(jnp.concatenate([deep_parts(sum_a), notes], axis=1))
    sum_c, arrived_rows = tie(add(keep_c, arrived_c), arrived_rows)
    parts_c, notes = deep_parts(sum_c), sum_c[pairs * shard :]
    own_c = jnp.concatenate([part_at(parts_c, 0), notes]).astype(F32)
    for k in range(1, pairs):
        own_c = own_c + swap(jnp.concatenate([part_at(parts_c, k), notes]), 2 * k, 0).astype(F32)
    own_a = total(deep_a)
    grad_inputs = grad_hidden + own_rows + moved[:rows].astype(F32) + arrived_rows.astype(F32)
    sums = own_a[shard:, :width]
    sum_up = lax.dynamic_index_in_dim(sums[3:7], place_tensor, 0, False)
    head_sums = own_c[shard]

    return (
        layer_out[None],
        grad_inputs[None],
        own_c[:shard, :feats],
        head_sums[:feats],
        own_c[:shard, feats : 2 * feats],
        own_c[:shard, 2 * feats :],
        head_sums[2 * feats :],
        own_a[:shard, units:].T,
        sums[0],
        own_a[:shard, :units],
        sum_up,
        own_b.T,
        sums[7],
        sums[1],
        sums[2],
        sums[8],
        sums[9],
    )


def solution(mesh):
    axis_dp, axis_tensor = mesh.shape["dp"], mesh.shape["tensor"]
    if axis_tensor != 4 or axis_dp < 2 or axis_dp & (axis_dp - 1):
        raise ValueError("mesh sizes")
    return jax.shard_map(
        functools.partial(local, axis_dp, axis_tensor),
        mesh=mesh,
        in_specs=(
            P("dp", "tensor", None),
            P("dp", "tensor"),
            P("dp", "tensor"),
            P("tensor"),
            P("dp", "tensor"),
            P("dp", "tensor"),
            P("tensor"),
            P("tensor", "dp"),
            P(),
            P("dp", "tensor"),
            P("tensor"),
            P("tensor", "dp"),
            P(),
            P(),
            P(),
            P(),
            P(),
            P("dp", "tensor", None),
        ),
        out_specs=(
            P("dp", "tensor", None),
            P("dp", "tensor", None),
            P("dp", "tensor"),
            P("tensor"),
            P("dp", "tensor"),
            P("dp", "tensor"),
            P("tensor"),
            P("tensor", "dp"),
            P(),
            P("dp", "tensor"),
            P("tensor"),
            P("tensor", "dp"),
            P(),
            P(),
            P(),
            P(),
            P(),
        ),
        check_vma=False,
    )
```

```python
import functools

import jax
import jax.numpy as jnp
from jax import lax
from jax.experimental import pallas as pl
from jax.experimental.pallas import tpu as pltpu
from jax.sharding import PartitionSpec as P

HEAD = 64
BF = jnp.bfloat16
F32 = jnp.float32

eps_norm = 1e-12
root_half = 0.7071067811865476
density = 0.3989422804014327
scale = 0.125
log2e = 1.4426950408889634
far_score = 1e30
vmem_bytes = 60 * 1024 * 1024


def product(left, right):
    return jnp.dot(left, right, preferred_element_type=F32)


def product_nt(left, right):
    return lax.dot_general(left, right, (((1,), (1,)), ((), ())), preferred_element_type=F32)


def product_tn(left, right):
    return lax.dot_general(left, right, (((0,), (0,)), ((), ())), preferred_element_type=F32)


def normalize(values, gain, offset):
    average = jnp.mean(values, axis=-1, keepdims=True)
    centred = values - average
    inverse = lax.rsqrt(jnp.mean(centred * centred, axis=-1, keepdims=True) + eps_norm)
    normed = centred * inverse
    return (normed * gain + offset, normed, inverse)


def norm_back(upstream, normed, inverse, gain):
    scaled = upstream * gain
    centred = scaled - jnp.mean(scaled, axis=-1, keepdims=True)
    return (centred - normed * jnp.mean(scaled * normed, axis=-1, keepdims=True)) * inverse


def fold(values):
    return functools.reduce(jnp.add, [values[i : i + 8] for i in range(0, values.shape[0], 8)])


def by_chunks(rows, width, size, chunk):
    def step(i, sums):
        at = pl.ds(pl.multiple_of(i * size, size), size)
        return tuple(a + fold(b) for a, b in zip(sums, chunk(at)))

    sums = lax.fori_loop(0, rows // size, step, (jnp.zeros((8, width), F32),) * 3)
    return [jnp.sum(v, axis=0, keepdims=True) for v in sums]


def vmem():
    return pl.BlockSpec(memory_space=pltpu.VMEM)


def smem():
    return pl.BlockSpec(memory_space=pltpu.SMEM)


def params():
    return pltpu.CompilerParams(vmem_limit_bytes=vmem_bytes)


def cost(flops, moved, hard=0):
    return pl.CostEstimate(flops=int(flops), bytes_accessed=int(moved), transcendentals=int(hard))


def spec(dtype, *dims):
    return jax.ShapeDtypeStruct(dims, dtype)


def project_body(heads, *refs):
    token_refs, (weight_ref, row_bias_ref, column_bias_ref, aux_query_ref, aux_key_ref) = refs[:4], refs[4:9]
    all_ref, turned_ref, query_ref, key_ref, value_ref, value_t_ref, key_t_ref = refs[9:16]
    step = pl.program_id(0)
    width = heads * HEAD
    rows = all_ref.shape[0]

    @pl.when(step == 0)
    def _():
        turned_ref[...] = weight_ref[...].T

    for r, ref in enumerate(token_refs):

        @pl.when(step == r)
        def _(ref=ref):
            all_ref[...] = ref[:rows, :]

    tokens = all_ref[...]
    turned = (product_nt(turned_ref[...], tokens) + column_bias_ref[...]).astype(BF)
    plain = (product(tokens, weight_ref[:, width : 3 * width]) + row_bias_ref[...]).astype(BF)
    for h in range(heads):
        at = slice(h * HEAD, (h + 1) * HEAD)
        query_ref[h, :HEAD, :] = turned[at]
        query_ref[h, HEAD:, :] = aux_query_ref[...]
        key_t_ref[at, :] = turned[width : 2 * width][at]
        value_t_ref[at, :] = turned[2 * width :][at]
        key_ref[h] = jnp.concatenate([plain[:, at], aux_key_ref[...]], axis=1)
        value_ref[h] = plain[:, width + h * HEAD : width + (h + 1) * HEAD]


def project(weight, tokens, rows, row_bias, column_bias, aux_query, aux_key, heads):
    width = weight.shape[0]
    length = 4 * rows
    by_row = lambda n: pl.BlockSpec((rows, n), lambda r: (r, 0))
    headed = lambda n: pl.BlockSpec((heads, rows, n), lambda r: (0, r, 0))
    flat = pl.BlockSpec((heads * HEAD, rows), lambda r: (0, r))
    return pl.pallas_call(
        functools.partial(project_body, heads),
        grid=(4,),
        in_specs=[vmem()] * 7 + [pl.BlockSpec((HEAD, rows), lambda r: (0, r)), by_row(HEAD)],
        out_specs=[
            by_row(width),
            pl.BlockSpec((3 * heads * HEAD, width), lambda r: (0, 0)),
            pl.BlockSpec((heads, 2 * HEAD, rows), lambda r: (0, 0, r)),
            headed(2 * HEAD),
            headed(HEAD),
            flat,
            flat,
        ],
        out_shape=[
            spec(BF, length, width),
            spec(BF, 3 * heads * HEAD, width),
            spec(BF, heads, 2 * HEAD, length),
            spec(BF, heads, length, 2 * HEAD),
            spec(BF, heads, length, HEAD),
            spec(BF, heads * HEAD, length),
            spec(BF, heads * HEAD, length),
        ],
        compiler_params=params(),
        cost_estimate=cost(4 * length * width * 3 * heads * HEAD, 16 << 20),
        name="project",
    )(*tokens, weight, row_bias, column_bias, aux_query, aux_key)


def forward_body(count, key_ref, *refs):
    query_refs, value_ref, out_ref, log_ref = refs[:count], refs[count], refs[count + 1], refs[count + 2]
    chunk = key_ref.shape[1] // 4
    for i in range(count):
        query = query_refs[i][0]
        scores = [product(key_ref[0, c * chunk : (c + 1) * chunk, :], query) for c in range(4)]
        highest = None
        for c in range(4):
            peak = jnp.max(scores[c], axis=0, keepdims=True)
            now = peak if highest is None else jnp.maximum(highest, peak)
            raised = jnp.exp2((scores[c] - now) * (scale * log2e))
            part = jnp.sum(raised, axis=0, keepdims=True)
            mixed = product(value_ref[:, c * chunk : (c + 1) * chunk], raised.astype(BF))
            if highest is None:
                total, out = part, mixed
            else:
                shrink = jnp.exp2((highest - now) * (scale * log2e))
                total, out = total * shrink + part, out * shrink + mixed
            highest = now
        out_ref[i] = (out / total).astype(BF)
        log_ref[i, 0] = highest * (scale * log2e) + jnp.log2(total)


def attend_forward(keys, queries, values_t, quarters):
    heads, length, _ = keys.shape
    rows = length // 4
    count = len(quarters)
    return pl.pallas_call(
        functools.partial(forward_body, count),
        grid=(heads,),
        in_specs=[pl.BlockSpec((1, length, 2 * HEAD), lambda h: (h, 0, 0))]
        + [pl.BlockSpec((1, 2 * HEAD, rows), lambda h, q=q: (h, 0, q)) for q in quarters]
        + [pl.BlockSpec((HEAD, length), lambda h: (h, 0))],
        out_specs=[
            pl.BlockSpec((count, HEAD, rows), lambda h: (0, h, 0)),
            pl.BlockSpec((count, 1, 1, rows), lambda h: (0, h, 0, 0)),
        ],
        out_shape=[spec(BF, count, heads * HEAD, rows), spec(F32, count, heads, 1, rows)],
        compiler_params=params(),
        cost_estimate=cost(
            20 * count * heads * rows * length * HEAD, 4 << 20, heads * rows * length
        ),
        name="attend_forward",
    )(keys, *[queries] * count, values_t)


def backward_body(count, first, last, key_ref, value_ref, key_t_ref, *refs):
    groups, refs = [refs[4 * i : 4 * i + 4] for i in range(count)], refs[4 * count :]
    if not first:
        (old_dk_ref, old_dv_ref), refs = refs[:2], refs[2:]
    dq_refs, (dk_ref, dv_ref) = refs[:count], refs[count:]
    dk = dv = None
    for (query_ref, log_ref, mixed_ref, grad_ref), dq_ref in zip(groups, dq_refs):
        grad = grad_ref[...]
        delta = jnp.sum(grad.astype(F32) * mixed_ref[0].astype(F32), axis=0, keepdims=True)
        scores = product(key_ref[0], query_ref[0])
        weights = jnp.exp2(scores * (scale * log2e) - log_ref[0, 0])
        grad_weights = product(value_ref[0], grad)
        grad_scores = (weights * (grad_weights - delta)).astype(BF)
        dq_ref[...] = (product(key_t_ref[...], grad_scores) * scale).astype(BF)
        add_dk = product_nt(query_ref[0, :HEAD, :], grad_scores)
        add_dv = product_nt(grad, weights.astype(BF))
        dk = add_dk if dk is None else dk + add_dk
        dv = add_dv if dv is None else dv + add_dv
    if not first:
        dk = dk + old_dk_ref[...]
        dv = dv + old_dv_ref[...]
    if last:
        dk = dk * scale
    dk_ref[...] = dk.astype(dk_ref.dtype)
    dv_ref[...] = dv.astype(dv_ref.dtype)


def attend_back(operands, quarters, logs, mixed, grads, carried, last):
    keys, queries, values, keys_t = operands
    heads, length, _ = keys.shape
    rows = length // 4
    first = carried is None
    flat = lambda n: pl.BlockSpec((HEAD, n), lambda h: (h, 0))
    by_head = lambda *dims: pl.BlockSpec((1,) + dims, lambda h: (h, 0, 0))
    in_specs = [by_head(length, 2 * HEAD), by_head(length, HEAD), flat(length)]
    args = [keys, values, keys_t]
    for q, (log, i), (out, j), grad in zip(quarters, logs, mixed, grads):
        in_specs += [
            pl.BlockSpec((1, 2 * HEAD, rows), lambda h, q=q: (h, 0, q)),
            pl.BlockSpec((1, 1, 1, rows), lambda h, i=i: (i, h, 0, 0)),
            pl.BlockSpec((1, HEAD, rows), lambda h, j=j: (j, h, 0)),
            flat(rows),
        ]
        args += [queries, log, out, grad]
    count = len(quarters)
    aliases = {}
    if not first:
        if not last:
            aliases = {len(args): count, len(args) + 1: count + 1}
        in_specs += [flat(length)] * 2
        args += list(carried)
    kind = BF if last else F32
    outs = pl.pallas_call(
        functools.partial(backward_body, count, first, last),
        grid=(heads,),
        in_specs=in_specs,
        out_specs=[flat(rows)] * count + [flat(length)] * 2,
        out_shape=[spec(BF, heads * HEAD, rows)] * count + [spec(kind, heads * HEAD, length)] * 2,
        input_output_aliases=aliases,
        compiler_params=params(),
        cost_estimate=cost(
            50 * count * heads * rows * length * HEAD, 8 << 20, count * heads * rows * length
        ),
        name="attend_back",
    )(*args)
    return outs[:count], outs[count:]


def side_copies(meta_ref, bundle_ref, held_ref, sems, start):
    lanes = pl.ds(start, held_ref.shape[2])
    return [
        pltpu.make_async_copy(bundle_ref.at[meta_ref[0] ^ g, :, lanes], held_ref.at[g], sems.at[g])
        for g in range(4)
    ]


def side_wait(bundle_ref, held_ref, sems, start, group):
    lanes = pl.ds(start, held_ref.shape[2])
    pltpu.make_async_copy(bundle_ref.at[0, :, lanes], held_ref.at[group], sems.at[group]).wait()


def down_copies(meta_ref, down_refs, held_ref, sems):
    parts = len(down_refs) // 4
    copies = []
    for g in range(4):
        for b in range(parts):
            ref = down_refs[parts * g + b]
            blocks, shard, _ = ref.shape
            for k in range(blocks):
                at = held_ref.at[g]
                if parts > 1:
                    place = pl.multiple_of(((2 * k + b) ^ meta_ref[2]) * shard, shard)
                    at = held_ref.at[g, pl.ds(place, shard)]
                copies.append(pltpu.make_async_copy(ref.at[k], at, sems.at[g]))
    return copies


def down_group(held_ref, sems, group):
    pltpu.make_async_copy(held_ref.at[group], held_ref.at[group], sems.at[group]).wait()
    return held_ref[group]


def held(*dims):
    return [pltpu.VMEM((4, *dims), BF), pltpu.SemaphoreType.DMA((4,))]


def unmoved():
    return pl.BlockSpec(memory_space=pl.ANY)


def gelu_parts(inner):
    both = 0.5 * (1.0 + lax.erf(inner * root_half))
    slope = both + inner * density * jnp.exp(-0.5 * inner * inner)
    return (inner * both).astype(BF), slope.astype(BF)


def group_spec(rows, units):
    return pl.BlockSpec((1, rows, units), lambda t: (t, 0, 0))


def fixed(*dims):
    return pl.BlockSpec(dims, lambda t: (0,) * len(dims))


def enter_body(units, meta_ref, bundle_ref, *refs):
    mixed_refs, (own_ref, out_bias_ref, gain_ref, shift_ref, bias_ref) = refs[:4], refs[4:9]
    low_ref, unit_ref, inverse_ref, act_ref, slope_ref = refs[9:14]
    out_ref, out_sems, up_ref, up_sems = refs[14:]
    group = pl.program_id(0)

    @pl.when(group == 0)
    def _():
        copies = side_copies(meta_ref, bundle_ref, out_ref, out_sems, units)
        for copy in copies + side_copies(meta_ref, bundle_ref, up_ref, up_sems, 0):
            copy.start()
        hidden = own_ref[...].astype(F32) + out_bias_ref[...]
        for copy in copies:
            copy.wait()
        for j, ref in enumerate(mixed_refs):
            hidden = hidden + product_nt(ref[0].T, out_ref[j])
        first, unit, inverse = normalize(hidden, gain_ref[...], shift_ref[...])
        unit_ref[...] = unit
        inverse_ref[...] = inverse
        low_ref[...] = first.astype(BF)

    side_wait(bundle_ref, up_ref, up_sems, 0, group)
    low = low_ref[...]
    step = units // 3
    for c in range(0, units, step):
        lanes = slice(c, c + step)
        inner = product(low, up_ref[group, :, lanes]) + bias_ref[0, :, lanes]
        act_ref[0, :, lanes], slope_ref[0, :, lanes] = gelu_parts(inner)


def enter(meta, bundle, mixed, own, out_bias, gain, shift, bias):
    rows, width = own.shape
    groups, _, units = bias.shape
    return pl.pallas_call(
        functools.partial(enter_body, units),
        grid=(groups,),
        in_specs=[smem(), unmoved()]
        + [pl.BlockSpec((1, *v.shape[1:]), lambda t: (0, 0, 0)) for v in mixed]
        + [vmem()] * 4
        + [group_spec(1, units)],
        out_specs=[fixed(rows, width), fixed(rows, width), fixed(rows, 1)]
        + [group_spec(rows, units)] * 2,
        out_shape=[spec(BF, rows, width), spec(F32, rows, width), spec(F32, rows, 1)]
        + [spec(BF, groups, rows, units)] * 2,
        scratch_shapes=held(width, mixed[0].shape[1]) + held(width, units),
        compiler_params=params(),
        cost_estimate=cost(12 * rows * width * units, 20 << 20, 8 * rows * units),
        name="enter",
    )(meta, bundle, *mixed, own, out_bias, gain, shift, bias)


def turn_body(count, meta_ref, *refs):
    down_refs, act_ref, refs = refs[:count], refs[count], refs[count + 1 :]
    unit_ref, first_gain_ref, first_shift_ref, bias_ref, gain_ref, shift_ref, up_ref = refs[:7]
    out_ref, grad_ref, low_ref, sums_ref, total_ref, down_ref, sems = refs[7:]
    step = pl.program_id(0)

    @pl.when(step == 0)
    def _():
        for copy in down_copies(meta_ref, down_refs, down_ref, sems):
            copy.start()

    part = product_nt(act_ref[0], down_group(down_ref, sems, step))

    @pl.when(step == 0)
    def _():
        total_ref[...] = part

    @pl.when(step > 0)
    def _():
        total_ref[...] += part

    @pl.when(step == pl.num_programs(0) - 1)
    def _():
        def chunk(at):
            first = unit_ref[at, :] * first_gain_ref[...] + first_shift_ref[...]
            second, unit, inverse = normalize(
                first + total_ref[at, :] + bias_ref[...], gain_ref[...], shift_ref[...]
            )
            out_ref[at, :] = second.astype(BF)
            upstream = up_ref[at, :].astype(F32)
            grad = norm_back(upstream, unit, inverse, gain_ref[...])
            grad_ref[at, :] = grad
            low_ref[at, :] = grad.astype(BF)
            return grad, upstream * unit, upstream

        sums = by_chunks(total_ref.shape[0], total_ref.shape[1], 64, chunk)
        for k in range(3):
            sums_ref[k : k + 1, :] = sums[k]


def turn(meta, downs, acts, unit, first_gain, first_shift, bias, gain, shift, cotangent):
    rows, width = unit.shape
    groups, _, units = acts.shape
    return pl.pallas_call(
        functools.partial(turn_body, len(downs)),
        grid=(groups,),
        in_specs=[smem()] + [unmoved()] * len(downs) + [group_spec(rows, units)] + [vmem()] * 7,
        out_specs=[fixed(rows, width)] * 3 + [fixed(3, width)],
        out_shape=[
            spec(BF, rows, width),
            spec(F32, rows, width),
            spec(BF, rows, width),
            spec(F32, 3, width),
        ],
        scratch_shapes=[pltpu.VMEM((rows, width), F32)] + held(width, units),
        compiler_params=params(),
        cost_estimate=cost(8 * rows * width * units, 16 << 20),
        name="turn",
    )(meta, *downs, acts, unit, first_gain, first_shift, bias, gain, shift, cotangent)


def leave_body(units, count, meta_ref, bundle_ref, *refs):
    down_refs, refs = refs[:count], refs[count:]
    slope_ref, low_ref, second_ref, unit_ref, inverse_ref, gain_ref = refs[:6]
    inner_ref, hidden_ref, attn_ref, own_ref, next_ref, far_rows_ref, sums_ref = refs[6:13]
    out_ref, out_sems, up_ref, up_sems, down_ref, down_sems = refs[13:]
    step = pl.program_id(0)

    @pl.when(step == 0)
    def _():
        copies = down_copies(meta_ref, down_refs, down_ref, down_sems)
        copies += side_copies(meta_ref, bundle_ref, up_ref, up_sems, 0)
        copies += side_copies(meta_ref, bundle_ref, out_ref, out_sems, units)
        for copy in copies:
            copy.start()
        hidden_ref[...] = second_ref[...]

    down = down_group(down_ref, down_sems, step)
    grad = product(low_ref[...], down) * slope_ref[0].astype(F32)
    inner = grad.astype(BF)
    inner_ref[0] = inner
    total_inner = jnp.sum(inner.astype(F32), axis=0, keepdims=True)
    sums_ref[pl.ds(3 + (meta_ref[0] ^ step), 1), :] = total_inner
    side_wait(bundle_ref, up_ref, up_sems, 0, step)
    hidden_ref[...] += product_nt(inner, up_ref[step])

    @pl.when(step == pl.num_programs(0) - 1)
    def _():
        for copy in side_copies(meta_ref, bundle_ref, out_ref, out_sems, units):
            copy.wait()
        back = hidden_ref[...]
        unit = unit_ref[...]
        hidden = norm_back(back, unit, inverse_ref[...], gain_ref[...])
        hidden_ref[...] = hidden
        sums_ref[0:1, :] = jnp.sum(hidden, axis=0, keepdims=True)
        sums_ref[1:2, :] = jnp.sum(back * unit, axis=0, keepdims=True)
        sums_ref[2:3, :] = jnp.sum(back, axis=0, keepdims=True)
        attn = hidden.astype(BF)
        attn_ref[...] = attn
        for j in range(4):
            mixed = product(attn, out_ref[j]).T.astype(BF)
            if j == 0:
                own_ref[...] = mixed
            elif j == 1:
                next_ref[...] = mixed
            else:
                far_rows_ref[j - 2] = mixed


def leave(meta, bundle, downs, slopes, low, second, unit, inverse, gain):
    rows, width = low.shape
    groups, _, units = slopes.shape
    feats = bundle.shape[2] - units
    return pl.pallas_call(
        functools.partial(leave_body, units, len(downs)),
        grid=(groups,),
        in_specs=[smem()] + [unmoved()] * (1 + len(downs)) + [group_spec(rows, units)] + [vmem()] * 5,
        out_specs=[
            group_spec(rows, units),
            fixed(rows, width),
            fixed(rows, width),
            fixed(feats, rows),
            fixed(feats, rows),
            fixed(2, feats, rows),
            fixed(3 + groups, width),
        ],
        out_shape=[
            spec(BF, groups, rows, units),
            spec(F32, rows, width),
            spec(BF, rows, width),
            spec(BF, feats, rows),
            spec(BF, feats, rows),
            spec(BF, 2, feats, rows),
            spec(F32, 3 + groups, width),
        ],
        scratch_shapes=held(width, feats) + held(width, units) + held(width, units),
        compiler_params=params(),
        cost_estimate=cost(16 * rows * width * units, 28 << 20),
        name="leave",
    )(meta, bundle, *downs, slopes, low, second, unit, inverse, gain)


def outer_body(shard, extra, keep, meta_ref, left_ref, right_ref, *refs):
    if extra:
        attn_ref, mixed_refs, sum_refs, refs = refs[0], refs[1:3], refs[3:5], refs[5:]
    if keep:
        arrived_ref, refs = refs[0], refs[1:]
        left_t_ref, attn_t_ref = left_ref, attn_ref if extra else None
    else:
        left_t_ref, attn_t_ref = refs[1], refs[2] if extra else None
    out_ref = refs[0]
    step = pl.program_id(0)
    units = right_ref.shape[2]
    width = left_t_ref.shape[0]
    pairs = width // shard // 2
    lanes = out_ref.shape[3]

    if not keep:

        @pl.when(step == 0)
        def _():
            left_t_ref[...] = left_ref[...].T
            if extra:
                attn_t_ref[...] = attn_ref[...].T

    def put(low, rows, lane, values):
        if keep:
            values = values + arrived_ref[low, 0, rows, lane].astype(F32)
        out_ref[low, 0, rows, lane] = values.astype(BF)

    def spread(values, lane):
        for block in range(2 * pairs):
            rows = slice(block // 2 * shard, (block // 2 + 1) * shard)
            put(block % 2, rows, lane, values[block * shard : (block + 1) * shard])

    spread(product(left_t_ref[...], right_ref[0]), slice(0, units))
    if extra:
        for j in range(2):

            @pl.when(step ^ (meta_ref[0] // 2) == j)
            def _(j=j):
                spread(product_nt(attn_t_ref[...], mixed_refs[j][0]), slice(units, lanes))

        sums = jnp.concatenate(
            [sum_refs[0][...], sum_refs[1][...], jnp.zeros((16 - 10, width), F32)], axis=0
        )
        for low in range(2):
            put(low, slice(pairs * shard, pairs * shard + 16), slice(0, width), sums)
            out_ref[low, 0, pairs * shard :, width:lanes] = jnp.zeros((16, lanes - width), BF)


def outer(meta, shard, left, rights, attn=None, mixed=(), sums=(), arrived=None):
    keep = arrived is not None
    rows, width = left.shape[::-1] if keep else left.shape
    groups, _, units = rights.shape
    extra = attn is not None
    feats = mixed[0].shape[1] if extra else 0
    depth = width // 2 + (16 if extra else 0)

    def group(i, meta_ref):
        return 2 * (i ^ (meta_ref[0] // 2)) + (0 if keep else 1)

    args = [left, rights] + ([attn, *mixed, *sums] if extra else [])
    block = pl.BlockSpec((2, 1, depth, units + feats), lambda i, m: (0, i, 0, 0))
    turned = [] if keep else [left, attn] if extra else [left]
    grid_spec = pltpu.PrefetchScalarGridSpec(
        num_scalar_prefetch=1,
        grid=(2,),
        in_specs=[vmem(), pl.BlockSpec((1, rows, units), lambda i, m: (group(i, m), 0, 0))]
        + ([vmem()] if extra else [])
        + [pl.BlockSpec((1, *v.shape[1:]), lambda i, m: (0, 0, 0)) for v in mixed]
        + [vmem()] * len(sums)
        + ([block] if keep else []),
        out_specs=[block] + [vmem()] * len(turned),
    )
    return pl.pallas_call(
        functools.partial(outer_body, shard, extra, keep),
        grid_spec=grid_spec,
        out_shape=[spec(BF, 2, 2, depth, units + feats)] + [spec(BF, width, rows) for _ in turned],
        compiler_params=params(),
        cost_estimate=cost(4 * rows * width * units, 8 << 20),
        name="outer",
    )(meta, *args, *([arrived] if keep else []))


def inputs_body(*refs):
    dq_refs, (dk_ref, dv_ref, turned_ref) = refs[:4], refs[4:7]
    own_ref, next_ref, out_ref = refs[7:10]
    rows = dq_refs[0].shape[1]
    weight = turned_ref[...]
    for r in (1, 3, 0, 2):
        at = slice(r * rows, (r + 1) * rows)
        grad = jnp.concatenate([dq_refs[r][...], dk_ref[:, at], dv_ref[:, at]], axis=0)
        back = product(grad.T, weight)
        if r == 0:
            own_ref[...] = back
        elif r == 2:
            next_ref[...] = back
        else:
            out_ref[(r // 2) * rows : (r // 2 + 1) * rows, :] = back.astype(BF)


def input_grads(dq, dk, dv, turned):
    rows = dq[0].shape[1]
    width = turned.shape[1]
    return pl.pallas_call(
        inputs_body,
        in_specs=[vmem()] * 7,
        out_specs=[vmem()] * 3,
        out_shape=[spec(F32, rows, width), spec(F32, rows, width), spec(BF, 2 * rows, width)],
        compiler_params=params(),
        cost_estimate=cost(8 * rows * width * width, 12 << 20),
        name="input_grads",
    )(*dq, dk, dv, turned)


def projections_body(shard, *refs):
    meta_ref, dq_refs, (dk_ref, dv_ref, all_ref, keep_ref, send_ref) = refs[0], refs[1:5], refs[5:10]
    held_ref = refs[10]
    rows = dq_refs[0].shape[1]
    depth = keep_ref.shape[0] - 16
    grad = jnp.concatenate(
        [jnp.concatenate([ref[...] for ref in dq_refs], axis=1), dk_ref[...], dv_ref[...]], axis=0
    )
    held_ref[...] = product(grad, all_ref[...]).T.astype(BF)
    sums = product_nt(jnp.ones((16, 4 * rows), BF), grad).astype(BF)
    for flip, out_ref in ((0, keep_ref), (1, send_ref)):
        for i in range(depth // shard):
            block = 2 * i + (meta_ref[1] ^ flip)
            if shard % 16 == 0:
                start = pl.multiple_of(block * shard, shard)
                out_ref[i * shard : (i + 1) * shard, :] = held_ref[pl.ds(start, shard), :]
            else:
                even = held_ref[2 * i * shard : (2 * i + 1) * shard, :]
                odd = held_ref[(2 * i + 1) * shard : (2 * i + 2) * shard, :]
                out_ref[i * shard : (i + 1) * shard, :] = jnp.where(block % 2 == 0, even, odd)
        out_ref[depth:, :] = sums


def projection_grads(meta, shard, dq, dk, dv, tokens):
    width = tokens.shape[1]
    feats = dq[0].shape[0]
    return pl.pallas_call(
        functools.partial(projections_body, shard),
        in_specs=[smem()] + [vmem()] * 7,
        out_specs=[vmem()] * 2,
        out_shape=[spec(BF, width // 2 + 16, 3 * feats)] * 2,
        scratch_shapes=[pltpu.VMEM((width, 3 * feats), BF)],
        compiler_params=params(),
        cost_estimate=cost(2 * tokens.shape[0] * width * 3 * feats, 12 << 20),
        name="projection_grads",
    )(meta, *dq, dk, dv, tokens)


def exchanger(axis_dp, axis_tensor):
    def swap(values, dp_bits, tensor_bits):
        pairs = [
            (d * axis_tensor + t, (d ^ dp_bits) * axis_tensor + (t ^ tensor_bits))
            for d in range(axis_dp)
            for t in range(axis_tensor)
        ]
        return lax.ppermute(values, ("dp", "tensor"), pairs)

    return swap


def tie(*values):
    return lax.optimization_barrier(values)


def add(left, right):
    return (left.astype(F32) + right.astype(F32)).astype(BF)


def total(parts):
    return functools.reduce(jnp.add, [parts[i].astype(F32) for i in range(parts.shape[0])])


def local(
    axis_dp,
    axis_tensor,
    inputs,
    segments,
    query_weight,
    query_bias,
    key_weight,
    value_weight,
    value_bias,
    output_weight,
    output_bias,
    up_weight,
    up_bias,
    down_weight,
    down_bias,
    first_gain,
    first_shift,
    second_gain,
    second_shift,
    cotangent,
):
    swap = exchanger(axis_dp, axis_tensor)
    place_dp, place_tensor = lax.axis_index("dp"), lax.axis_index("tensor")
    meta = jnp.stack([place_tensor, place_dp % 2, place_dp]).astype(jnp.int32)
    rows, width = inputs.shape[1:]
    shard = query_weight.shape[0]
    feats = output_weight.shape[0]
    heads = feats // HEAD
    units = up_weight.shape[1]
    pairs = axis_dp // 2
    row = lambda v: v.reshape(1, -1).astype(F32)
    flat = lambda z, x, y, c: (2 * z + x) * axis_tensor + 2 * y + c
    near_groups = [
        [flat(z, x, y, c) for x in range(2) for y in range(2)] for z in range(pairs) for c in range(2)
    ]
    deep_groups = [[2 * z + x for z in range(pairs)] for x in range(2)]

    own = inputs[0]
    notes = jnp.zeros((16, width), BF)
    notes = notes.at[0, :rows].set(segments[0].astype(BF)).at[1, :units].set(up_bias)
    message = jnp.concatenate([own, notes])
    across = swap(message, 0, 2)
    bundle = jnp.concatenate([query_weight, key_weight, value_weight], axis=1)
    copies = jnp.broadcast_to(bundle[None], (axis_dp,) + bundle.shape)
    qkv_weight = lax.all_to_all(copies, "dp", 0, 0, tiled=True).reshape(width, 3 * feats)
    near = swap(message, 0, 1)
    far = swap(across, 0, 1)
    tokens = [message, near, across, far]

    up_bundle = lax.all_gather(
        jnp.concatenate([up_weight, output_weight.T], axis=1), ("tensor", "dp"), axis=0, tiled=True
    ).reshape(axis_tensor, width, units + feats)
    down = down_weight.T
    around = jnp.stack([down] + [swap(down, 2 * k, 0) for k in range(1, pairs)])
    across_around = swap(around, 0, 2)
    qkv_weight, around_late = tie(qkv_weight, around)
    beside = swap(around_late, 1, 0)

    noted = jnp.stack([v[rows:] for v in tokens]).astype(F32)
    docs = noted[:, 0, :rows].reshape(-1)
    bias = noted[:, 1:2, :units]
    lane = jnp.arange(HEAD, dtype=F32)
    same = docs[:, None] == lane[None, :]
    aux_query = (docs[None, :] == lane[:, None]).astype(BF)
    aux_key = jnp.where(same | (lane[None, :] >= 8), 0.0, -far_score).astype(BF)
    output_bias, first_gain, first_shift, down_bias, second_gain, second_shift, bias, aux_key = tie(
        *[row(v) for v in (output_bias, first_gain, first_shift, down_bias, second_gain, second_shift)],
        bias, aux_key,
    )
    qkv_bias = jnp.concatenate([query_bias, jnp.zeros_like(query_bias), value_bias]).astype(F32)
    all_tokens, turned, queries, keys, values, values_t, keys_t = project(
        qkv_weight, tokens, rows, qkv_bias[feats:].reshape(1, -1), qkv_bias.reshape(-1, 1),
        aux_query, aux_key, heads,
    )

    mixed23, log23 = attend_forward(keys, queries, values_t, (2, 3))
    queries, mixed23 = tie(queries, mixed23)
    arrived = swap(mixed23, 0, 2)
    _, around_late, across_around = tie(mixed23, around_late, across_around)
    columns = [around, None, swap(around_late, 0, 1), None, across_around, None]
    columns += [swap(across_around, 0, 1), None]
    mixed1, log1 = attend_forward(keys, queries, values_t, (1,))
    queries, mixed1 = tie(queries, mixed1)
    arrived1 = swap(mixed1, 0, 1)
    _, beside = tie(mixed1, beside)
    across_beside = swap(beside, 0, 2)
    queries, arrived = tie(queries, arrived)
    arrived3 = swap(arrived[1:], 0, 1)
    mixed0, log0 = attend_forward(keys, queries, values_t, (0,))
    mixed = [mixed0, arrived1, arrived, arrived3]

    _, later = tie(mixed0, across_beside)
    columns[1::2] = [beside, swap(beside, 0, 1), across_beside, swap(later, 0, 1)]
    downs = columns
    if shard % 16:
        order = [2 * k + b for b in range(2) for k in range(pairs)]
        places = jnp.argsort(jnp.array(order) ^ place_dp)
        downs = [jnp.concatenate(columns[2 * g : 2 * g + 2]) for g in range(4)]
        downs = [v[places].reshape(1, width, units) for v in downs]

    low, unit_first, inverse_first, acts, slopes = enter(
        meta, up_bundle, mixed, own, output_bias, first_gain, first_shift, bias
    )
    layer_out, grad_second, second_low, sums_second = turn(
        meta, downs, acts, unit_first, first_gain, first_shift,
        down_bias, second_gain, second_shift, cotangent[0],
    )
    send_b, second_t = outer(meta, shard, second_low, acts)
    second_low, send_b = tie(second_low, send_b)
    moved_b = swap(send_b, 0, 1)
    inners, grad_hidden, grad_attn, grad0, next_mixed, far_mixed, sums_first = leave(
        meta, up_bundle, downs, slopes, second_low, grad_second, unit_first, inverse_first, first_gain
    )

    def reduce_near(values):
        values = values.reshape((4,) + values.shape[2:])
        return lax.all_to_all(values, ("dp", "tensor"), 0, 0, axis_index_groups=near_groups, tiled=True)

    def reduce_deep(values):
        return lax.all_to_all(values, "dp", 0, 0, axis_index_groups=deep_groups, tiled=True)

    def deep_parts(values):
        return values[: pairs * shard].reshape(pairs, shard, -1)

    def part_at(parts, k):
        return lax.dynamic_index_in_dim(parts, (place_dp // 2) ^ k, 0, False)

    arrived_g = swap(far_mixed, 0, 2)
    g1 = swap(next_mixed, 0, 1)
    (part_b,) = outer(meta, shard, second_t, acts, arrived=moved_b)
    inners, part_b = tie(inners, part_b)
    near_b = reduce_near(part_b)
    sums_both = (sums_first, sums_second)
    send_a, low_t, attn_t = outer(meta, shard, low, inners, grad_attn, mixed[1::2], sums_both)
    grad0, send_a, g1, arrived_g = tie(grad0, send_a, g1, arrived_g)
    moved_a = swap(send_a, 0, 1)
    g2, g3 = arrived_g[0], swap(arrived_g[1], 0, 1)
    operands = (keys, queries, values, keys_t)
    (dq0, dq1), carried = attend_back(
        operands, (0, 1), ((log0, 0), (log1, 0)), ((mixed0, 0), (mixed1, 0)), (grad0, g1), None, False
    )
    low_t, carried, moved_a = tie(low_t, carried, moved_a)
    (part_a,) = outer(meta, shard, low_t, inners, attn_t, mixed[::2], sums_both, moved_a)
    carried, part_a, near_b, g2, g3 = tie(carried, part_a, near_b, g2, g3)
    near_a = reduce_near(part_a)
    parts_b = deep_parts(total(near_b).astype(BF))
    sent_b = [part_at(parts_b, k) for k in range(1, pairs)]
    carried, parts_b, *sent_b = tie(carried, parts_b, *sent_b)
    own_b = part_at(parts_b, 0).astype(F32)
    for k in range(1, pairs):
        own_b = own_b + swap(sent_b[k - 1], 2 * k, 0).astype(F32)
    (dq2, dq3), (dk, dv) = attend_back(
        operands, (2, 3), ((log23, 0), (log23, 1)), ((mixed23, 0), (mixed23, 1)), (g2, g3), carried, True
    )
    dq2, own_b = tie(dq2, own_b)
    dq = (dq0, dq1, dq2, dq3)
    own_rows, next_rows, sent_rows = input_grads(dq, dk, dv, turned)
    moved = swap(sent_rows, 0, 1)
    dk, sent_rows = tie(dk, sent_rows)
    keep_c, send_c = projection_grads(meta, shard, dq, dk, dv, all_tokens)
    _, moved = tie(send_c, moved)
    next_rows = add(next_rows, moved[rows:])
    arrived_c = swap(send_c, 1, 0)
    arrived_rows = swap(next_rows, 0, 2)
    _, _, near_a = tie(send_c, next_rows, near_a)
    sum_a = total(near_a).astype(BF)
    notes = jnp.broadcast_to(sum_a[None, pairs * shard :], (pairs, 16, sum_a.shape[1]))
    packed_a = jnp.concatenate([deep_parts(sum_a), notes], axis=1)
    deep_a = reduce_deep(packed_a)
    _, arrived_c = tie(packed_a, arrived_c)
    sum_c, arrived_rows = tie(add(keep_c, arrived_c), arrived_rows)
    parts_c, notes = deep_parts(sum_c), sum_c[pairs * shard :]
    own_c = jnp.concatenate([part_at(parts_c, 0), notes]).astype(F32)
    for k in range(1, pairs):
        own_c = own_c + swap(jnp.concatenate([part_at(parts_c, k), notes]), 2 * k, 0).astype(F32)
    own_a = total(deep_a)
    grad_inputs = grad_hidden + own_rows + moved[:rows].astype(F32) + arrived_rows.astype(F32)
    sums = own_a[shard:, :width]
    sum_up = lax.dynamic_index_in_dim(sums[3:7], place_tensor, 0, False)
    head_sums = own_c[shard]

    return (
        layer_out[None],
        grad_inputs[None],
        own_c[:shard, :feats],
        head_sums[:feats],
        own_c[:shard, feats : 2 * feats],
        own_c[:shard, 2 * feats :],
        head_sums[2 * feats :],
        own_a[:shard, units:].T,
        sums[0],
        own_a[:shard, :units],
        sum_up,
        own_b.T,
        sums[7],
        sums[1],
        sums[2],
        sums[8],
        sums[9],
    )


def solution(mesh):
    axis_dp, axis_tensor = mesh.shape["dp"], mesh.shape["tensor"]
    if axis_tensor != 4 or axis_dp < 2 or axis_dp & (axis_dp - 1):
        raise ValueError("mesh sizes")
    return jax.shard_map(
        functools.partial(local, axis_dp, axis_tensor),
        mesh=mesh,
        in_specs=(
            P("dp", "tensor", None),
            P("dp", "tensor"),
            P("dp", "tensor"),
            P("tensor"),
            P("dp", "tensor"),
            P("dp", "tensor"),
            P("tensor"),
            P("tensor", "dp"),
            P(),
            P("dp", "tensor"),
            P("tensor"),
            P("tensor", "dp"),
            P(),
            P(),
            P(),
            P(),
            P(),
            P("dp", "tensor", None),
        ),
        out_specs=(
            P("dp", "tensor", None),
            P("dp", "tensor", None),
            P("dp", "tensor"),
            P("tensor"),
            P("dp", "tensor"),
            P("dp", "tensor"),
            P("tensor"),
            P("tensor", "dp"),
            P(),
            P("dp", "tensor"),
            P("tensor"),
            P("tensor", "dp"),
            P(),
            P(),
            P(),
            P(),
            P(),
        ),
        check_vma=False,
    )
```

```python
import functools

import jax
import jax.numpy as jnp
from jax import lax
from jax.experimental import pallas as pl
from jax.experimental.pallas import tpu as pltpu
from jax.sharding import PartitionSpec as P

HEAD = 64
BF = jnp.bfloat16
F32 = jnp.float32

eps_norm = 1e-12
root_half = 0.7071067811865476
density = 0.3989422804014327
scale = 0.125
log2e = 1.4426950408889634
far_score = 1e30
vmem_bytes = 60 * 1024 * 1024


def product(left, right):
    return jnp.dot(left, right, preferred_element_type=F32)


def product_nt(left, right):
    return lax.dot_general(left, right, (((1,), (1,)), ((), ())), preferred_element_type=F32)


def product_tn(left, right):
    return lax.dot_general(left, right, (((0,), (0,)), ((), ())), preferred_element_type=F32)


def normalize(values, gain, offset):
    average = jnp.mean(values, axis=-1, keepdims=True)
    centred = values - average
    inverse = lax.rsqrt(jnp.mean(centred * centred, axis=-1, keepdims=True) + eps_norm)
    normed = centred * inverse
    return (normed * gain + offset, normed, inverse)


def norm_back(upstream, normed, inverse, gain):
    scaled = upstream * gain
    centred = scaled - jnp.mean(scaled, axis=-1, keepdims=True)
    return (centred - normed * jnp.mean(scaled * normed, axis=-1, keepdims=True)) * inverse


def fold(values):
    return functools.reduce(jnp.add, [values[i : i + 8] for i in range(0, values.shape[0], 8)])


def by_chunks(rows, width, size, chunk):
    def step(i, sums):
        at = pl.ds(pl.multiple_of(i * size, size), size)
        return tuple(a + fold(b) for a, b in zip(sums, chunk(at)))

    sums = lax.fori_loop(0, rows // size, step, (jnp.zeros((8, width), F32),) * 3)
    return [jnp.sum(v, axis=0, keepdims=True) for v in sums]


def vmem():
    return pl.BlockSpec(memory_space=pltpu.VMEM)


def smem():
    return pl.BlockSpec(memory_space=pltpu.SMEM)


def params():
    return pltpu.CompilerParams(vmem_limit_bytes=vmem_bytes)


def cost(flops, moved, hard=0):
    return pl.CostEstimate(flops=int(flops), bytes_accessed=int(moved), transcendentals=int(hard))


def spec(dtype, *dims):
    return jax.ShapeDtypeStruct(dims, dtype)


def project_body(heads, *refs):
    token_refs, (weight_ref, row_bias_ref, column_bias_ref, aux_query_ref, aux_key_ref) = refs[:4], refs[4:9]
    all_ref, turned_ref, query_ref, key_ref, value_ref, value_t_ref, key_t_ref = refs[9:16]
    step = pl.program_id(0)
    width = heads * HEAD
    rows = all_ref.shape[0]

    @pl.when(step == 0)
    def _():
        turned_ref[...] = weight_ref[...].T

    for r, ref in enumerate(token_refs):

        @pl.when(step == r)
        def _(ref=ref):
            all_ref[...] = ref[:rows, :]

    tokens = all_ref[...]
    turned = (product_nt(turned_ref[...], tokens) + column_bias_ref[...]).astype(BF)
    plain = (product(tokens, weight_ref[:, width : 3 * width]) + row_bias_ref[...]).astype(BF)
    for h in range(heads):
        at = slice(h * HEAD, (h + 1) * HEAD)
        query_ref[h, :HEAD, :] = turned[at]
        query_ref[h, HEAD:, :] = aux_query_ref[...]
        key_t_ref[at, :] = turned[width : 2 * width][at]
        value_t_ref[at, :] = turned[2 * width :][at]
        key_ref[h] = jnp.concatenate([plain[:, at], aux_key_ref[...]], axis=1)
        value_ref[h] = plain[:, width + h * HEAD : width + (h + 1) * HEAD]


def project(weight, tokens, rows, row_bias, column_bias, aux_query, aux_key, heads):
    width = weight.shape[0]
    length = 4 * rows
    by_row = lambda n: pl.BlockSpec((rows, n), lambda r: (r, 0))
    headed = lambda n: pl.BlockSpec((heads, rows, n), lambda r: (0, r, 0))
    flat = pl.BlockSpec((heads * HEAD, rows), lambda r: (0, r))
    return pl.pallas_call(
        functools.partial(project_body, heads),
        grid=(4,),
        in_specs=[vmem()] * 7 + [pl.BlockSpec((HEAD, rows), lambda r: (0, r)), by_row(HEAD)],
        out_specs=[
            by_row(width),
            pl.BlockSpec((3 * heads * HEAD, width), lambda r: (0, 0)),
            pl.BlockSpec((heads, 2 * HEAD, rows), lambda r: (0, 0, r)),
            headed(2 * HEAD),
            headed(HEAD),
            flat,
            flat,
        ],
        out_shape=[
            spec(BF, length, width),
            spec(BF, 3 * heads * HEAD, width),
            spec(BF, heads, 2 * HEAD, length),
            spec(BF, heads, length, 2 * HEAD),
            spec(BF, heads, length, HEAD),
            spec(BF, heads * HEAD, length),
            spec(BF, heads * HEAD, length),
        ],
        compiler_params=params(),
        cost_estimate=cost(4 * length * width * 3 * heads * HEAD, 16 << 20),
        name="project",
    )(*tokens, weight, row_bias, column_bias, aux_query, aux_key)


def forward_body(count, key_ref, *refs):
    query_refs, value_ref, out_ref, log_ref = refs[:count], refs[count], refs[count + 1], refs[count + 2]
    chunk = key_ref.shape[1] // 4
    for i in range(count):
        query = query_refs[i][0]
        scores = [product(key_ref[0, c * chunk : (c + 1) * chunk, :], query) for c in range(4)]
        highest = None
        for c in range(4):
            peak = jnp.max(scores[c], axis=0, keepdims=True)
            now = peak if highest is None else jnp.maximum(highest, peak)
            raised = jnp.exp2((scores[c] - now) * (scale * log2e))
            part = jnp.sum(raised, axis=0, keepdims=True)
            mixed = product(value_ref[:, c * chunk : (c + 1) * chunk], raised.astype(BF))
            if highest is None:
                total, out = part, mixed
            else:
                shrink = jnp.exp2((highest - now) * (scale * log2e))
                total, out = total * shrink + part, out * shrink + mixed
            highest = now
        out_ref[i] = (out / total).astype(BF)
        log_ref[i, 0] = highest * (scale * log2e) + jnp.log2(total)


def attend_forward(keys, queries, values_t, quarters):
    heads, length, _ = keys.shape
    rows = length // 4
    count = len(quarters)
    return pl.pallas_call(
        functools.partial(forward_body, count),
        grid=(heads,),
        in_specs=[pl.BlockSpec((1, length, 2 * HEAD), lambda h: (h, 0, 0))]
        + [pl.BlockSpec((1, 2 * HEAD, rows), lambda h, q=q: (h, 0, q)) for q in quarters]
        + [pl.BlockSpec((HEAD, length), lambda h: (h, 0))],
        out_specs=[
            pl.BlockSpec((count, HEAD, rows), lambda h: (0, h, 0)),
            pl.BlockSpec((count, 1, 1, rows), lambda h: (0, h, 0, 0)),
        ],
        out_shape=[spec(BF, count, heads * HEAD, rows), spec(F32, count, heads, 1, rows)],
        compiler_params=params(),
        cost_estimate=cost(
            20 * count * heads * rows * length * HEAD, 4 << 20, heads * rows * length
        ),
        name="attend_forward",
    )(keys, *[queries] * count, values_t)


def backward_body(count, first, last, key_ref, value_ref, key_t_ref, *refs):
    groups, refs = [refs[4 * i : 4 * i + 4] for i in range(count)], refs[4 * count :]
    if not first:
        (old_dk_ref, old_dv_ref), refs = refs[:2], refs[2:]
    dq_refs, (dk_ref, dv_ref) = refs[:count], refs[count:]
    dk = dv = None
    for (query_ref, log_ref, mixed_ref, grad_ref), dq_ref in zip(groups, dq_refs):
        grad = grad_ref[...]
        delta = jnp.sum(grad.astype(F32) * mixed_ref[0].astype(F32), axis=0, keepdims=True)
        scores = product(key_ref[0], query_ref[0])
        weights = jnp.exp2(scores * (scale * log2e) - log_ref[0, 0])
        grad_weights = product(value_ref[0], grad)
        grad_scores = (weights * (grad_weights - delta)).astype(BF)
        dq_ref[...] = (product(key_t_ref[...], grad_scores) * scale).astype(BF)
        add_dk = product_nt(query_ref[0, :HEAD, :], grad_scores)
        add_dv = product_nt(grad, weights.astype(BF))
        dk = add_dk if dk is None else dk + add_dk
        dv = add_dv if dv is None else dv + add_dv
    if not first:
        dk = dk + old_dk_ref[...]
        dv = dv + old_dv_ref[...]
    if last:
        dk = dk * scale
    dk_ref[...] = dk.astype(dk_ref.dtype)
    dv_ref[...] = dv.astype(dv_ref.dtype)


def attend_back(operands, quarters, logs, mixed, grads, carried, last):
    keys, queries, values, keys_t = operands
    heads, length, _ = keys.shape
    rows = length // 4
    first = carried is None
    flat = lambda n: pl.BlockSpec((HEAD, n), lambda h: (h, 0))
    by_head = lambda *dims: pl.BlockSpec((1,) + dims, lambda h: (h, 0, 0))
    in_specs = [by_head(length, 2 * HEAD), by_head(length, HEAD), flat(length)]
    args = [keys, values, keys_t]
    for q, (log, i), (out, j), grad in zip(quarters, logs, mixed, grads):
        in_specs += [
            pl.BlockSpec((1, 2 * HEAD, rows), lambda h, q=q: (h, 0, q)),
            pl.BlockSpec((1, 1, 1, rows), lambda h, i=i: (i, h, 0, 0)),
            pl.BlockSpec((1, HEAD, rows), lambda h, j=j: (j, h, 0)),
            flat(rows),
        ]
        args += [queries, log, out, grad]
    count = len(quarters)
    aliases = {}
    if not first:
        if not last:
            aliases = {len(args): count, len(args) + 1: count + 1}
        in_specs += [flat(length)] * 2
        args += list(carried)
    kind = BF if last else F32
    outs = pl.pallas_call(
        functools.partial(backward_body, count, first, last),
        grid=(heads,),
        in_specs=in_specs,
        out_specs=[flat(rows)] * count + [flat(length)] * 2,
        out_shape=[spec(BF, heads * HEAD, rows)] * count + [spec(kind, heads * HEAD, length)] * 2,
        input_output_aliases=aliases,
        compiler_params=params(),
        cost_estimate=cost(
            50 * count * heads * rows * length * HEAD, 8 << 20, count * heads * rows * length
        ),
        name="attend_back",
    )(*args)
    return outs[:count], outs[count:]


def side_copies(meta_ref, bundle_ref, held_ref, sems, start):
    lanes = pl.ds(start, held_ref.shape[2])
    return [
        pltpu.make_async_copy(bundle_ref.at[meta_ref[0] ^ g, :, lanes], held_ref.at[g], sems.at[g])
        for g in range(4)
    ]


def side_wait(bundle_ref, held_ref, sems, start, group):
    lanes = pl.ds(start, held_ref.shape[2])
    pltpu.make_async_copy(bundle_ref.at[0, :, lanes], held_ref.at[group], sems.at[group]).wait()


def down_copies(meta_ref, down_refs, held_ref, sems):
    parts = len(down_refs) // 4
    copies = []
    for g in range(4):
        for b in range(parts):
            ref = down_refs[parts * g + b]
            blocks, shard, _ = ref.shape
            for k in range(blocks):
                at = held_ref.at[g]
                if parts > 1:
                    place = pl.multiple_of(((2 * k + b) ^ meta_ref[2]) * shard, shard)
                    at = held_ref.at[g, pl.ds(place, shard)]
                copies.append(pltpu.make_async_copy(ref.at[k], at, sems.at[g]))
    return copies


def down_group(held_ref, sems, group):
    pltpu.make_async_copy(held_ref.at[group], held_ref.at[group], sems.at[group]).wait()
    return held_ref[group]


def held(*dims):
    return [pltpu.VMEM((4, *dims), BF), pltpu.SemaphoreType.DMA((4,))]


def unmoved():
    return pl.BlockSpec(memory_space=pl.ANY)


def gelu_parts(inner):
    both = 0.5 * (1.0 + lax.erf(inner * root_half))
    slope = both + inner * density * jnp.exp(-0.5 * inner * inner)
    return (inner * both).astype(BF), slope.astype(BF)


def group_spec(rows, units):
    return pl.BlockSpec((1, rows, units), lambda t: (t, 0, 0))


def fixed(*dims):
    return pl.BlockSpec(dims, lambda t: (0,) * len(dims))


def enter_body(units, meta_ref, bundle_ref, *refs):
    mixed_refs, (own_ref, out_bias_ref, gain_ref, shift_ref, bias_ref) = refs[:4], refs[4:9]
    low_ref, unit_ref, inverse_ref, act_ref, slope_ref = refs[9:14]
    out_ref, out_sems, up_ref, up_sems = refs[14:]
    group = pl.program_id(0)

    @pl.when(group == 0)
    def _():
        copies = side_copies(meta_ref, bundle_ref, out_ref, out_sems, units)
        for copy in copies + side_copies(meta_ref, bundle_ref, up_ref, up_sems, 0):
            copy.start()
        hidden = own_ref[...].astype(F32) + out_bias_ref[...]
        for copy in copies:
            copy.wait()
        for j, ref in enumerate(mixed_refs):
            hidden = hidden + product_nt(ref[0].T, out_ref[j])
        first, unit, inverse = normalize(hidden, gain_ref[...], shift_ref[...])
        unit_ref[...] = unit
        inverse_ref[...] = inverse
        low_ref[...] = first.astype(BF)

    side_wait(bundle_ref, up_ref, up_sems, 0, group)
    low = low_ref[...]
    step = units // 3
    for c in range(0, units, step):
        lanes = slice(c, c + step)
        inner = product(low, up_ref[group, :, lanes]) + bias_ref[0, :, lanes]
        act_ref[0, :, lanes], slope_ref[0, :, lanes] = gelu_parts(inner)


def enter(meta, bundle, mixed, own, out_bias, gain, shift, bias):
    rows, width = own.shape
    groups, _, units = bias.shape
    return pl.pallas_call(
        functools.partial(enter_body, units),
        grid=(groups,),
        in_specs=[smem(), unmoved()]
        + [pl.BlockSpec((1, *v.shape[1:]), lambda t: (0, 0, 0)) for v in mixed]
        + [vmem()] * 4
        + [group_spec(1, units)],
        out_specs=[fixed(rows, width), fixed(rows, width), fixed(rows, 1)]
        + [group_spec(rows, units)] * 2,
        out_shape=[spec(BF, rows, width), spec(F32, rows, width), spec(F32, rows, 1)]
        + [spec(BF, groups, rows, units)] * 2,
        scratch_shapes=held(width, mixed[0].shape[1]) + held(width, units),
        compiler_params=params(),
        cost_estimate=cost(12 * rows * width * units, 20 << 20, 8 * rows * units),
        name="enter",
    )(meta, bundle, *mixed, own, out_bias, gain, shift, bias)


def turn_body(count, meta_ref, *refs):
    down_refs, act_ref, refs = refs[:count], refs[count], refs[count + 1 :]
    unit_ref, first_gain_ref, first_shift_ref, bias_ref, gain_ref, shift_ref, up_ref = refs[:7]
    out_ref, grad_ref, low_ref, sums_ref, total_ref, down_ref, sems = refs[7:]
    step = pl.program_id(0)

    @pl.when(step == 0)
    def _():
        for copy in down_copies(meta_ref, down_refs, down_ref, sems):
            copy.start()

    part = product_nt(act_ref[0], down_group(down_ref, sems, step))

    @pl.when(step == 0)
    def _():
        total_ref[...] = part

    @pl.when(step > 0)
    def _():
        total_ref[...] += part

    @pl.when(step == pl.num_programs(0) - 1)
    def _():
        def chunk(at):
            first = unit_ref[at, :] * first_gain_ref[...] + first_shift_ref[...]
            second, unit, inverse = normalize(
                first + total_ref[at, :] + bias_ref[...], gain_ref[...], shift_ref[...]
            )
            out_ref[at, :] = second.astype(BF)
            upstream = up_ref[at, :].astype(F32)
            grad = norm_back(upstream, unit, inverse, gain_ref[...])
            grad_ref[at, :] = grad
            low_ref[at, :] = grad.astype(BF)
            return grad, upstream * unit, upstream

        sums = by_chunks(total_ref.shape[0], total_ref.shape[1], 32, chunk)
        for k in range(3):
            sums_ref[k : k + 1, :] = sums[k]


def turn(meta, downs, acts, unit, first_gain, first_shift, bias, gain, shift, cotangent):
    rows, width = unit.shape
    groups, _, units = acts.shape
    return pl.pallas_call(
        functools.partial(turn_body, len(downs)),
        grid=(groups,),
        in_specs=[smem()] + [unmoved()] * len(downs) + [group_spec(rows, units)] + [vmem()] * 7,
        out_specs=[fixed(rows, width)] * 3 + [fixed(3, width)],
        out_shape=[
            spec(BF, rows, width),
            spec(F32, rows, width),
            spec(BF, rows, width),
            spec(F32, 3, width),
        ],
        scratch_shapes=[pltpu.VMEM((rows, width), F32)] + held(width, units),
        compiler_params=params(),
        cost_estimate=cost(8 * rows * width * units, 16 << 20),
        name="turn",
    )(meta, *downs, acts, unit, first_gain, first_shift, bias, gain, shift, cotangent)


def leave_body(units, count, meta_ref, bundle_ref, *refs):
    down_refs, refs = refs[:count], refs[count:]
    slope_ref, low_ref, second_ref, unit_ref, inverse_ref, gain_ref = refs[:6]
    inner_ref, hidden_ref, attn_ref, own_ref, next_ref, far_rows_ref, sums_ref = refs[6:13]
    out_ref, out_sems, up_ref, up_sems, down_ref, down_sems = refs[13:]
    step = pl.program_id(0)

    @pl.when(step == 0)
    def _():
        copies = down_copies(meta_ref, down_refs, down_ref, down_sems)
        copies += side_copies(meta_ref, bundle_ref, up_ref, up_sems, 0)
        copies += side_copies(meta_ref, bundle_ref, out_ref, out_sems, units)
        for copy in copies:
            copy.start()
        hidden_ref[...] = second_ref[...]

    down = down_group(down_ref, down_sems, step)
    grad = product(low_ref[...], down) * slope_ref[0].astype(F32)
    inner = grad.astype(BF)
    inner_ref[0] = inner
    total_inner = jnp.sum(inner.astype(F32), axis=0, keepdims=True)
    sums_ref[pl.ds(3 + (meta_ref[0] ^ step), 1), :] = total_inner
    side_wait(bundle_ref, up_ref, up_sems, 0, step)
    hidden_ref[...] += product_nt(inner, up_ref[step])

    @pl.when(step == pl.num_programs(0) - 1)
    def _():
        for copy in side_copies(meta_ref, bundle_ref, out_ref, out_sems, units):
            copy.wait()
        back = hidden_ref[...]
        unit = unit_ref[...]
        hidden = norm_back(back, unit, inverse_ref[...], gain_ref[...])
        hidden_ref[...] = hidden
        sums_ref[0:1, :] = jnp.sum(hidden, axis=0, keepdims=True)
        sums_ref[1:2, :] = jnp.sum(back * unit, axis=0, keepdims=True)
        sums_ref[2:3, :] = jnp.sum(back, axis=0, keepdims=True)
        attn = hidden.astype(BF)
        attn_ref[...] = attn
        for j in range(4):
            mixed = product(attn, out_ref[j]).T.astype(BF)
            if j == 0:
                own_ref[...] = mixed
            elif j == 1:
                next_ref[...] = mixed
            else:
                far_rows_ref[j - 2] = mixed


def leave(meta, bundle, downs, slopes, low, second, unit, inverse, gain):
    rows, width = low.shape
    groups, _, units = slopes.shape
    feats = bundle.shape[2] - units
    return pl.pallas_call(
        functools.partial(leave_body, units, len(downs)),
        grid=(groups,),
        in_specs=[smem()] + [unmoved()] * (1 + len(downs)) + [group_spec(rows, units)] + [vmem()] * 5,
        out_specs=[
            group_spec(rows, units),
            fixed(rows, width),
            fixed(rows, width),
            fixed(feats, rows),
            fixed(feats, rows),
            fixed(2, feats, rows),
            fixed(3 + groups, width),
        ],
        out_shape=[
            spec(BF, groups, rows, units),
            spec(F32, rows, width),
            spec(BF, rows, width),
            spec(BF, feats, rows),
            spec(BF, feats, rows),
            spec(BF, 2, feats, rows),
            spec(F32, 3 + groups, width),
        ],
        scratch_shapes=held(width, feats) + held(width, units) + held(width, units),
        compiler_params=params(),
        cost_estimate=cost(16 * rows * width * units, 28 << 20),
        name="leave",
    )(meta, bundle, *downs, slopes, low, second, unit, inverse, gain)


def outer_body(shard, extra, keep, meta_ref, left_ref, right_ref, *refs):
    if extra:
        attn_ref, mixed_refs, sum_refs, refs = refs[0], refs[1:3], refs[3:5], refs[5:]
    if keep:
        arrived_ref, refs = refs[0], refs[1:]
        left_t_ref, attn_t_ref = left_ref, attn_ref if extra else None
    else:
        left_t_ref, attn_t_ref = refs[1], refs[2] if extra else None
    out_ref = refs[0]
    step = pl.program_id(0)
    units = right_ref.shape[2]
    width = left_t_ref.shape[0]
    pairs = width // shard // 2
    lanes = out_ref.shape[3]

    if not keep:

        @pl.when(step == 0)
        def _():
            left_t_ref[...] = left_ref[...].T
            if extra:
                attn_t_ref[...] = attn_ref[...].T

    def put(low, rows, lane, values):
        if keep:
            values = values + arrived_ref[low, 0, rows, lane].astype(F32)
        out_ref[low, 0, rows, lane] = values.astype(BF)

    def spread(values, lane):
        for block in range(2 * pairs):
            rows = slice(block // 2 * shard, (block // 2 + 1) * shard)
            put(block % 2, rows, lane, values[block * shard : (block + 1) * shard])

    spread(product(left_t_ref[...], right_ref[0]), slice(0, units))
    if extra:
        for j in range(2):

            @pl.when(step ^ (meta_ref[0] // 2) == j)
            def _(j=j):
                spread(product_nt(attn_t_ref[...], mixed_refs[j][0]), slice(units, lanes))

        sums = jnp.concatenate(
            [sum_refs[0][...], sum_refs[1][...], jnp.zeros((16 - 10, width), F32)], axis=0
        )
        for low in range(2):
            put(low, slice(pairs * shard, pairs * shard + 16), slice(0, width), sums)
            out_ref[low, 0, pairs * shard :, width:lanes] = jnp.zeros((16, lanes - width), BF)


def outer(meta, shard, left, rights, attn=None, mixed=(), sums=(), arrived=None):
    keep = arrived is not None
    rows, width = left.shape[::-1] if keep else left.shape
    groups, _, units = rights.shape
    extra = attn is not None
    feats = mixed[0].shape[1] if extra else 0
    depth = width // 2 + (16 if extra else 0)

    def group(i, meta_ref):
        return 2 * (i ^ (meta_ref[0] // 2)) + (0 if keep else 1)

    args = [left, rights] + ([attn, *mixed, *sums] if extra else [])
    block = pl.BlockSpec((2, 1, depth, units + feats), lambda i, m: (0, i, 0, 0))
    turned = [] if keep else [left, attn] if extra else [left]
    grid_spec = pltpu.PrefetchScalarGridSpec(
        num_scalar_prefetch=1,
        grid=(2,),
        in_specs=[vmem(), pl.BlockSpec((1, rows, units), lambda i, m: (group(i, m), 0, 0))]
        + ([vmem()] if extra else [])
        + [pl.BlockSpec((1, *v.shape[1:]), lambda i, m: (0, 0, 0)) for v in mixed]
        + [vmem()] * len(sums)
        + ([block] if keep else []),
        out_specs=[block] + [vmem()] * len(turned),
    )
    return pl.pallas_call(
        functools.partial(outer_body, shard, extra, keep),
        grid_spec=grid_spec,
        out_shape=[spec(BF, 2, 2, depth, units + feats)] + [spec(BF, width, rows) for _ in turned],
        compiler_params=params(),
        cost_estimate=cost(4 * rows * width * units, 8 << 20),
        name="outer",
    )(meta, *args, *([arrived] if keep else []))


def inputs_body(*refs):
    dq_refs, (dk_ref, dv_ref, turned_ref) = refs[:4], refs[4:7]
    own_ref, next_ref, out_ref = refs[7:10]
    rows = dq_refs[0].shape[1]
    weight = turned_ref[...]
    for r in (1, 3, 0, 2):
        at = slice(r * rows, (r + 1) * rows)
        grad = jnp.concatenate([dq_refs[r][...], dk_ref[:, at], dv_ref[:, at]], axis=0)
        back = product(grad.T, weight)
        if r == 0:
            own_ref[...] = back
        elif r == 2:
            next_ref[...] = back
        else:
            out_ref[(r // 2) * rows : (r // 2 + 1) * rows, :] = back.astype(BF)


def input_grads(dq, dk, dv, turned):
    rows = dq[0].shape[1]
    width = turned.shape[1]
    return pl.pallas_call(
        inputs_body,
        in_specs=[vmem()] * 7,
        out_specs=[vmem()] * 3,
        out_shape=[spec(F32, rows, width), spec(F32, rows, width), spec(BF, 2 * rows, width)],
        compiler_params=params(),
        cost_estimate=cost(8 * rows * width * width, 12 << 20),
        name="input_grads",
    )(*dq, dk, dv, turned)


def projections_body(shard, *refs):
    meta_ref, dq_refs, (dk_ref, dv_ref, all_ref, keep_ref, send_ref) = refs[0], refs[1:5], refs[5:10]
    held_ref = refs[10]
    rows = dq_refs[0].shape[1]
    depth = keep_ref.shape[0] - 16
    grad = jnp.concatenate(
        [jnp.concatenate([ref[...] for ref in dq_refs], axis=1), dk_ref[...], dv_ref[...]], axis=0
    )
    held_ref[...] = product(grad, all_ref[...]).T.astype(BF)
    sums = product_nt(jnp.ones((16, 4 * rows), BF), grad).astype(BF)
    for flip, out_ref in ((0, keep_ref), (1, send_ref)):
        for i in range(depth // shard):
            block = 2 * i + (meta_ref[1] ^ flip)
            if shard % 16 == 0:
                start = pl.multiple_of(block * shard, shard)
                out_ref[i * shard : (i + 1) * shard, :] = held_ref[pl.ds(start, shard), :]
            else:
                even = held_ref[2 * i * shard : (2 * i + 1) * shard, :]
                odd = held_ref[(2 * i + 1) * shard : (2 * i + 2) * shard, :]
                out_ref[i * shard : (i + 1) * shard, :] = jnp.where(block % 2 == 0, even, odd)
        out_ref[depth:, :] = sums


def projection_grads(meta, shard, dq, dk, dv, tokens):
    width = tokens.shape[1]
    feats = dq[0].shape[0]
    return pl.pallas_call(
        functools.partial(projections_body, shard),
        in_specs=[smem()] + [vmem()] * 7,
        out_specs=[vmem()] * 2,
        out_shape=[spec(BF, width // 2 + 16, 3 * feats)] * 2,
        scratch_shapes=[pltpu.VMEM((width, 3 * feats), BF)],
        compiler_params=params(),
        cost_estimate=cost(2 * tokens.shape[0] * width * 3 * feats, 12 << 20),
        name="projection_grads",
    )(meta, *dq, dk, dv, tokens)


def exchanger(axis_dp, axis_tensor):
    def swap(values, dp_bits, tensor_bits):
        pairs = [
            (d * axis_tensor + t, (d ^ dp_bits) * axis_tensor + (t ^ tensor_bits))
            for d in range(axis_dp)
            for t in range(axis_tensor)
        ]
        return lax.ppermute(values, ("dp", "tensor"), pairs)

    return swap


def tie(*values):
    return lax.optimization_barrier(values)


def add(left, right):
    return (left.astype(F32) + right.astype(F32)).astype(BF)


def total(parts):
    return functools.reduce(jnp.add, [parts[i].astype(F32) for i in range(parts.shape[0])])


def local(
    axis_dp,
    axis_tensor,
    inputs,
    segments,
    query_weight,
    query_bias,
    key_weight,
    value_weight,
    value_bias,
    output_weight,
    output_bias,
    up_weight,
    up_bias,
    down_weight,
    down_bias,
    first_gain,
    first_shift,
    second_gain,
    second_shift,
    cotangent,
):
    swap = exchanger(axis_dp, axis_tensor)
    place_dp, place_tensor = lax.axis_index("dp"), lax.axis_index("tensor")
    meta = jnp.stack([place_tensor, place_dp % 2, place_dp]).astype(jnp.int32)
    rows, width = inputs.shape[1:]
    shard = query_weight.shape[0]
    feats = output_weight.shape[0]
    heads = feats // HEAD
    units = up_weight.shape[1]
    pairs = axis_dp // 2
    row = lambda v: v.reshape(1, -1).astype(F32)
    flat = lambda z, x, y, c: (2 * z + x) * axis_tensor + 2 * y + c
    near_groups = [
        [flat(z, x, y, c) for x in range(2) for y in range(2)] for z in range(pairs) for c in range(2)
    ]
    deep_groups = [[2 * z + x for z in range(pairs)] for x in range(2)]

    own = inputs[0]
    notes = jnp.zeros((16, width), BF)
    notes = notes.at[0, :rows].set(segments[0].astype(BF)).at[1, :units].set(up_bias)
    message = jnp.concatenate([own, notes])
    across = swap(message, 0, 2)
    bundle = jnp.concatenate([query_weight, key_weight, value_weight], axis=1)
    copies = jnp.broadcast_to(bundle[None], (axis_dp,) + bundle.shape)
    qkv_weight = lax.all_to_all(copies, "dp", 0, 0, tiled=True).reshape(width, 3 * feats)
    near = swap(message, 0, 1)
    far = swap(across, 0, 1)
    tokens = [message, near, across, far]

    up_bundle = lax.all_gather(
        jnp.concatenate([up_weight, output_weight.T], axis=1), ("tensor", "dp"), axis=0, tiled=True
    ).reshape(axis_tensor, width, units + feats)
    down = down_weight.T
    around = jnp.stack([down] + [swap(down, 2 * k, 0) for k in range(1, pairs)])
    across_around = swap(around, 0, 2)

    noted = jnp.stack([v[rows:] for v in tokens]).astype(F32)
    docs = noted[:, 0, :rows].reshape(-1)
    bias = noted[:, 1:2, :units]
    lane = jnp.arange(HEAD, dtype=F32)
    same = docs[:, None] == lane[None, :]
    aux_query = (docs[None, :] == lane[:, None]).astype(BF)
    aux_key = jnp.where(same | (lane[None, :] >= 8), 0.0, -far_score).astype(BF)
    output_bias, first_gain, first_shift, down_bias, second_gain, second_shift, bias, aux_key = tie(
        *[row(v) for v in (output_bias, first_gain, first_shift, down_bias, second_gain, second_shift)],
        bias, aux_key,
    )
    qkv_bias = jnp.concatenate([query_bias, jnp.zeros_like(query_bias), value_bias]).astype(F32)
    all_tokens, turned, queries, keys, values, values_t, keys_t = project(
        qkv_weight, tokens, rows, qkv_bias[feats:].reshape(1, -1), qkv_bias.reshape(-1, 1),
        aux_query, aux_key, heads,
    )

    _, around_late = tie(queries, around)
    beside = swap(around_late, 1, 0)

    mixed23, log23 = attend_forward(keys, queries, values_t, (2, 3))
    queries, mixed23 = tie(queries, mixed23)
    arrived = swap(mixed23, 0, 2)
    _, around_late, across_around = tie(mixed23, around_late, across_around)
    columns = [around, None, swap(around_late, 0, 1), None, across_around, None]
    columns += [swap(across_around, 0, 1), None]
    mixed1, log1 = attend_forward(keys, queries, values_t, (1,))
    queries, mixed1 = tie(queries, mixed1)
    arrived1 = swap(mixed1, 0, 1)
    _, beside = tie(mixed1, beside)
    across_beside = swap(beside, 0, 2)
    queries, arrived = tie(queries, arrived)
    arrived3 = swap(arrived[1:], 0, 1)
    mixed0, log0 = attend_forward(keys, queries, values_t, (0,))
    mixed = [mixed0, arrived1, arrived, arrived3]

    _, later = tie(mixed0, across_beside)
    columns[1::2] = [beside, swap(beside, 0, 1), across_beside, swap(later, 0, 1)]
    downs = columns
    if shard % 16:
        order = [2 * k + b for b in range(2) for k in range(pairs)]
        places = jnp.argsort(jnp.array(order) ^ place_dp)
        downs = [jnp.concatenate(columns[2 * g : 2 * g + 2]) for g in range(4)]
        downs = [v[places].reshape(1, width, units) for v in downs]

    low, unit_first, inverse_first, acts, slopes = enter(
        meta, up_bundle, mixed, own, output_bias, first_gain, first_shift, bias
    )
    layer_out, grad_second, second_low, sums_second = turn(
        meta, downs, acts, unit_first, first_gain, first_shift,
        down_bias, second_gain, second_shift, cotangent[0],
    )
    send_b, second_t = outer(meta, shard, second_low, acts)
    second_low, send_b = tie(second_low, send_b)
    moved_b = swap(send_b, 0, 1)
    inners, grad_hidden, grad_attn, grad0, next_mixed, far_mixed, sums_first = leave(
        meta, up_bundle, downs, slopes, second_low, grad_second, unit_first, inverse_first, first_gain
    )

    def reduce_near(values):
        values = values.reshape((4,) + values.shape[2:])
        return lax.all_to_all(values, ("dp", "tensor"), 0, 0, axis_index_groups=near_groups, tiled=True)

    def reduce_deep(values):
        return lax.all_to_all(values, "dp", 0, 0, axis_index_groups=deep_groups, tiled=True)

    def deep_parts(values):
        return values[: pairs * shard].reshape(pairs, shard, -1)

    def part_at(parts, k):
        return lax.dynamic_index_in_dim(parts, (place_dp // 2) ^ k, 0, False)

    arrived_g = swap(far_mixed, 0, 2)
    g1 = swap(next_mixed, 0, 1)
    (part_b,) = outer(meta, shard, second_t, acts, arrived=moved_b)
    inners, part_b = tie(inners, part_b)
    near_b = reduce_near(part_b)
    sums_both = (sums_first, sums_second)
    send_a, low_t, attn_t = outer(meta, shard, low, inners, grad_attn, mixed[1::2], sums_both)
    grad0, send_a, g1, arrived_g = tie(grad0, send_a, g1, arrived_g)
    moved_a = swap(send_a, 0, 1)
    g2, g3 = arrived_g[0], swap(arrived_g[1], 0, 1)
    operands = (keys, queries, values, keys_t)
    (dq0, dq1), carried = attend_back(
        operands, (0, 1), ((log0, 0), (log1, 0)), ((mixed0, 0), (mixed1, 0)), (grad0, g1), None, False
    )
    low_t, carried, moved_a = tie(low_t, carried, moved_a)
    (part_a,) = outer(meta, shard, low_t, inners, attn_t, mixed[::2], sums_both, moved_a)
    carried, part_a, near_b, g2, g3 = tie(carried, part_a, near_b, g2, g3)
    near_a = reduce_near(part_a)
    parts_b = deep_parts(total(near_b).astype(BF))
    sent_b = [part_at(parts_b, k) for k in range(1, pairs)]
    carried, parts_b, *sent_b = tie(carried, parts_b, *sent_b)
    own_b = part_at(parts_b, 0).astype(F32)
    for k in range(1, pairs):
        own_b = own_b + swap(sent_b[k - 1], 2 * k, 0).astype(F32)
    (dq2, dq3), (dk, dv) = attend_back(
        operands, (2, 3), ((log23, 0), (log23, 1)), ((mixed23, 0), (mixed23, 1)), (g2, g3), carried, True
    )
    dq2, own_b = tie(dq2, own_b)
    dq = (dq0, dq1, dq2, dq3)
    own_rows, next_rows, sent_rows = input_grads(dq, dk, dv, turned)
    moved = swap(sent_rows, 0, 1)
    dk, sent_rows = tie(dk, sent_rows)
    keep_c, send_c = projection_grads(meta, shard, dq, dk, dv, all_tokens)
    _, moved = tie(send_c, moved)
    next_rows = add(next_rows, moved[rows:])
    arrived_c = swap(send_c, 1, 0)
    arrived_rows = swap(next_rows, 0, 2)
    _, _, near_a = tie(send_c, next_rows, near_a)
    sum_a = total(near_a).astype(BF)
    notes = jnp.broadcast_to(sum_a[None, pairs * shard :], (pairs, 16, sum_a.shape[1]))
    packed_a = jnp.concatenate([deep_parts(sum_a), notes], axis=1)
    deep_a = reduce_deep(packed_a)
    _, arrived_c = tie(packed_a, arrived_c)
    sum_c = add(keep_c, arrived_c)
    parts_c, notes = deep_parts(sum_c), sum_c[pairs * shard :]
    own_c = jnp.concatenate([part_at(parts_c, 0), notes]).astype(F32)
    for k in range(1, pairs):
        arrived_part = swap(jnp.concatenate([part_at(parts_c, k), notes]), 2 * k, 0)
        _, arrived_part = tie(arrived_rows, arrived_part)
        own_c = own_c + arrived_part.astype(F32)
    own_a = total(deep_a)
    grad_inputs = grad_hidden + own_rows + moved[:rows].astype(F32) + arrived_rows.astype(F32)
    sums = own_a[shard:, :width]
    sum_up = lax.dynamic_index_in_dim(sums[3:7], place_tensor, 0, False)
    head_sums = own_c[shard]

    return (
        layer_out[None],
        grad_inputs[None],
        own_c[:shard, :feats],
        head_sums[:feats],
        own_c[:shard, feats : 2 * feats],
        own_c[:shard, 2 * feats :],
        head_sums[2 * feats :],
        own_a[:shard, units:].T,
        sums[0],
        own_a[:shard, :units],
        sum_up,
        own_b.T,
        sums[7],
        sums[1],
        sums[2],
        sums[8],
        sums[9],
    )


def solution(mesh):
    axis_dp, axis_tensor = mesh.shape["dp"], mesh.shape["tensor"]
    if axis_tensor != 4 or axis_dp < 2 or axis_dp & (axis_dp - 1):
        raise ValueError("mesh sizes")
    return jax.shard_map(
        functools.partial(local, axis_dp, axis_tensor),
        mesh=mesh,
        in_specs=(
            P("dp", "tensor", None),
            P("dp", "tensor"),
            P("dp", "tensor"),
            P("tensor"),
            P("dp", "tensor"),
            P("dp", "tensor"),
            P("tensor"),
            P("tensor", "dp"),
            P(),
            P("dp", "tensor"),
            P("tensor"),
            P("tensor", "dp"),
            P(),
            P(),
            P(),
            P(),
            P(),
            P("dp", "tensor", None),
        ),
        out_specs=(
            P("dp", "tensor", None),
            P("dp", "tensor", None),
            P("dp", "tensor"),
            P("tensor"),
            P("dp", "tensor"),
            P("dp", "tensor"),
            P("tensor"),
            P("tensor", "dp"),
            P(),
            P("dp", "tensor"),
            P("tensor"),
            P("tensor", "dp"),
            P(),
            P(),
            P(),
            P(),
            P(),
        ),
        check_vma=False,
    )
```

```python
import functools

import jax
import jax.numpy as jnp
from jax import lax
from jax.experimental import pallas as pl
from jax.experimental.pallas import tpu as pltpu
from jax.sharding import PartitionSpec as P

HEAD = 64
BF = jnp.bfloat16
F32 = jnp.float32

eps_norm = 1e-12
root_half = 0.7071067811865476
density = 0.3989422804014327
scale = 0.125
log2e = 1.4426950408889634
far_score = 1e30
vmem_bytes = 60 * 1024 * 1024


def product(left, right):
    return jnp.dot(left, right, preferred_element_type=F32)


def product_nt(left, right):
    return lax.dot_general(left, right, (((1,), (1,)), ((), ())), preferred_element_type=F32)


def product_tn(left, right):
    return lax.dot_general(left, right, (((0,), (0,)), ((), ())), preferred_element_type=F32)


def normalize(values, gain, offset):
    average = jnp.mean(values, axis=-1, keepdims=True)
    centred = values - average
    inverse = lax.rsqrt(jnp.mean(centred * centred, axis=-1, keepdims=True) + eps_norm)
    normed = centred * inverse
    return (normed * gain + offset, normed, inverse)


def norm_back(upstream, normed, inverse, gain):
    scaled = upstream * gain
    centred = scaled - jnp.mean(scaled, axis=-1, keepdims=True)
    return (centred - normed * jnp.mean(scaled * normed, axis=-1, keepdims=True)) * inverse


def fold(values):
    return functools.reduce(jnp.add, [values[i : i + 8] for i in range(0, values.shape[0], 8)])


def by_chunks(rows, width, size, chunk):
    def step(i, sums):
        at = pl.ds(pl.multiple_of(i * size, size), size)
        return tuple(a + fold(b) for a, b in zip(sums, chunk(at)))

    sums = lax.fori_loop(0, rows // size, step, (jnp.zeros((8, width), F32),) * 3)
    return [jnp.sum(v, axis=0, keepdims=True) for v in sums]


def vmem():
    return pl.BlockSpec(memory_space=pltpu.VMEM)


def smem():
    return pl.BlockSpec(memory_space=pltpu.SMEM)


def params():
    return pltpu.CompilerParams(vmem_limit_bytes=vmem_bytes)


def cost(flops, moved, hard=0):
    return pl.CostEstimate(flops=int(flops), bytes_accessed=int(moved), transcendentals=int(hard))


def spec(dtype, *dims):
    return jax.ShapeDtypeStruct(dims, dtype)


def project_body(heads, *refs):
    token_refs, (weight_ref, row_bias_ref, column_bias_ref, aux_query_ref, aux_key_ref) = refs[:4], refs[4:9]
    all_ref, turned_ref, query_ref, key_ref, value_ref, value_t_ref, key_t_ref = refs[9:16]
    step = pl.program_id(0)
    width = heads * HEAD
    rows = all_ref.shape[0]

    @pl.when(step == 0)
    def _():
        turned_ref[...] = weight_ref[...].T

    for r, ref in enumerate(token_refs):

        @pl.when(step == r)
        def _(ref=ref):
            all_ref[...] = ref[:rows, :]

    tokens = all_ref[...]
    turned = (product_nt(turned_ref[...], tokens) + column_bias_ref[...]).astype(BF)
    plain = (product(tokens, weight_ref[:, width : 3 * width]) + row_bias_ref[...]).astype(BF)
    for h in range(heads):
        at = slice(h * HEAD, (h + 1) * HEAD)
        query_ref[h, :HEAD, :] = turned[at]
        query_ref[h, HEAD:, :] = aux_query_ref[...]
        key_t_ref[at, :] = turned[width : 2 * width][at]
        value_t_ref[at, :] = turned[2 * width :][at]
        key_ref[h] = jnp.concatenate([plain[:, at], aux_key_ref[...]], axis=1)
        value_ref[h] = plain[:, width + h * HEAD : width + (h + 1) * HEAD]


def project(weight, tokens, rows, row_bias, column_bias, aux_query, aux_key, heads):
    width = weight.shape[0]
    length = 4 * rows
    by_row = lambda n: pl.BlockSpec((rows, n), lambda r: (r, 0))
    headed = lambda n: pl.BlockSpec((heads, rows, n), lambda r: (0, r, 0))
    flat = pl.BlockSpec((heads * HEAD, rows), lambda r: (0, r))
    return pl.pallas_call(
        functools.partial(project_body, heads),
        grid=(4,),
        in_specs=[vmem()] * 7 + [pl.BlockSpec((HEAD, rows), lambda r: (0, r)), by_row(HEAD)],
        out_specs=[
            by_row(width),
            pl.BlockSpec((3 * heads * HEAD, width), lambda r: (0, 0)),
            pl.BlockSpec((heads, 2 * HEAD, rows), lambda r: (0, 0, r)),
            headed(2 * HEAD),
            headed(HEAD),
            flat,
            flat,
        ],
        out_shape=[
            spec(BF, length, width),
            spec(BF, 3 * heads * HEAD, width),
            spec(BF, heads, 2 * HEAD, length),
            spec(BF, heads, length, 2 * HEAD),
            spec(BF, heads, length, HEAD),
            spec(BF, heads * HEAD, length),
            spec(BF, heads * HEAD, length),
        ],
        compiler_params=params(),
        cost_estimate=cost(4 * length * width * 3 * heads * HEAD, 16 << 20),
        name="project",
    )(*tokens, weight, row_bias, column_bias, aux_query, aux_key)


def forward_body(count, key_ref, *refs):
    query_refs, value_ref, out_ref, log_ref = refs[:count], refs[count], refs[count + 1], refs[count + 2]
    chunk = key_ref.shape[1] // 4
    for i in range(count):
        query = query_refs[i][0]
        scores = [product(key_ref[0, c * chunk : (c + 1) * chunk, :], query) for c in range(4)]
        highest = None
        for c in range(4):
            peak = jnp.max(scores[c], axis=0, keepdims=True)
            now = peak if highest is None else jnp.maximum(highest, peak)
            raised = jnp.exp2((scores[c] - now) * (scale * log2e))
            part = jnp.sum(raised, axis=0, keepdims=True)
            mixed = product(value_ref[:, c * chunk : (c + 1) * chunk], raised.astype(BF))
            if highest is None:
                total, out = part, mixed
            else:
                shrink = jnp.exp2((highest - now) * (scale * log2e))
                total, out = total * shrink + part, out * shrink + mixed
            highest = now
        out_ref[i] = (out / total).astype(BF)
        log_ref[i, 0] = highest * (scale * log2e) + jnp.log2(total)


def attend_forward(keys, queries, values_t, quarters):
    heads, length, _ = keys.shape
    rows = length // 4
    count = len(quarters)
    return pl.pallas_call(
        functools.partial(forward_body, count),
        grid=(heads,),
        in_specs=[pl.BlockSpec((1, length, 2 * HEAD), lambda h: (h, 0, 0))]
        + [pl.BlockSpec((1, 2 * HEAD, rows), lambda h, q=q: (h, 0, q)) for q in quarters]
        + [pl.BlockSpec((HEAD, length), lambda h: (h, 0))],
        out_specs=[
            pl.BlockSpec((count, HEAD, rows), lambda h: (0, h, 0)),
            pl.BlockSpec((count, 1, 1, rows), lambda h: (0, h, 0, 0)),
        ],
        out_shape=[spec(BF, count, heads * HEAD, rows), spec(F32, count, heads, 1, rows)],
        compiler_params=params(),
        cost_estimate=cost(
            20 * count * heads * rows * length * HEAD, 4 << 20, heads * rows * length
        ),
        name="attend_forward",
    )(keys, *[queries] * count, values_t)


def backward_body(count, first, last, key_ref, value_ref, key_t_ref, *refs):
    groups, refs = [refs[4 * i : 4 * i + 4] for i in range(count)], refs[4 * count :]
    if not first:
        (old_dk_ref, old_dv_ref), refs = refs[:2], refs[2:]
    dq_refs, (dk_ref, dv_ref) = refs[:count], refs[count:]
    dk = dv = None
    for (query_ref, log_ref, mixed_ref, grad_ref), dq_ref in zip(groups, dq_refs):
        grad = grad_ref[...]
        delta = jnp.sum(grad.astype(F32) * mixed_ref[0].astype(F32), axis=0, keepdims=True)
        scores = product(key_ref[0], query_ref[0])
        weights = jnp.exp2(scores * (scale * log2e) - log_ref[0, 0])
        grad_weights = product(value_ref[0], grad)
        grad_scores = (weights * (grad_weights - delta)).astype(BF)
        dq_ref[...] = (product(key_t_ref[...], grad_scores) * scale).astype(BF)
        add_dk = product_nt(query_ref[0, :HEAD, :], grad_scores)
        add_dv = product_nt(grad, weights.astype(BF))
        dk = add_dk if dk is None else dk + add_dk
        dv = add_dv if dv is None else dv + add_dv
    if not first:
        dk = dk + old_dk_ref[...]
        dv = dv + old_dv_ref[...]
    if last:
        dk = dk * scale
    dk_ref[...] = dk.astype(dk_ref.dtype)
    dv_ref[...] = dv.astype(dv_ref.dtype)


def attend_back(operands, quarters, logs, mixed, grads, carried, last):
    keys, queries, values, keys_t = operands
    heads, length, _ = keys.shape
    rows = length // 4
    first = carried is None
    flat = lambda n: pl.BlockSpec((HEAD, n), lambda h: (h, 0))
    by_head = lambda *dims: pl.BlockSpec((1,) + dims, lambda h: (h, 0, 0))
    in_specs = [by_head(length, 2 * HEAD), by_head(length, HEAD), flat(length)]
    args = [keys, values, keys_t]
    for q, (log, i), (out, j), grad in zip(quarters, logs, mixed, grads):
        in_specs += [
            pl.BlockSpec((1, 2 * HEAD, rows), lambda h, q=q: (h, 0, q)),
            pl.BlockSpec((1, 1, 1, rows), lambda h, i=i: (i, h, 0, 0)),
            pl.BlockSpec((1, HEAD, rows), lambda h, j=j: (j, h, 0)),
            flat(rows),
        ]
        args += [queries, log, out, grad]
    count = len(quarters)
    aliases = {}
    if not first:
        if not last:
            aliases = {len(args): count, len(args) + 1: count + 1}
        in_specs += [flat(length)] * 2
        args += list(carried)
    kind = BF if last else F32
    outs = pl.pallas_call(
        functools.partial(backward_body, count, first, last),
        grid=(heads,),
        in_specs=in_specs,
        out_specs=[flat(rows)] * count + [flat(length)] * 2,
        out_shape=[spec(BF, heads * HEAD, rows)] * count + [spec(kind, heads * HEAD, length)] * 2,
        input_output_aliases=aliases,
        compiler_params=params(),
        cost_estimate=cost(
            50 * count * heads * rows * length * HEAD, 8 << 20, count * heads * rows * length
        ),
        name="attend_back",
    )(*args)
    return outs[:count], outs[count:]


def side_copies(meta_ref, bundle_ref, held_ref, sems, start):
    lanes = pl.ds(start, held_ref.shape[2])
    return [
        pltpu.make_async_copy(bundle_ref.at[meta_ref[0] ^ g, :, lanes], held_ref.at[g], sems.at[g])
        for g in range(4)
    ]


def side_wait(bundle_ref, held_ref, sems, start, group):
    lanes = pl.ds(start, held_ref.shape[2])
    pltpu.make_async_copy(bundle_ref.at[0, :, lanes], held_ref.at[group], sems.at[group]).wait()


def down_copies(meta_ref, down_refs, held_ref, sems):
    parts = len(down_refs) // 4
    copies = []
    for g in range(4):
        for b in range(parts):
            ref = down_refs[parts * g + b]
            blocks, shard, _ = ref.shape
            for k in range(blocks):
                at = held_ref.at[g]
                if parts > 1:
                    place = pl.multiple_of(((2 * k + b) ^ meta_ref[2]) * shard, shard)
                    at = held_ref.at[g, pl.ds(place, shard)]
                copies.append(pltpu.make_async_copy(ref.at[k], at, sems.at[g]))
    return copies


def down_group(held_ref, sems, group):
    pltpu.make_async_copy(held_ref.at[group], held_ref.at[group], sems.at[group]).wait()
    return held_ref[group]


def held(*dims):
    return [pltpu.VMEM((4, *dims), BF), pltpu.SemaphoreType.DMA((4,))]


def unmoved():
    return pl.BlockSpec(memory_space=pl.ANY)


def gelu_parts(inner):
    both = 0.5 * (1.0 + lax.erf(inner * root_half))
    slope = both + inner * density * jnp.exp(-0.5 * inner * inner)
    return (inner * both).astype(BF), slope.astype(BF)


def group_spec(rows, units):
    return pl.BlockSpec((1, rows, units), lambda t: (t, 0, 0))


def fixed(*dims):
    return pl.BlockSpec(dims, lambda t: (0,) * len(dims))


def enter_body(units, meta_ref, bundle_ref, *refs):
    mixed_refs, (own_ref, out_bias_ref, gain_ref, shift_ref, bias_ref) = refs[:4], refs[4:9]
    low_ref, unit_ref, inverse_ref, act_ref, slope_ref = refs[9:14]
    out_ref, out_sems, up_ref, up_sems = refs[14:]
    group = pl.program_id(0)

    @pl.when(group == 0)
    def _():
        copies = side_copies(meta_ref, bundle_ref, out_ref, out_sems, units)
        for copy in copies + side_copies(meta_ref, bundle_ref, up_ref, up_sems, 0):
            copy.start()
        hidden = own_ref[...].astype(F32) + out_bias_ref[...]
        for copy in copies:
            copy.wait()
        for j, ref in enumerate(mixed_refs):
            hidden = hidden + product_nt(ref[0].T, out_ref[j])
        first, unit, inverse = normalize(hidden, gain_ref[...], shift_ref[...])
        unit_ref[...] = unit
        inverse_ref[...] = inverse
        low_ref[...] = first.astype(BF)

    side_wait(bundle_ref, up_ref, up_sems, 0, group)
    low = low_ref[...]
    step = units // 3
    for c in range(0, units, step):
        lanes = slice(c, c + step)
        inner = product(low, up_ref[group, :, lanes]) + bias_ref[0, :, lanes]
        act_ref[0, :, lanes], slope_ref[0, :, lanes] = gelu_parts(inner)


def enter(meta, bundle, mixed, own, out_bias, gain, shift, bias):
    rows, width = own.shape
    groups, _, units = bias.shape
    return pl.pallas_call(
        functools.partial(enter_body, units),
        grid=(groups,),
        in_specs=[smem(), unmoved()]
        + [pl.BlockSpec((1, *v.shape[1:]), lambda t: (0, 0, 0)) for v in mixed]
        + [vmem()] * 4
        + [group_spec(1, units)],
        out_specs=[fixed(rows, width), fixed(rows, width), fixed(rows, 1)]
        + [group_spec(rows, units)] * 2,
        out_shape=[spec(BF, rows, width), spec(F32, rows, width), spec(F32, rows, 1)]
        + [spec(BF, groups, rows, units)] * 2,
        scratch_shapes=held(width, mixed[0].shape[1]) + held(width, units),
        compiler_params=params(),
        cost_estimate=cost(12 * rows * width * units, 20 << 20, 8 * rows * units),
        name="enter",
    )(meta, bundle, *mixed, own, out_bias, gain, shift, bias)


def turn_body(count, meta_ref, *refs):
    down_refs, act_ref, refs = refs[:count], refs[count], refs[count + 1 :]
    unit_ref, first_gain_ref, first_shift_ref, bias_ref, gain_ref, shift_ref, up_ref = refs[:7]
    out_ref, grad_ref, low_ref, sums_ref, total_ref, down_ref, sems = refs[7:]
    step = pl.program_id(0)

    @pl.when(step == 0)
    def _():
        for copy in down_copies(meta_ref, down_refs, down_ref, sems):
            copy.start()

    part = product_nt(act_ref[0], down_group(down_ref, sems, step))

    @pl.when(step == 0)
    def _():
        total_ref[...] = part

    @pl.when(step > 0)
    def _():
        total_ref[...] += part

    @pl.when(step == pl.num_programs(0) - 1)
    def _():
        def chunk(at):
            first = unit_ref[at, :] * first_gain_ref[...] + first_shift_ref[...]
            second, unit, inverse = normalize(
                first + total_ref[at, :] + bias_ref[...], gain_ref[...], shift_ref[...]
            )
            out_ref[at, :] = second.astype(BF)
            upstream = up_ref[at, :].astype(F32)
            grad = norm_back(upstream, unit, inverse, gain_ref[...])
            grad_ref[at, :] = grad
            low_ref[at, :] = grad.astype(BF)
            return grad, upstream * unit, upstream

        sums = by_chunks(total_ref.shape[0], total_ref.shape[1], 64, chunk)
        for k in range(3):
            sums_ref[k : k + 1, :] = sums[k]


def turn(meta, downs, acts, unit, first_gain, first_shift, bias, gain, shift, cotangent):
    rows, width = unit.shape
    groups, _, units = acts.shape
    return pl.pallas_call(
        functools.partial(turn_body, len(downs)),
        grid=(groups,),
        in_specs=[smem()] + [unmoved()] * len(downs) + [group_spec(rows, units)] + [vmem()] * 7,
        out_specs=[fixed(rows, width)] * 3 + [fixed(3, width)],
        out_shape=[
            spec(BF, rows, width),
            spec(F32, rows, width),
            spec(BF, rows, width),
            spec(F32, 3, width),
        ],
        scratch_shapes=[pltpu.VMEM((rows, width), F32)] + held(width, units),
        compiler_params=params(),
        cost_estimate=cost(8 * rows * width * units, 16 << 20),
        name="turn",
    )(meta, *downs, acts, unit, first_gain, first_shift, bias, gain, shift, cotangent)


def leave_body(units, count, meta_ref, bundle_ref, *refs):
    down_refs, refs = refs[:count], refs[count:]
    slope_ref, low_ref, second_ref, unit_ref, inverse_ref, gain_ref = refs[:6]
    inner_ref, hidden_ref, attn_ref, own_ref, next_ref, far_rows_ref, sums_ref = refs[6:13]
    out_ref, out_sems, up_ref, up_sems, down_ref, down_sems = refs[13:]
    step = pl.program_id(0)

    @pl.when(step == 0)
    def _():
        copies = down_copies(meta_ref, down_refs, down_ref, down_sems)
        copies += side_copies(meta_ref, bundle_ref, up_ref, up_sems, 0)
        copies += side_copies(meta_ref, bundle_ref, out_ref, out_sems, units)
        for copy in copies:
            copy.start()
        hidden_ref[...] = second_ref[...]

    down = down_group(down_ref, down_sems, step)
    grad = product(low_ref[...], down) * slope_ref[0].astype(F32)
    inner = grad.astype(BF)
    inner_ref[0] = inner
    total_inner = jnp.sum(inner.astype(F32), axis=0, keepdims=True)
    sums_ref[pl.ds(3 + (meta_ref[0] ^ step), 1), :] = total_inner
    side_wait(bundle_ref, up_ref, up_sems, 0, step)
    hidden_ref[...] += product_nt(inner, up_ref[step])

    @pl.when(step == pl.num_programs(0) - 1)
    def _():
        for copy in side_copies(meta_ref, bundle_ref, out_ref, out_sems, units):
            copy.wait()
        back = hidden_ref[...]
        unit = unit_ref[...]
        hidden = norm_back(back, unit, inverse_ref[...], gain_ref[...])
        hidden_ref[...] = hidden
        sums_ref[0:1, :] = jnp.sum(hidden, axis=0, keepdims=True)
        sums_ref[1:2, :] = jnp.sum(back * unit, axis=0, keepdims=True)
        sums_ref[2:3, :] = jnp.sum(back, axis=0, keepdims=True)
        attn = hidden.astype(BF)
        attn_ref[...] = attn
        for j in range(4):
            mixed = product(attn, out_ref[j]).T.astype(BF)
            if j == 0:
                own_ref[...] = mixed
            elif j == 1:
                next_ref[...] = mixed
            else:
                far_rows_ref[j - 2] = mixed


def leave(meta, bundle, downs, slopes, low, second, unit, inverse, gain):
    rows, width = low.shape
    groups, _, units = slopes.shape
    feats = bundle.shape[2] - units
    return pl.pallas_call(
        functools.partial(leave_body, units, len(downs)),
        grid=(groups,),
        in_specs=[smem()] + [unmoved()] * (1 + len(downs)) + [group_spec(rows, units)] + [vmem()] * 5,
        out_specs=[
            group_spec(rows, units),
            fixed(rows, width),
            fixed(rows, width),
            fixed(feats, rows),
            fixed(feats, rows),
            fixed(2, feats, rows),
            fixed(3 + groups, width),
        ],
        out_shape=[
            spec(BF, groups, rows, units),
            spec(F32, rows, width),
            spec(BF, rows, width),
            spec(BF, feats, rows),
            spec(BF, feats, rows),
            spec(BF, 2, feats, rows),
            spec(F32, 3 + groups, width),
        ],
        scratch_shapes=held(width, feats) + held(width, units) + held(width, units),
        compiler_params=params(),
        cost_estimate=cost(16 * rows * width * units, 28 << 20),
        name="leave",
    )(meta, bundle, *downs, slopes, low, second, unit, inverse, gain)


def outer_body(shard, extra, keep, meta_ref, left_ref, right_ref, *refs):
    if extra:
        attn_ref, mixed_refs, sum_refs, refs = refs[0], refs[1:3], refs[3:5], refs[5:]
    if keep:
        arrived_ref, refs = refs[0], refs[1:]
        left_t_ref, attn_t_ref = left_ref, attn_ref if extra else None
    else:
        left_t_ref, attn_t_ref = refs[1], refs[2] if extra else None
    out_ref = refs[0]
    step = pl.program_id(0)
    units = right_ref.shape[2]
    width = left_t_ref.shape[0]
    pairs = width // shard // 2
    lanes = out_ref.shape[3]

    if not keep:

        @pl.when(step == 0)
        def _():
            left_t_ref[...] = left_ref[...].T
            if extra:
                attn_t_ref[...] = attn_ref[...].T

    def put(low, rows, lane, values):
        if keep:
            values = values + arrived_ref[low, 0, rows, lane].astype(F32)
        out_ref[low, 0, rows, lane] = values.astype(BF)

    def spread(values, lane):
        for block in range(2 * pairs):
            rows = slice(block // 2 * shard, (block // 2 + 1) * shard)
            put(block % 2, rows, lane, values[block * shard : (block + 1) * shard])

    spread(product(left_t_ref[...], right_ref[0]), slice(0, units))
    if extra:
        for j in range(2):

            @pl.when(step ^ (meta_ref[0] // 2) == j)
            def _(j=j):
                spread(product_nt(attn_t_ref[...], mixed_refs[j][0]), slice(units, lanes))

        sums = jnp.concatenate(
            [sum_refs[0][...], sum_refs[1][...], jnp.zeros((16 - 10, width), F32)], axis=0
        )
        for low in range(2):
            put(low, slice(pairs * shard, pairs * shard + 16), slice(0, width), sums)
            out_ref[low, 0, pairs * shard :, width:lanes] = jnp.zeros((16, lanes - width), BF)


def outer(meta, shard, left, rights, attn=None, mixed=(), sums=(), arrived=None):
    keep = arrived is not None
    rows, width = left.shape[::-1] if keep else left.shape
    groups, _, units = rights.shape
    extra = attn is not None
    feats = mixed[0].shape[1] if extra else 0
    depth = width // 2 + (16 if extra else 0)

    def group(i, meta_ref):
        return 2 * (i ^ (meta_ref[0] // 2)) + (0 if keep else 1)

    args = [left, rights] + ([attn, *mixed, *sums] if extra else [])
    block = pl.BlockSpec((2, 1, depth, units + feats), lambda i, m: (0, i, 0, 0))
    turned = [] if keep else [left, attn] if extra else [left]
    grid_spec = pltpu.PrefetchScalarGridSpec(
        num_scalar_prefetch=1,
        grid=(2,),
        in_specs=[vmem(), pl.BlockSpec((1, rows, units), lambda i, m: (group(i, m), 0, 0))]
        + ([vmem()] if extra else [])
        + [pl.BlockSpec((1, *v.shape[1:]), lambda i, m: (0, 0, 0)) for v in mixed]
        + [vmem()] * len(sums)
        + ([block] if keep else []),
        out_specs=[block] + [vmem()] * len(turned),
    )
    return pl.pallas_call(
        functools.partial(outer_body, shard, extra, keep),
        grid_spec=grid_spec,
        out_shape=[spec(BF, 2, 2, depth, units + feats)] + [spec(BF, width, rows) for _ in turned],
        compiler_params=params(),
        cost_estimate=cost(4 * rows * width * units, 8 << 20),
        name="outer",
    )(meta, *args, *([arrived] if keep else []))


def inputs_body(*refs):
    dq_refs, (dk_ref, dv_ref, turned_ref) = refs[:4], refs[4:7]
    own_ref, next_ref, out_ref = refs[7:10]
    rows = dq_refs[0].shape[1]
    weight = turned_ref[...]
    for r in (1, 3, 0, 2):
        at = slice(r * rows, (r + 1) * rows)
        grad = jnp.concatenate([dq_refs[r][...], dk_ref[:, at], dv_ref[:, at]], axis=0)
        back = product(grad.T, weight)
        if r == 0:
            own_ref[...] = back
        elif r == 2:
            next_ref[...] = back
        else:
            out_ref[(r // 2) * rows : (r // 2 + 1) * rows, :] = back.astype(BF)


def input_grads(dq, dk, dv, turned):
    rows = dq[0].shape[1]
    width = turned.shape[1]
    return pl.pallas_call(
        inputs_body,
        in_specs=[vmem()] * 7,
        out_specs=[vmem()] * 3,
        out_shape=[spec(F32, rows, width), spec(F32, rows, width), spec(BF, 2 * rows, width)],
        compiler_params=params(),
        cost_estimate=cost(8 * rows * width * width, 12 << 20),
        name="input_grads",
    )(*dq, dk, dv, turned)


def projections_body(shard, *refs):
    meta_ref, dq_refs, (dk_ref, dv_ref, all_ref, keep_ref, send_ref) = refs[0], refs[1:5], refs[5:10]
    held_ref = refs[10]
    rows = dq_refs[0].shape[1]
    depth = keep_ref.shape[0] - 16
    grad = jnp.concatenate(
        [jnp.concatenate([ref[...] for ref in dq_refs], axis=1), dk_ref[...], dv_ref[...]], axis=0
    )
    held_ref[...] = product(grad, all_ref[...]).T.astype(BF)
    sums = product_nt(jnp.ones((16, 4 * rows), BF), grad).astype(BF)
    for flip, out_ref in ((0, keep_ref), (1, send_ref)):
        for i in range(depth // shard):
            block = 2 * i + (meta_ref[1] ^ flip)
            if shard % 16 == 0:
                start = pl.multiple_of(block * shard, shard)
                out_ref[i * shard : (i + 1) * shard, :] = held_ref[pl.ds(start, shard), :]
            else:
                even = held_ref[2 * i * shard : (2 * i + 1) * shard, :]
                odd = held_ref[(2 * i + 1) * shard : (2 * i + 2) * shard, :]
                out_ref[i * shard : (i + 1) * shard, :] = jnp.where(block % 2 == 0, even, odd)
        out_ref[depth:, :] = sums


def projection_grads(meta, shard, dq, dk, dv, tokens):
    width = tokens.shape[1]
    feats = dq[0].shape[0]
    return pl.pallas_call(
        functools.partial(projections_body, shard),
        in_specs=[smem()] + [vmem()] * 7,
        out_specs=[vmem()] * 2,
        out_shape=[spec(BF, width // 2 + 16, 3 * feats)] * 2,
        scratch_shapes=[pltpu.VMEM((width, 3 * feats), BF)],
        compiler_params=params(),
        cost_estimate=cost(2 * tokens.shape[0] * width * 3 * feats, 12 << 20),
        name="projection_grads",
    )(meta, *dq, dk, dv, tokens)


def exchanger(axis_dp, axis_tensor):
    def swap(values, dp_bits, tensor_bits):
        pairs = [
            (d * axis_tensor + t, (d ^ dp_bits) * axis_tensor + (t ^ tensor_bits))
            for d in range(axis_dp)
            for t in range(axis_tensor)
        ]
        return lax.ppermute(values, ("dp", "tensor"), pairs)

    return swap


def tie(*values):
    return lax.optimization_barrier(values)


def add(left, right):
    return (left.astype(F32) + right.astype(F32)).astype(BF)


def total(parts):
    return functools.reduce(jnp.add, [parts[i].astype(F32) for i in range(parts.shape[0])])


def local(
    axis_dp,
    axis_tensor,
    inputs,
    segments,
    query_weight,
    query_bias,
    key_weight,
    value_weight,
    value_bias,
    output_weight,
    output_bias,
    up_weight,
    up_bias,
    down_weight,
    down_bias,
    first_gain,
    first_shift,
    second_gain,
    second_shift,
    cotangent,
):
    swap = exchanger(axis_dp, axis_tensor)
    place_dp, place_tensor = lax.axis_index("dp"), lax.axis_index("tensor")
    meta = jnp.stack([place_tensor, place_dp % 2, place_dp]).astype(jnp.int32)
    rows, width = inputs.shape[1:]
    shard = query_weight.shape[0]
    feats = output_weight.shape[0]
    heads = feats // HEAD
    units = up_weight.shape[1]
    pairs = axis_dp // 2
    row = lambda v: v.reshape(1, -1).astype(F32)
    flat = lambda z, x, y, c: (2 * z + x) * axis_tensor + 2 * y + c
    near_groups = [
        [flat(z, x, y, c) for x in range(2) for y in range(2)] for z in range(pairs) for c in range(2)
    ]
    deep_groups = [[2 * z + x for z in range(pairs)] for x in range(2)]

    own = inputs[0]
    notes = jnp.zeros((16, width), BF)
    notes = notes.at[0, :rows].set(segments[0].astype(BF)).at[1, :units].set(up_bias)
    message = jnp.concatenate([own, notes])
    across = swap(message, 0, 2)
    bundle = jnp.concatenate([query_weight, key_weight, value_weight], axis=1)
    copies = jnp.broadcast_to(bundle[None], (axis_dp,) + bundle.shape)
    qkv_weight = lax.all_to_all(copies, "dp", 0, 0, tiled=True).reshape(width, 3 * feats)
    near = swap(message, 0, 1)
    far = swap(across, 0, 1)
    tokens = [message, near, across, far]

    up_bundle = lax.all_gather(
        jnp.concatenate([up_weight, output_weight.T], axis=1), ("tensor", "dp"), axis=0, tiled=True
    ).reshape(axis_tensor, width, units + feats)
    _, down = tie(qkv_weight, down_weight.T)
    around = jnp.stack([down] + [swap(down, 2 * k, 0) for k in range(1, pairs)])
    across_around = swap(around, 0, 2)

    noted = jnp.stack([v[rows:] for v in tokens]).astype(F32)
    docs = noted[:, 0, :rows].reshape(-1)
    bias = noted[:, 1:2, :units]
    lane = jnp.arange(HEAD, dtype=F32)
    same = docs[:, None] == lane[None, :]
    aux_query = (docs[None, :] == lane[:, None]).astype(BF)
    aux_key = jnp.where(same | (lane[None, :] >= 8), 0.0, -far_score).astype(BF)
    output_bias, first_gain, first_shift, down_bias, second_gain, second_shift, bias, aux_key = tie(
        *[row(v) for v in (output_bias, first_gain, first_shift, down_bias, second_gain, second_shift)],
        bias, aux_key,
    )
    qkv_bias = jnp.concatenate([query_bias, jnp.zeros_like(query_bias), value_bias]).astype(F32)
    all_tokens, turned, queries, keys, values, values_t, keys_t = project(
        qkv_weight, tokens, rows, qkv_bias[feats:].reshape(1, -1), qkv_bias.reshape(-1, 1),
        aux_query, aux_key, heads,
    )

    _, around_late = tie(queries, around)
    beside = swap(around_late, 1, 0)

    mixed23, log23 = attend_forward(keys, queries, values_t, (2, 3))
    queries, mixed23 = tie(queries, mixed23)
    arrived = swap(mixed23, 0, 2)
    _, around_late, across_around = tie(mixed23, around_late, across_around)
    columns = [around, None, swap(around_late, 0, 1), None, across_around, None]
    columns += [swap(across_around, 0, 1), None]
    mixed1, log1 = attend_forward(keys, queries, values_t, (1,))
    queries, mixed1 = tie(queries, mixed1)
    arrived1 = swap(mixed1, 0, 1)
    _, beside = tie(mixed1, beside)
    across_beside = swap(beside, 0, 2)
    queries, arrived = tie(queries, arrived)
    arrived3 = swap(arrived[1:], 0, 1)
    mixed0, log0 = attend_forward(keys, queries, values_t, (0,))
    mixed = [mixed0, arrived1, arrived, arrived3]

    low, unit_first, inverse_first, acts, slopes = enter(
        meta, up_bundle, mixed, own, output_bias, first_gain, first_shift, bias
    )
    _, later = tie(inverse_first, across_beside)
    columns[1::2] = [beside, swap(beside, 0, 1), across_beside, swap(later, 0, 1)]
    downs = columns
    if shard % 16:
        order = [2 * k + b for b in range(2) for k in range(pairs)]
        places = jnp.argsort(jnp.array(order) ^ place_dp)
        downs = [jnp.concatenate(columns[2 * g : 2 * g + 2]) for g in range(4)]
        downs = [v[places].reshape(1, width, units) for v in downs]
    layer_out, grad_second, second_low, sums_second = turn(
        meta, downs, acts, unit_first, first_gain, first_shift,
        down_bias, second_gain, second_shift, cotangent[0],
    )
    send_b, second_t = outer(meta, shard, second_low, acts)
    second_low, send_b = tie(second_low, send_b)
    moved_b = swap(send_b, 0, 1)
    inners, grad_hidden, grad_attn, grad0, next_mixed, far_mixed, sums_first = leave(
        meta, up_bundle, downs, slopes, second_low, grad_second, unit_first, inverse_first, first_gain
    )

    def reduce_near(values):
        values = values.reshape((4,) + values.shape[2:])
        return lax.all_to_all(values, ("dp", "tensor"), 0, 0, axis_index_groups=near_groups, tiled=True)

    def reduce_deep(values):
        return lax.all_to_all(values, "dp", 0, 0, axis_index_groups=deep_groups, tiled=True)

    def deep_parts(values):
        return values[: pairs * shard].reshape(pairs, shard, -1)

    def part_at(parts, k):
        return lax.dynamic_index_in_dim(parts, (place_dp // 2) ^ k, 0, False)

    arrived_g = swap(far_mixed, 0, 2)
    g1 = swap(next_mixed, 0, 1)
    (part_b,) = outer(meta, shard, second_t, acts, arrived=moved_b)
    inners, part_b = tie(inners, part_b)
    near_b = reduce_near(part_b)
    sums_both = (sums_first, sums_second)
    send_a, low_t, attn_t = outer(meta, shard, low, inners, grad_attn, mixed[1::2], sums_both)
    grad0, send_a, g1, arrived_g = tie(grad0, send_a, g1, arrived_g)
    moved_a = swap(send_a, 0, 1)
    g2, g3 = arrived_g[0], swap(arrived_g[1], 0, 1)
    operands = (keys, queries, values, keys_t)
    (dq0, dq1), carried = attend_back(
        operands, (0, 1), ((log0, 0), (log1, 0)), ((mixed0, 0), (mixed1, 0)), (grad0, g1), None, False
    )
    low_t, carried, moved_a = tie(low_t, carried, moved_a)
    (part_a,) = outer(meta, shard, low_t, inners, attn_t, mixed[::2], sums_both, moved_a)
    carried, part_a, near_b, g2, g3 = tie(carried, part_a, near_b, g2, g3)
    near_a = reduce_near(part_a)
    parts_b = deep_parts(total(near_b).astype(BF))
    sent_b = [part_at(parts_b, k) for k in range(1, pairs)]
    carried, parts_b, *sent_b = tie(carried, parts_b, *sent_b)
    own_b = part_at(parts_b, 0).astype(F32)
    for k in range(1, pairs):
        own_b = own_b + swap(sent_b[k - 1], 2 * k, 0).astype(F32)
    (dq2, dq3), (dk, dv) = attend_back(
        operands, (2, 3), ((log23, 0), (log23, 1)), ((mixed23, 0), (mixed23, 1)), (g2, g3), carried, True
    )
    dq2, own_b = tie(dq2, own_b)
    dq = (dq0, dq1, dq2, dq3)
    own_rows, next_rows, sent_rows = input_grads(dq, dk, dv, turned)
    moved = swap(sent_rows, 0, 1)
    dk, sent_rows = tie(dk, sent_rows)
    keep_c, send_c = projection_grads(meta, shard, dq, dk, dv, all_tokens)
    _, moved = tie(send_c, moved)
    next_rows = add(next_rows, moved[rows:])
    arrived_c = swap(send_c, 1, 0)
    arrived_rows = swap(next_rows, 0, 2)
    _, _, near_a = tie(send_c, next_rows, near_a)
    sum_a = total(near_a).astype(BF)
    notes = jnp.broadcast_to(sum_a[None, pairs * shard :], (pairs, 16, sum_a.shape[1]))
    packed_a = jnp.concatenate([deep_parts(sum_a), notes], axis=1)
    deep_a = reduce_deep(packed_a)
    _, arrived_c = tie(packed_a, arrived_c)
    sum_c = add(keep_c, arrived_c)
    parts_c, notes = deep_parts(sum_c), sum_c[pairs * shard :]
    own_c = jnp.concatenate([part_at(parts_c, 0), notes]).astype(F32)
    for k in range(1, pairs):
        arrived_part = swap(jnp.concatenate([part_at(parts_c, k), notes]), 2 * k, 0)
        _, arrived_part = tie(arrived_rows, arrived_part)
        own_c = own_c + arrived_part.astype(F32)
    own_a = total(deep_a)
    grad_inputs = grad_hidden + own_rows + moved[:rows].astype(F32) + arrived_rows.astype(F32)
    sums = own_a[shard:, :width]
    sum_up = lax.dynamic_index_in_dim(sums[3:7], place_tensor, 0, False)
    head_sums = own_c[shard]

    return (
        layer_out[None],
        grad_inputs[None],
        own_c[:shard, :feats],
        head_sums[:feats],
        own_c[:shard, feats : 2 * feats],
        own_c[:shard, 2 * feats :],
        head_sums[2 * feats :],
        own_a[:shard, units:].T,
        sums[0],
        own_a[:shard, :units],
        sum_up,
        own_b.T,
        sums[7],
        sums[1],
        sums[2],
        sums[8],
        sums[9],
    )


def solution(mesh):
    axis_dp, axis_tensor = mesh.shape["dp"], mesh.shape["tensor"]
    if axis_tensor != 4 or axis_dp < 2 or axis_dp & (axis_dp - 1):
        raise ValueError("mesh sizes")
    return jax.shard_map(
        functools.partial(local, axis_dp, axis_tensor),
        mesh=mesh,
        in_specs=(
            P("dp", "tensor", None),
            P("dp", "tensor"),
            P("dp", "tensor"),
            P("tensor"),
            P("dp", "tensor"),
            P("dp", "tensor"),
            P("tensor"),
            P("tensor", "dp"),
            P(),
            P("dp", "tensor"),
            P("tensor"),
            P("tensor", "dp"),
            P(),
            P(),
            P(),
            P(),
            P(),
            P("dp", "tensor", None),
        ),
        out_specs=(
            P("dp", "tensor", None),
            P("dp", "tensor", None),
            P("dp", "tensor"),
            P("tensor"),
            P("dp", "tensor"),
            P("dp", "tensor"),
            P("tensor"),
            P("tensor", "dp"),
            P(),
            P("dp", "tensor"),
            P("tensor"),
            P("tensor", "dp"),
            P(),
            P(),
            P(),
            P(),
            P(),
        ),
        check_vma=False,
    )
```
